32 devices in a mesh: dp: 8 (over z, x), mp: 4 (over y, core).
Axes of the slice: x: 2, y: 2, z: 4, core: 2. Of those that a mesh axis runs over, the one named last changes fastest.
Arguments:
- q_latent: bfloat16 [2048, 2, 768], P('dp', None, 'mp'), may hold values from -6 to 6
- kv_latent: bfloat16 [2048, 2, 256], P('dp', None, 'mp'), may hold values from -6 to 6
- q_head_grad: bfloat16 [2048, 512], P('dp'), may hold values from -0.1875 to 0.1875
- k_head_grad: bfloat16 [2048, 512], P('dp'), may hold values from -0.1875 to 0.1875
- q_heads: bfloat16 [2048, 512], P('dp', 'mp'), may hold values from -6 to 6
- k_heads: bfloat16 [2048, 512], P('dp', 'mp'), may hold values from -6 to 6
- query_pick: int32 [8, 16, 4], P('dp', None, 'mp'), may hold values from 0 to 255
- key_pick: int32 [8, 16, 4], P('dp', None, 'mp'), may hold values from 0 to 255
- q_weight: float32 [8, 768, 128], P('dp', 'mp'), may hold values from -6 to 6
- k_weight: float32 [8, 256, 128], P('dp', 'mp'), may hold values from -6 to 6
- q_moment: float32 [8, 768, 128], P('dp', 'mp'), may hold values from -6 to 6
- k_moment: float32 [8, 256, 128], P('dp', 'mp'), may hold values from -6 to 6
Outputs:
- q_weight_new: float32 [8, 768, 128], P('dp', 'mp')
- k_weight_new: float32 [8, 256, 128], P('dp', 'mp')
- q_moment_new: float32 [8, 768, 128], P('dp', 'mp')
- k_moment_new: float32 [8, 256, 128], P('dp', 'mp')
The draws below stay inside these ranges and needn't reach their ends.
Inputs may be any that keep to these rules, and one draw needn't show every extreme that they name: `query_pick`: the index of a token among the 256 tokens of its own block b. `key_pick`: the index of a token among the 256 tokens of its own block b.
All inputs are finite; a program needn't handle non-finite values.
Results may differ from the reference program's by a relative error of at most 0.0003.
Values sent between devices are 32-bit elements; how exact they have to be, the bound alone decides.
A program may use at most 64 MiB of HBM per device.

```python
import math
import jax
import jax.numpy as jnp
from jax import lax

QR = 1536
KR = 512
DN = 128
TOK_DEV = 256
PICKS = 16
ITERS = 5
HEADS = 4
TOKENS = 2048
N_DP = 8


def touch_ends(result, stream_key, low, top_value):
    dims = result.shape
    spot = [jax.random.randint(jax.random.fold_in(stream_key, axis), (), 0, dims[axis]) for axis in range(len(dims))]
    result = result.at[tuple(spot)].set(low)
    longest = dims.index(max(dims))
    spot[longest] = (spot[longest] + 1) % dims[longest]
    return result.at[tuple(spot)].set(top_value)


def strengthened(result, stream_key, source, target, parts, factor):
    owner, partner = [(jnp.arange(result.shape[axis_at]) // (result.shape[axis_at] // parts)).reshape([-1 if axis == axis_at else 1 for axis in range(result.ndim)]) for axis_at in (source, target)]
    chosen = jax.random.permutation(stream_key, parts)[partner]
    strong = (owner == chosen) | (owner == (partner + parts // 2) % parts)
    return jnp.where(strong, factor * result, result)


def levels(key, dims, pieces, low, high):
    def one(position, shards_of):
        steps = jax.random.uniform(jax.random.fold_in(jax.random.fold_in(key, 6), position), (shards_of,), jnp.float32, low / len(pieces), high / len(pieces))
        return jnp.repeat(jnp.exp(steps), dims[position] // shards_of).reshape((-1,) + (1,) * (len(dims) - position - 1))

    loudness = one(*pieces[0])
    for cut in pieces[1:]:
        loudness = loudness * one(*cut)
    return loudness


def gaussian(own_key, extent, spread, bound, cuts=(), kind=jnp.bfloat16):
    result = spread * jax.random.normal(own_key, extent, jnp.float32)
    if cuts:
        result = result * levels(own_key, extent, cuts, -0.22, 0.18)
    return jnp.clip(result, -bound, bound).astype(kind)


def bell_draw_with(rng, dims, scale, limit, shards, heavy, held_as=jnp.bfloat16):
    entries = scale * jax.random.normal(rng, dims, jnp.float32)
    if shards:
        entries = entries * levels(rng, dims, shards, -0.22, 0.18)
    return jnp.clip(strengthened(entries, jax.random.fold_in(rng, 3), *heavy), -limit, limit).astype(held_as)


def setup_inputs(seed: int = 0) -> dict:
    key_list = jax.random.split(jax.random.key(seed), 13)
    return {
        "q_latent": gaussian(key_list[0], (TOKENS, 2, QR // 2), 1.0, 6.0, ((0, 8), (2, 4))),
        "kv_latent": gaussian(key_list[1], (TOKENS, 2, KR // 2), 1.0, 6.0, ((0, 8), (2, 4))),
        "q_head_grad": bell_draw_with(key_list[2], (TOKENS, HEADS * DN), TOKENS ** -0.5, 0.1875, ((0, 8),), (0, 1, 8, 2.0)),
        "k_head_grad": bell_draw_with(key_list[3], (TOKENS, HEADS * DN), TOKENS ** -0.5, 0.1875, ((0, 8),), (0, 1, 8, 2.0)),
        "q_heads": gaussian(key_list[4], (TOKENS, HEADS * DN), 1.0, 6.0, ((0, 8), (1, 4))),
        "k_heads": gaussian(key_list[5], (TOKENS, HEADS * DN), 1.0, 6.0, ((0, 8), (1, 4))),
        "query_pick": touch_ends(jax.random.randint(key_list[6], (N_DP, PICKS, HEADS), 0, TOK_DEV), jax.random.fold_in(key_list[6], 1), 0, TOK_DEV - 1).astype(jnp.int32),
        "key_pick": touch_ends(jax.random.randint(key_list[7], (N_DP, PICKS, HEADS), 0, TOK_DEV), jax.random.fold_in(key_list[7], 1), 0, TOK_DEV - 1).astype(jnp.int32),
        "q_weight": gaussian(key_list[8], (2 * HEADS, QR // 2, DN), 1.0, 6.0, ((0, 8), (1, 4)), jnp.float32),
        "k_weight": gaussian(key_list[9], (2 * HEADS, KR // 2, DN), 1.0, 6.0, ((0, 8), (1, 4)), jnp.float32),
        "q_moment": gaussian(key_list[10], (2 * HEADS, QR // 2, DN), 1.0, 6.0, ((0, 8), (1, 4)), jnp.float32),
        "k_moment": gaussian(key_list[11], (2 * HEADS, KR // 2, DN), 1.0, 6.0, ((0, 8), (1, 4)), jnp.float32),
    }


MOMENTUM = 0.95
STEP_SIZE = 1.0
DECAY = 0.1
CLIP_LEVEL = 0.1
SCORE_SCALE = 1.0 / math.sqrt(192.0)
COEFF_A = 3.4445
COEFF_B = -4.775
COEFF_C = 2.0315
HIGHEST = lax.Precision.HIGHEST

def grad_slots(latent, head_grad):
    flat = latent.reshape(latent.shape[0], -1)
    total = jnp.dot(flat.T, head_grad, preferred_element_type=jnp.float32)
    rows_all = total.shape[0]
    total = total.reshape(2, rows_all // 2, HEADS, DN).transpose(0, 2, 1, 3)
    return total.reshape(2 * HEADS, rows_all // 2, DN)

def to_heads(slots):
    count, half_rows, width = slots.shape
    stacked = slots.reshape(2, count // 2, half_rows, width).transpose(1, 0, 2, 3)
    return stacked.reshape(count // 2, 2 * half_rows, width)

def to_slots(stacked):
    heads, rows_all, width = stacked.shape
    split = stacked.reshape(heads, 2, rows_all // 2, width).transpose(1, 0, 2, 3)
    return split.reshape(2 * heads, rows_all // 2, width)

def gramians(stacked):
    return jnp.einsum('hrc,hrd->hcd', stacked, stacked, precision=HIGHEST)

def polar(stacked):
    grams = gramians(stacked)
    scale = 1.0 / jnp.sqrt(jnp.trace(grams, axis1=1, axis2=2) + 1.0)
    current = stacked * scale[:, None, None]
    grams = grams * (scale * scale)[:, None, None]
    for step in range(ITERS):
        square = jnp.einsum('hcd,hde->hce', grams, grams, precision=HIGHEST)
        mixer = COEFF_B * grams + COEFF_C * square
        current = COEFF_A * current + jnp.einsum('hrc,hcd->hrd', current, mixer, precision=HIGHEST)
        if step + 1 < ITERS:
            grams = gramians(current)
    return current

def head_peaks(q_heads, k_heads, query_pick, key_pick):
    q_cube = q_heads.reshape(N_DP, TOK_DEV, HEADS, DN)
    k_cube = k_heads.reshape(N_DP, TOK_DEV, HEADS, DN)
    picked_q = jnp.take_along_axis(q_cube, query_pick.astype(jnp.int32)[..., None], axis=1)
    picked_k = jnp.take_along_axis(k_cube, key_pick.astype(jnp.int32)[..., None], axis=1)
    scores = lax.optimization_barrier(jnp.sum(picked_q.astype(jnp.float32) * picked_k.astype(jnp.float32), axis=3)) * SCORE_SCALE
    return lax.optimization_barrier(jnp.max(scores, axis=(0, 1)))

def reference(q_latent, kv_latent, q_head_grad, k_head_grad, q_heads, k_heads, query_pick, key_pick, q_weight, k_weight, q_moment, k_moment):
    q_moment_new = MOMENTUM * q_moment + grad_slots(q_latent, q_head_grad)
    k_moment_new = MOMENTUM * k_moment + grad_slots(kv_latent, k_head_grad)
    q_ortho = to_slots(polar(to_heads(q_moment_new)))
    k_ortho = to_slots(polar(to_heads(k_moment_new)))
    peak = head_peaks(q_heads, k_heads, query_pick, key_pick)
    shrink = jnp.sqrt(CLIP_LEVEL / jnp.maximum(peak, CLIP_LEVEL))
    shrink_slots = jnp.concatenate([shrink, shrink])[:, None, None]
    keep = 1.0 - STEP_SIZE * DECAY
    q_weight_new = (q_weight * keep - STEP_SIZE * 0.2 * math.sqrt(QR) * q_ortho) * shrink_slots
    k_weight_new = (k_weight * keep - STEP_SIZE * 0.2 * math.sqrt(KR) * k_ortho) * shrink_slots
    return (q_weight_new, k_weight_new, q_moment_new, k_moment_new)
```

```python
import functools
import math

import jax
import jax.numpy as jnp
from jax import lax
from jax.experimental import pallas as pl
from jax.experimental.pallas import tpu as pltpu
from jax.sharding import PartitionSpec as P

ITERS = 5
CHUNKS = 4
MOMENTUM = 0.95
STEP_SIZE = 1.0
DECAY = 0.1
CLIP_LEVEL = 0.1
SCORE_SCALE = 1.0 / math.sqrt(192.0)
COEFF_A = 3.4445
COEFF_B = -4.775
COEFF_C = 2.0315
LOWEST = -1e30
MESH = pl.DeviceIdType.MESH
F32 = jnp.float32
BF16 = jnp.bfloat16


def split(value):
    high = value.astype(BF16)
    return high, (value - high.astype(F32)).astype(BF16)


def mm(a, b):
    return jnp.dot(a, b, preferred_element_type=F32)


def mm3(a, b):
    both = mm(a[0], jnp.concatenate([b[0], b[1]], axis=1))
    width = b[0].shape[1]
    return both[:, :width] + (both[:, width:] + mm(a[1], b[0]))


def gram(rows):
    high, low = split(rows)
    high_t = high.T
    cross = mm(high_t, low)
    return mm(high_t, high) + (cross + cross.T)


def fold(matrix):
    width = matrix.shape[0]
    half = width // 2
    row = lax.broadcasted_iota(jnp.int32, (half, width), 0)
    lane = lax.broadcasted_iota(jnp.int32, (half, width), 1)
    lower = matrix[half:]
    body = jnp.where(lane >= row, matrix[:half], pltpu.roll(lower, half, 1))
    ends = jnp.sum(jnp.where(lane == row + half, lower, 0.0), axis=0, keepdims=True)
    return body, jnp.broadcast_to(ends, (8, width))


def unfold(message):
    width = message.shape[1]
    half = width // 2
    row = lax.broadcasted_iota(jnp.int32, (half, width), 0)
    lane = lax.broadcasted_iota(jnp.int32, (half, width), 1)
    body = message[:half]
    ends = jnp.broadcast_to(message[half : half + 1], (half, width))
    top = jnp.where(lane >= row, body, 0.0)
    strict = jnp.where((lane >= half) & (lane - half < row), pltpu.roll(body, half, 1), 0.0)
    one_side = jnp.concatenate([top, jnp.where(lane == row + half, ends, strict)], axis=0)
    full_row = lax.broadcasted_iota(jnp.int32, (width, width), 0)
    full_lane = lax.broadcasted_iota(jnp.int32, (width, width), 1)
    return one_side + jnp.where(full_row == full_lane, 0.0, one_side.T)


def column(row):
    count = row.shape[1]
    spread = jnp.broadcast_to(row, (count, count))
    same = lax.broadcasted_iota(jnp.int32, (count, count), 0) == lax.broadcasted_iota(
        jnp.int32, (count, count), 1
    )
    picked = jnp.where(same, spread, 0).astype(F32)
    return jnp.sum(picked, axis=1, keepdims=True).astype(jnp.int32)


def partner(index, count, step):
    if count & (count - 1):
        return lax.rem(index + step, count)
    result = 0
    bit = 1
    while bit < count:
        held = lax.rem(lax.div(index, bit), 2)
        result = result + bit * ((1 - held) if step & bit else held)
        bit *= 2
    return result


def kernel(
    n_dp, n_mp, heads,
    ql_in, kl_in, qg_in, kg_in, qh_in, kh_in, qp_in, kp_in, qw_in, kw_in, qm_in, km_in,
    qw_out, kw_out, qm_out, km_out, mix, shrink_out,
    ql_ref, kl_ref, qg_ref, kg_ref, qh_ref, kh_ref, qp_ref, kp_ref, qw_ref, kw_ref, qm_ref, km_ref, in_sems,
    near_send, near_recv, own, far_recv, raw_recv, peak_send, peak_recv, peak2_send, peak2_recv,
    grams, gram_recv, row_send, row_recv,
    ns_s, ns_r, fs_s, fs_r, rw_s, rw_r, pk_s, pk_r, pm_s, pm_r, g_s, g_r, y_s, y_r, m_s, m_r,
):
    dp = lax.axis_index("dp")
    mp = lax.axis_index("mp")
    n_outer = n_dp // 2
    outer = lax.div(dp, 2)
    inner = lax.rem(dp, 2)
    core = lax.rem(mp, 2)
    group = lax.div(mp, 2)
    n_group = n_mp // 2
    q_rows = qm_ref.shape[1]
    k_rows = km_ref.shape[1]
    width = qm_ref.shape[2]
    tokens = qg_ref.shape[0]
    other_core = mp + 1 - 2 * core

    loads = [
        pltpu.make_async_copy(src, dst, in_sems.at[i])
        for i, (src, dst) in enumerate((
            (ql_in, ql_ref), (kl_in, kl_ref), (qg_in, qg_ref), (kg_in, kg_ref),
            (qp_in, qp_ref), (kp_in, kp_ref), (qh_in, qh_ref), (kh_in, kh_ref),
            (qm_in, qm_ref), (km_in, km_ref), (qw_in, qw_ref), (kw_in, kw_ref),
        ))
    ]
    for each in loads:
        each.start()

    barrier = pltpu.get_barrier_semaphore()
    for step in range(1, n_dp):
        pl.semaphore_signal(
            barrier, inc=1, device_id=(lax.rem(dp + step, n_dp), mp), device_id_type=MESH
        )
    def owner(step):
        across = lax.rem(dp + (step // n_group) * heads, n_dp)
        return across, 2 * lax.rem(group + step, n_group) + core

    for step in range(n_group + 1, 2 * n_group):
        pl.semaphore_signal(barrier, inc=1, device_id=owner(step), device_id_type=MESH)
    for step in range(1, n_mp):
        pl.semaphore_signal(
            barrier, inc=1, device_id=(dp, lax.rem(mp + step, n_mp)), device_id_type=MESH
        )

    def copy(src, dst, send, recv, where):
        return pltpu.make_async_remote_copy(
            src_ref=src, dst_ref=dst, send_sem=send, recv_sem=recv,
            device_id=where, device_id_type=MESH,
        )

    def term(dst, where, to_outer, to_inner):
        slot = 2 * to_outer + to_inner
        half = lax.div(slot, heads)
        cols = pl.ds(pl.multiple_of(lax.rem(slot, heads) * width, width), width)
        dst[where, :q_rows, :] = mm(ql_ref[half], qg_ref[:, cols])
        dst[where, q_rows:, :] = mm(kl_ref[half], kg_ref[:, cols])

    for each in loads[:4]:
        each.wait()
    entered = n_dp + n_mp + n_group - 3
    neighbour = (dp + 1 - 2 * inner, mp)
    last = n_outer - 1
    line = n_outer == 4
    tall = q_rows + k_rows
    step_rows = tall // CHUNKS
    half = tall // 2
    inside = lax.rem(lax.div(outer, 2) + lax.rem(outer, 2), 2)
    by = [partner(outer, n_outer, step) for step in range(n_outer)]

    def rows_of(chunk):
        return pl.ds(chunk * step_rows, step_rows)

    if line:
        split_to = by[2] + inside * (by[1] - by[2])
        whole_to = by[1] + inside * (by[2] - by[1])
        order = [by[3], split_to, whole_to, by[0]]
        spans = [range(CHUNKS), range(CHUNKS // 2), range(CHUNKS), range(CHUNKS)]
    else:
        order = by[::-1]
        spans = [range(CHUNKS)] * n_outer

    def near_copy(spot, chunk):
        where = rows_of(chunk)
        return copy(
            near_send.at[spot, where], near_recv.at[spot, where],
            ns_s.at[spot, chunk], ns_r.at[spot, chunk], neighbour,
        )

    def far_copy(spot, slot, chunk, target):
        where = rows_of(chunk)
        return copy(
            own.at[spot, where], far_recv.at[slot, where],
            fs_s.at[spot, chunk], fs_r.at[slot, chunk], (2 * target + inner, mp),
        )

    def raw_copy(which):
        source = (near_send, own)[which]
        return copy(
            source.at[1, pl.ds(half, half)], raw_recv.at[which],
            rw_s.at[which], rw_r.at[which], (2 * split_to + inner, mp),
        )

    near, far, raw = [], [], []

    def start(into, each):
        each.start()
        into.append(each)

    term(near_send, 0, order[0], 1 - inner)
    pl.semaphore_wait(barrier, entered)
    for chunk in spans[0]:
        start(near, near_copy(0, chunk))
    if line:
        term(near_send, 1, order[1], 1 - inner)
        start(raw, raw_copy(0))
        for chunk in spans[1]:
            start(near, near_copy(1, chunk))
        term(own, 1, order[1], inner)
        start(raw, raw_copy(1))
    for spot in range(2 if line else 1, n_outer):
        term(near_send, spot, order[spot], 1 - inner)
        for chunk in spans[spot]:
            if line and spot == last and chunk >= CHUNKS // 2:
                continue
            start(near, near_copy(spot, chunk))
    for spot in range(n_outer):
        if not (line and spot == 1):
            term(own, spot, order[spot], inner)

    for each in loads[4:8]:
        each.wait()
    local_heads = qp_ref.shape[0]
    lane = lax.broadcasted_iota(jnp.int32, (8, width), 1)
    peaks = jnp.full((8, width), LOWEST, F32)
    ids = lax.broadcasted_iota(jnp.int32, (qp_ref.shape[2], tokens), 1)
    for head in range(local_heads):
        span = slice(head * width, (head + 1) * width)
        pick_q = (ids == column(qp_ref[head])).astype(F32).astype(BF16)
        pick_k = (ids == column(kp_ref[head])).astype(F32).astype(BF16)
        score = jnp.sum(
            mm(pick_q, qh_ref[:, span]) * mm(pick_k, kh_ref[:, span]), axis=1, keepdims=True
        )
        top = jnp.max(score * SCORE_SCALE, axis=0, keepdims=True)
        peaks = jnp.where(lane == mp * local_heads + head, top, peaks)
    peak_send[...] = peaks
    peak_copies = []
    for step in range(1, n_dp):
        each = copy(
            peak_send, peak_recv.at[step - 1], pk_s.at[step - 1], pk_r.at[step - 1],
            (lax.rem(dp + step, n_dp), mp),
        )
        each.start()
        peak_copies.append(each)

    def meet(spot, chunk):
        near_copy(spot, chunk).wait_recv()
        where = rows_of(chunk)
        own[spot, where] = own[spot, where] + near_recv[spot, where]

    def gather(slot, chunk):
        far_copy(0, slot, chunk, outer).wait_recv()
        return far_recv[slot, rows_of(chunk)]

    relay = 3
    if line:
        first_to = by[1] + inside * (by[3] - by[1])
        for chunk in spans[0]:
            meet(0, chunk)
            start(far, far_copy(0, relay * (1 - inside), chunk, first_to))
        raw[0].wait_recv()
        low = pl.ds(half, half)
        near_send[last, low] = near_send[last, low] + raw_recv[0]
        for chunk in range(CHUNKS // 2, CHUNKS):
            start(near, near_copy(last, chunk))
        for chunk in spans[1]:
            meet(1, chunk)
            start(far, far_copy(1, 1, chunk, split_to))
        raw[1].wait_recv()
        own[last, low] = own[last, low] + raw_recv[1]
        for chunk in spans[2]:

            @pl.when(inside == 1)
            def _():
                own[2, rows_of(chunk)] = own[2, rows_of(chunk)] + gather(relay, chunk)

            meet(2, chunk)
            start(far, far_copy(2, 2, chunk, whole_to))
    else:
        for spot in range(last):
            for chunk in spans[spot]:
                meet(spot, chunk)
                start(far, far_copy(spot, spot, chunk, order[spot]))

    for each in peak_copies:
        each.wait_recv()
    peaks = jnp.maximum(peaks, jnp.max(peak_recv[...], axis=0))
    peak2_send[...] = peaks
    peak2_copies = []
    for step in range(1, n_mp):
        each = copy(
            peak2_send, peak2_recv.at[step - 1], pm_s.at[step - 1], pm_r.at[step - 1],
            (dp, lax.rem(mp + step, n_mp)),
        )
        each.start()
        peak2_copies.append(each)

    if line:

        @pl.when(inside == 1)
        def _():
            for chunk in spans[0]:
                own[last, rows_of(chunk)] = own[last, rows_of(chunk)] + gather(0, chunk)

        for chunk in spans[1]:
            own[last, rows_of(chunk)] = own[last, rows_of(chunk)] + gather(1, chunk)
        for chunk in spans[last]:
            meet(last, chunk)
            own[last, rows_of(chunk)] = own[last, rows_of(chunk)] + gather(2, chunk)
    else:
        for chunk in spans[last]:
            meet(last, chunk)
            for spot in range(last):
                own[last, rows_of(chunk)] = own[last, rows_of(chunk)] + gather(spot, chunk)
    total = own[last]
    for each in loads[8:]:
        each.wait()
    q_moment = MOMENTUM * qm_ref[0] + total[:q_rows]
    k_moment = MOMENTUM * km_ref[0] + total[q_rows:]
    qm_out[0] = q_moment
    km_out[0] = k_moment

    top = width // 2
    for which, matrix in enumerate((gram(q_moment), gram(k_moment))):
        body, ends = fold(matrix)
        grams[which, :top, :] = body
        grams[which, top:, :] = ends
    swap = copy(grams.at[1 - core], gram_recv, g_s, g_r, (dp, other_core))
    swap.start()
    swap.wait_recv()
    whole = grams[core] + gram_recv[...]
    row_send[...] = whole
    rows = []
    for step in range(1, 2 * n_group):
        each = copy(
            row_send, row_recv.at[step - 1], y_s.at[step - 1], y_r.at[step - 1], owner(step)
        )
        each.start()
        rows.append(each)
    for each in peak2_copies:
        each.wait_recv()
    peaks = jnp.maximum(peaks, jnp.max(peak2_recv[...], axis=0))
    mine = jnp.where(lane == lax.rem(dp, heads), peaks, LOWEST)
    peak = jnp.max(jnp.max(mine, axis=0, keepdims=True), axis=1, keepdims=True)
    shrink = jnp.sqrt(CLIP_LEVEL / jnp.maximum(peak, CLIP_LEVEL))
    keep = 1.0 - STEP_SIZE * DECAY
    shrink_out[...] = jnp.broadcast_to(shrink, shrink_out.shape)
    qw_out[0] = (qw_ref[0] * keep) * shrink
    kw_out[0] = (kw_ref[0] * keep) * shrink
    for each in rows:
        each.wait_recv()
    whole = unfold(whole + jnp.sum(row_recv[...], axis=0))

    eye = (
        lax.broadcasted_iota(jnp.int32, (width, width), 0)
        == lax.broadcasted_iota(jnp.int32, (width, width), 1)
    ).astype(F32)
    trace = jnp.sum(jnp.sum(whole * eye, axis=0, keepdims=True), axis=1, keepdims=True)
    scale = 1.0 / jnp.sqrt(trace + 1.0)
    current = whole * (scale * scale)
    mixed = None
    for step in range(ITERS):
        parts = split(current)
        square = mm3(parts, parts)
        poly = COEFF_A * eye + COEFF_B * current + COEFF_C * square
        pair = split(poly)
        mixed = poly * scale if mixed is None else mm3(split(mixed), pair)
        if step + 1 < ITERS:
            current = mm3(split(mm3(parts, pair)), pair)
    mix[core] = mixed
    swap2 = copy(mix.at[core], mix.at[core], m_s, m_r, (dp, other_core))
    swap2.start()

    swap2.wait_recv()
    for each in near + far + raw + peak_copies + peak2_copies + [swap] + rows + [swap2]:
        each.wait_send()


def finish(n_mp, qw_ref, kw_ref, qm_ref, km_ref, mix_ref, shrink_ref, qw_out, kw_out, qm_out, km_out):
    groups = ((qw_ref, qm_ref, qw_out, qm_out), (kw_ref, km_ref, kw_out, km_out))
    for which, (weight, moment, weight_out, moment_out) in enumerate(groups):
        rows = moment[0]
        size = STEP_SIZE * 0.2 * math.sqrt(2 * n_mp * rows.shape[0])
        ortho = mm3(split(rows), split(mix_ref[which]))
        moment_out[0] = rows
        weight_out[0] = weight[0] - (size * ortho) * shrink_ref[0:1, :]


def local(
    q_latent, kv_latent, q_head_grad, k_head_grad, q_heads, k_heads,
    query_pick, key_pick, q_weight, k_weight, q_moment, k_moment,
):
    n_dp = lax.axis_size("dp")
    n_mp = lax.axis_size("mp")
    heads = n_dp // 2
    n_outer = n_dp // 2
    n_group = n_mp // 2
    rows = q_latent.shape[2] + kv_latent.shape[2]
    width = q_moment.shape[2]
    operands = (
        q_latent.transpose(1, 2, 0), kv_latent.transpose(1, 2, 0), q_head_grad, k_head_grad,
        q_heads, k_heads, query_pick.transpose(2, 0, 1), key_pick.transpose(2, 0, 1),
        q_weight, k_weight, q_moment, k_moment,
    )
    vmem = pltpu.VMEM
    dma = pltpu.SemaphoreType.DMA
    square = (width, width)
    folded = (width // 2 + 8, width)
    tile = (8, width)
    shapes = [a.shape for a in (q_weight, k_weight, q_moment, k_moment)]
    parts = pl.pallas_call(
        functools.partial(kernel, n_dp, n_mp, heads),
        out_shape=[vmem(shape, F32) for shape in shapes + [(2,) + square, tile]],
        in_specs=[pl.BlockSpec(memory_space=pl.ANY)] * 12,
        out_specs=[pl.BlockSpec(memory_space=vmem)] * 6,
        scratch_shapes=[vmem(a.shape, a.dtype) for a in operands] + [
            dma((12,)),
            vmem((n_outer, rows, width), F32),
            vmem((n_outer, rows, width), F32),
            vmem((n_outer, rows, width), F32),
            vmem((n_outer, rows, width), F32),
            vmem((2, rows // 2, width), F32),
            vmem(tile, F32),
            vmem((n_dp - 1,) + tile, F32),
            vmem(tile, F32),
            vmem((n_mp - 1,) + tile, F32),
            vmem((2,) + folded, F32),
            vmem(folded, F32),
            vmem(folded, F32),
            vmem((2 * n_group - 1,) + folded, F32),
            dma((n_outer, CHUNKS)), dma((n_outer, CHUNKS)),
            dma((n_outer, CHUNKS)), dma((n_outer, CHUNKS)),
            dma((2,)), dma((2,)),
            dma((n_dp - 1,)), dma((n_dp - 1,)),
            dma((n_mp - 1,)), dma((n_mp - 1,)),
            dma, dma,
            dma((2 * n_group - 1,)), dma((2 * n_group - 1,)),
            dma, dma,
        ],
        compiler_params=pltpu.CompilerParams(
            collective_id=0, has_side_effects=True, vmem_limit_bytes=56 * 1024 * 1024
        ),
    )(*operands)
    return pl.pallas_call(
        functools.partial(finish, n_mp),
        out_shape=[jax.ShapeDtypeStruct(shape, F32) for shape in shapes],
        in_specs=[pl.BlockSpec(memory_space=vmem)] * 6,
        out_specs=[pl.BlockSpec(memory_space=vmem)] * 4,
    )(*[pltpu.with_memory_space_constraint(part, vmem) for part in parts])


def solution(mesh):
    rows3 = P("dp", "mp", None)
    in_specs = (
        P("dp", None, "mp"), P("dp", None, "mp"), P("dp", None), P("dp", None),
        P("dp", "mp"), P("dp", "mp"), P("dp", None, "mp"), P("dp", None, "mp"),
        rows3, rows3, rows3, rows3,
    )
    return jax.shard_map(
        lambda *args: tuple(local(*args)),
        mesh=mesh, in_specs=in_specs, out_specs=(rows3,) * 4, check_vma=False,
    )
```

```python
import functools
import math

import jax
import jax.numpy as jnp
from jax import lax
from jax.experimental import pallas as pl
from jax.experimental.pallas import tpu as pltpu
from jax.sharding import PartitionSpec as P

ITERS = 5
MOMENTUM = 0.95
STEP_SIZE = 1.0
DECAY = 0.1
CLIP_LEVEL = 0.1
SCORE_SCALE = 1.0 / math.sqrt(192.0)
COEFF_A = 3.4445
COEFF_B = -4.775
COEFF_C = 2.0315
LOWEST = -1e30
MESH = pl.DeviceIdType.MESH
F32 = jnp.float32
BF16 = jnp.bfloat16


def split(value):
    high = value.astype(BF16)
    return high, (value - high.astype(F32)).astype(BF16)


def mm(a, b):
    return jnp.dot(a, b, preferred_element_type=F32)


def mm3(a, b):
    both = mm(a[0], jnp.concatenate([b[0], b[1]], axis=1))
    width = b[0].shape[1]
    return both[:, :width] + (both[:, width:] + mm(a[1], b[0]))


def gram_pair(rows):
    high, low = split(rows)
    return mm(high.T, jnp.concatenate([high, low], axis=1))


def gram_of(pair):
    width = pair.shape[0]
    cross = pair[:, width:]
    return pair[:, :width] + (cross + cross.T)


def fold(matrix):
    width = matrix.shape[0]
    half = width // 2
    row = lax.broadcasted_iota(jnp.int32, (half, width), 0)
    lane = lax.broadcasted_iota(jnp.int32, (half, width), 1)
    lower = matrix[half:]
    body = jnp.where(lane >= row, matrix[:half], pltpu.roll(lower, half, 1))
    ends = jnp.sum(jnp.where(lane == row + half, lower, 0.0), axis=0, keepdims=True)
    return jnp.concatenate([body, ends], axis=0)


def unfold(message):
    width = message.shape[1]
    half = width // 2
    row = lax.broadcasted_iota(jnp.int32, (half, width), 0)
    lane = lax.broadcasted_iota(jnp.int32, (half, width), 1)
    body = message[:half]
    ends = jnp.broadcast_to(message[half : half + 1], (half, width))
    top = jnp.where(lane >= row, body, 0.0)
    strict = jnp.where((lane >= half) & (lane - half < row), pltpu.roll(body, half, 1), 0.0)
    one_side = jnp.concatenate([top, jnp.where(lane == row + half, ends, strict)], axis=0)
    full_row = lax.broadcasted_iota(jnp.int32, (width, width), 0)
    full_lane = lax.broadcasted_iota(jnp.int32, (width, width), 1)
    return one_side + jnp.where(full_row == full_lane, 0.0, one_side.T)


def column(row):
    count = row.shape[1]
    spread = jnp.broadcast_to(row, (count, count))
    same = lax.broadcasted_iota(jnp.int32, (count, count), 0) == lax.broadcasted_iota(
        jnp.int32, (count, count), 1
    )
    picked = jnp.where(same, spread, 0).astype(F32)
    return jnp.sum(picked, axis=1, keepdims=True).astype(jnp.int32)


def partner(index, count, step):
    if count & (count - 1):
        return lax.rem(index + step, count)
    result = 0
    bit = 1
    while bit < count:
        held = lax.rem(lax.div(index, bit), 2)
        result = result + bit * ((1 - held) if step & bit else held)
        bit *= 2
    return result


def kernel(
    n_dp, n_mp, heads,
    ql_in, kl_in, qg_in, kg_in, qh_in, kh_in, qp_in, kp_in, qw_in, kw_in, qm_in, km_in,
    qw_out, kw_out, qm_out, km_out, mix, shrink_out,
    ql_ref, kl_ref, qg_ref, kg_ref, qh_ref, kh_ref, qp_ref, kp_ref, qw_ref, kw_ref, qm_ref, km_ref, in_sems,
    near_send, near_recv, own, far_recv, raw_recv, peak_send, peak_recv, peak2_send, peak2_recv,
    grams, gram_recv, row_send, row_recv,
    ns_s, ns_r, fs_s, fs_r, rw_s, rw_r, pk_s, pk_r, pm_s, pm_r, g_s, g_r, y_s, y_r, m_s, m_r,
):
    dp = lax.axis_index("dp")
    mp = lax.axis_index("mp")
    n_outer = n_dp // 2
    outer = lax.div(dp, 2)
    inner = lax.rem(dp, 2)
    core = lax.rem(mp, 2)
    group = lax.div(mp, 2)
    n_group = n_mp // 2
    q_rows = qm_ref.shape[1]
    k_rows = km_ref.shape[1]
    width = qm_ref.shape[2]
    tokens = qg_ref.shape[0]
    other_core = mp + 1 - 2 * core

    loads = [
        pltpu.make_async_copy(src, dst, in_sems.at[i])
        for i, (src, dst) in enumerate((
            (ql_in, ql_ref), (kl_in, kl_ref), (qg_in, qg_ref), (kg_in, kg_ref),
            (qp_in, qp_ref), (kp_in, kp_ref), (qh_in, qh_ref), (kh_in, kh_ref),
            (qm_in, qm_ref), (km_in, km_ref), (qw_in, qw_ref), (kw_in, kw_ref),
        ))
    ]
    for each in loads:
        each.start()

    barrier = pltpu.get_barrier_semaphore()
    for step in range(1, n_dp):
        pl.semaphore_signal(
            barrier, inc=1, device_id=(lax.rem(dp + step, n_dp), mp), device_id_type=MESH
        )
    def owner(step):
        across = lax.rem(dp + (step // n_group) * heads, n_dp)
        return across, 2 * lax.rem(group + step, n_group) + core

    for step in range(n_group + 1, 2 * n_group):
        pl.semaphore_signal(barrier, inc=1, device_id=owner(step), device_id_type=MESH)
    for step in range(1, n_mp):
        pl.semaphore_signal(
            barrier, inc=1, device_id=(dp, lax.rem(mp + step, n_mp)), device_id_type=MESH
        )

    def copy(src, dst, send, recv, where):
        return pltpu.make_async_remote_copy(
            src_ref=src, dst_ref=dst, send_sem=send, recv_sem=recv,
            device_id=where, device_id_type=MESH,
        )

    def term(dst, where, to_outer, to_inner):
        slot = 2 * to_outer + to_inner
        half = lax.div(slot, heads)
        cols = pl.ds(pl.multiple_of(lax.rem(slot, heads) * width, width), width)
        dst[where, :k_rows, :] = mm(kl_ref[half], kg_ref[:, cols])
        dst[where, k_rows:, :] = mm(ql_ref[half], qg_ref[:, cols])

    for each in loads[:4]:
        each.wait()
    entered = n_dp + n_mp + n_group - 3
    neighbour = (dp + 1 - 2 * inner, mp)
    last = n_outer - 1
    line = n_outer == 4
    tall = q_rows + k_rows
    step_rows = k_rows
    chunks = tall // step_rows
    half = tall // 2
    inside = lax.rem(lax.div(outer, 2) + lax.rem(outer, 2), 2)
    by = [partner(outer, n_outer, step) for step in range(n_outer)]

    def rows_of(chunk):
        return pl.ds(chunk * step_rows, step_rows)

    if line:
        split_to = by[2] + inside * (by[1] - by[2])
        whole_to = by[1] + inside * (by[2] - by[1])
        order = [by[3], split_to, whole_to, by[0]]
        kept = chunks // 2
        spans = [range(chunks), range(kept), range(chunks), range(chunks)]
    else:
        order = by[::-1]
        spans = [range(chunks)] * n_outer

    def near_copy(spot, chunk):
        where = rows_of(chunk)
        return copy(
            near_send.at[spot, where], near_recv.at[spot, where],
            ns_s.at[spot, chunk], ns_r.at[spot, chunk], neighbour,
        )

    def far_copy(spot, slot, chunk, target):
        where = rows_of(chunk)
        return copy(
            own.at[spot, where], far_recv.at[slot, where],
            fs_s.at[spot, chunk], fs_r.at[slot, chunk], (2 * target + inner, mp),
        )

    def raw_copy(which):
        source = (near_send, own)[which]
        return copy(
            source.at[1, pl.ds(half, half)], raw_recv.at[which],
            rw_s.at[which], rw_r.at[which], (2 * split_to + inner, mp),
        )

    def send_near(spot, which):
        for chunk in which:
            near_copy(spot, chunk).start()

    raw = [raw_copy(0), raw_copy(1)] if line else []
    term(near_send, 0, order[0], 1 - inner)
    pl.semaphore_wait(barrier, entered)
    send_near(0, spans[0])
    if line:
        term(near_send, 1, order[1], 1 - inner)
        raw[0].start()
        term(own, 1, order[1], inner)
        raw[1].start()
        term(near_send, 2, order[2], 1 - inner)

        @pl.when(inside == 1)
        def _():
            send_near(2, spans[2])
            send_near(1, spans[1])

        @pl.when(inside == 0)
        def _():
            send_near(1, spans[1])
            send_near(2, spans[2])

    for each in loads[4:8]:
        each.wait()
    local_heads = qp_ref.shape[0]
    lane = lax.broadcasted_iota(jnp.int32, (1, width), 1)
    peaks = jnp.full((1, width), LOWEST, F32)
    ids = lax.broadcasted_iota(jnp.int32, (qp_ref.shape[2], tokens), 1)
    for head in range(local_heads):
        span = slice(head * width, (head + 1) * width)
        pick_q = (ids == column(qp_ref[head])).astype(F32).astype(BF16)
        pick_k = (ids == column(kp_ref[head])).astype(F32).astype(BF16)
        score = jnp.sum(
            mm(pick_q, qh_ref[:, span]) * mm(pick_k, kh_ref[:, span]), axis=1, keepdims=True
        )
        top = jnp.max(score * SCORE_SCALE, axis=0, keepdims=True)
        peaks = jnp.where(lane == mp * local_heads + head, top, peaks)
    peak_send[...] = peaks
    peak_copies = []
    for step in range(1, n_dp):
        each = copy(
            peak_send, peak_recv.at[step - 1], pk_s.at[step - 1], pk_r.at[step - 1],
            (lax.rem(dp + step, n_dp), mp),
        )
        each.start()
        peak_copies.append(each)

    if line:
        term(near_send, last, order[last], 1 - inner)
        send_near(last, range(kept))
    else:
        for spot in range(1, n_outer):
            term(near_send, spot, order[spot], 1 - inner)
            send_near(spot, spans[spot])
    for spot in range(n_outer):
        if not (line and spot == 1):
            term(own, spot, order[spot], inner)

    def meet(spot, chunk):
        near_copy(spot, chunk).wait_recv()
        where = rows_of(chunk)
        own[spot, where] = own[spot, where] + near_recv[spot, where]

    def gather(slot, chunk):
        far_copy(0, slot, chunk, outer).wait_recv()
        return far_recv[slot, rows_of(chunk)]

    relay = 3

    def pass_on(spot):
        for chunk in spans[spot]:
            meet(spot, chunk)
            far_copy(spot, spot, chunk, order[spot]).start()

    if line:
        first_to = by[1] + inside * (by[3] - by[1])
        for chunk in spans[0]:
            meet(0, chunk)
            far_copy(0, relay * (1 - inside), chunk, first_to).start()
        raw[0].wait_recv()
        low = pl.ds(half, half)
        near_send[last, low] = near_send[last, low] + raw_recv[0]
        send_near(last, range(kept, chunks))

        @pl.when(inside == 1)
        def _():
            for chunk in spans[2]:
                own[2, rows_of(chunk)] = own[2, rows_of(chunk)] + gather(relay, chunk)
                meet(2, chunk)
                far_copy(2, 2, chunk, whole_to).start()
            pass_on(1)
            for chunk in spans[0]:
                own[last, rows_of(chunk)] = own[last, rows_of(chunk)] + gather(0, chunk)

        @pl.when(inside == 0)
        def _():
            pass_on(1)
            pass_on(2)

        raw[1].wait_recv()
        own[last, low] = own[last, low] + raw_recv[1]
    else:
        for spot in range(last):
            pass_on(spot)

    for each in loads[8:]:
        each.wait()

    def complete(chunk):
        where = rows_of(chunk)
        meet(last, chunk)
        if line:
            if chunk in spans[1]:
                own[last, where] = own[last, where] + gather(1, chunk)
            total = own[last, where] + gather(2, chunk)
        else:
            total = own[last, where]
            for spot in range(last):
                total = total + gather(spot, chunk)
        if not chunk:
            rows = MOMENTUM * km_ref[0] + total
            km_out[0] = rows
        else:
            part = pl.ds((chunk - 1) * step_rows, step_rows)
            rows = MOMENTUM * qm_ref[0, part] + total
            qm_out[0, part] = rows
        return gram_pair(rows)

    swap = copy(grams.at[1 - core], gram_recv, g_s, g_r, (dp, other_core))
    grams[1] = fold(gram_of(complete(0)))

    @pl.when(core == 0)
    def _():
        swap.start()

    pair = complete(1)
    for chunk in range(2, chunks):
        pair = pair + complete(chunk)
    grams[0] = fold(gram_of(pair))

    @pl.when(core == 1)
    def _():
        swap.start()

    swap.wait_recv()
    whole = grams[core] + gram_recv[...]
    row_send[...] = whole
    rows = []
    for step in range(1, 2 * n_group):
        each = copy(
            row_send, row_recv.at[step - 1], y_s.at[step - 1], y_r.at[step - 1], owner(step)
        )
        each.start()
        rows.append(each)
    for each in peak_copies:
        each.wait_recv()
    peaks = jnp.maximum(peaks, jnp.max(peak_recv[...], axis=0))
    peak2_send[...] = peaks
    peak2_copies = []
    for step in range(1, n_mp):
        each = copy(
            peak2_send, peak2_recv.at[step - 1], pm_s.at[step - 1], pm_r.at[step - 1],
            (dp, lax.rem(mp + step, n_mp)),
        )
        each.start()
        peak2_copies.append(each)

    for each in rows:
        each.wait_recv()
    whole = unfold(whole + jnp.sum(row_recv[...], axis=0))

    eye = (
        lax.broadcasted_iota(jnp.int32, (width, width), 0)
        == lax.broadcasted_iota(jnp.int32, (width, width), 1)
    ).astype(F32)
    trace = jnp.sum(jnp.sum(whole * eye, axis=0, keepdims=True), axis=1, keepdims=True)
    scale = 1.0 / jnp.sqrt(trace + 1.0)
    current = whole * (scale * scale)
    mixed = None
    for step in range(ITERS):
        parts = split(current)
        square = mm3(parts, parts)
        poly = COEFF_A * eye + COEFF_B * current + COEFF_C * square
        pair = split(poly)
        mixed = poly * scale if mixed is None else mm3(split(mixed), pair)
        if step + 1 < ITERS:
            current = mm3(split(mm3(parts, pair)), pair)
    mix[core] = mixed
    swap2 = copy(mix.at[core], mix.at[core], m_s, m_r, (dp, other_core))
    swap2.start()
    for each in peak2_copies:
        each.wait_recv()
    peaks = jnp.maximum(peaks, jnp.max(peak2_recv[...], axis=0))
    mine = jnp.where(lane == lax.rem(dp, heads), peaks, LOWEST)
    peak = jnp.max(jnp.max(mine, axis=0, keepdims=True), axis=1, keepdims=True)
    shrink = jnp.sqrt(CLIP_LEVEL / jnp.maximum(peak, CLIP_LEVEL))
    keep = 1.0 - STEP_SIZE * DECAY
    shrink_out[...] = jnp.broadcast_to(shrink, shrink_out.shape)
    qw_out[0] = (qw_ref[0] * keep) * shrink
    kw_out[0] = (kw_ref[0] * keep) * shrink
    swap2.wait_recv()
    for spot in range(n_outer):
        for chunk in spans[spot]:
            near_copy(spot, chunk).wait_send()
            if spot < last:
                far_copy(spot, spot, chunk, order[spot]).wait_send()
    for each in raw + peak_copies + peak2_copies + [swap] + rows + [swap2]:
        each.wait_send()


def finish(n_mp, qw_ref, kw_ref, qm_ref, km_ref, mix_ref, shrink_ref, qw_out, kw_out, qm_out, km_out):
    groups = ((qw_ref, qm_ref, qw_out, qm_out), (kw_ref, km_ref, kw_out, km_out))
    for which, (weight, moment, weight_out, moment_out) in enumerate(groups):
        rows = moment[0]
        size = STEP_SIZE * 0.2 * math.sqrt(2 * n_mp * rows.shape[0])
        ortho = mm3(split(rows), split(mix_ref[which]))
        moment_out[0] = rows
        weight_out[0] = weight[0] - (size * ortho) * shrink_ref[...]


def local(
    q_latent, kv_latent, q_head_grad, k_head_grad, q_heads, k_heads,
    query_pick, key_pick, q_weight, k_weight, q_moment, k_moment,
):
    n_dp = lax.axis_size("dp")
    n_mp = lax.axis_size("mp")
    heads = n_dp // 2
    n_outer = n_dp // 2
    n_group = n_mp // 2
    rows = q_latent.shape[2] + kv_latent.shape[2]
    width = q_moment.shape[2]
    operands = (
        q_latent.transpose(1, 2, 0), kv_latent.transpose(1, 2, 0), q_head_grad, k_head_grad,
        q_heads, k_heads, query_pick.transpose(2, 0, 1), key_pick.transpose(2, 0, 1),
        q_weight, k_weight, q_moment, k_moment,
    )
    vmem = pltpu.VMEM
    dma = pltpu.SemaphoreType.DMA
    square = (width, width)
    folded = (width // 2 + 1, width)
    tile = (1, width)
    chunks = rows // k_moment.shape[1]
    shapes = [a.shape for a in (q_weight, k_weight, q_moment, k_moment)]
    parts = pl.pallas_call(
        functools.partial(kernel, n_dp, n_mp, heads),
        out_shape=[vmem(shape, F32) for shape in shapes + [(2,) + square, tile]],
        in_specs=[pl.BlockSpec(memory_space=pl.ANY)] * 12,
        out_specs=[pl.BlockSpec(memory_space=vmem)] * 6,
        scratch_shapes=[vmem(a.shape, a.dtype) for a in operands] + [
            dma((12,)),
            vmem((n_outer, rows, width), F32),
            vmem((n_outer, rows, width), F32),
            vmem((n_outer, rows, width), F32),
            vmem((n_outer, rows, width), F32),
            vmem((2, rows // 2, width), F32),
            vmem(tile, F32),
            vmem((n_dp - 1,) + tile, F32),
            vmem(tile, F32),
            vmem((n_mp - 1,) + tile, F32),
            vmem((2,) + folded, F32),
            vmem(folded, F32),
            vmem(folded, F32),
            vmem((2 * n_group - 1,) + folded, F32),
            dma((n_outer, chunks)), dma((n_outer, chunks)),
            dma((n_outer, chunks)), dma((n_outer, chunks)),
            dma((2,)), dma((2,)),
            dma((n_dp - 1,)), dma((n_dp - 1,)),
            dma((n_mp - 1,)), dma((n_mp - 1,)),
            dma, dma,
            dma((2 * n_group - 1,)), dma((2 * n_group - 1,)),
            dma, dma,
        ],
        compiler_params=pltpu.CompilerParams(
            collective_id=0, has_side_effects=True, vmem_limit_bytes=56 * 1024 * 1024
        ),
    )(*operands)
    return pl.pallas_call(
        functools.partial(finish, n_mp),
        out_shape=[jax.ShapeDtypeStruct(shape, F32) for shape in shapes],
        in_specs=[pl.BlockSpec(memory_space=vmem)] * 6,
        out_specs=[pl.BlockSpec(memory_space=vmem)] * 4,
    )(*[pltpu.with_memory_space_constraint(part, vmem) for part in parts])


def solution(mesh):
    rows3 = P("dp", "mp", None)
    in_specs = (
        P("dp", None, "mp"), P("dp", None, "mp"), P("dp", None), P("dp", None),
        P("dp", "mp"), P("dp", "mp"), P("dp", None, "mp"), P("dp", None, "mp"),
        rows3, rows3, rows3, rows3,
    )
    return jax.shard_map(
        lambda *args: tuple(local(*args)),
        mesh=mesh, in_specs=in_specs, out_specs=(rows3,) * 4, check_vma=False,
    )
```

```python
import functools
import math

import jax
import jax.numpy as jnp
from jax import lax
from jax.experimental import pallas as pl
from jax.experimental.pallas import tpu as pltpu
from jax.sharding import PartitionSpec as P

ITERS = 5
MOMENTUM = 0.95
STEP_SIZE = 1.0
DECAY = 0.1
CLIP_LEVEL = 0.1
SCORE_SCALE = 1.0 / math.sqrt(192.0)
COEFF_A = 3.4445
COEFF_B = -4.775
COEFF_C = 2.0315
LOWEST = -1e30
MESH = pl.DeviceIdType.MESH
F32 = jnp.float32
BF16 = jnp.bfloat16


def split(value):
    high = value.astype(BF16)
    return high, (value - high.astype(F32)).astype(BF16)


def mm(a, b):
    return jnp.dot(a, b, preferred_element_type=F32)


def mm3(a, b):
    both = mm(a[0], jnp.concatenate([b[0], b[1]], axis=1))
    width = b[0].shape[1]
    return both[:, :width] + (both[:, width:] + mm(a[1], b[0]))


def mm_deep(a, b):
    return mm(
        jnp.concatenate([a[0], a[1], a[0]], axis=1), jnp.concatenate([b[0], b[0], b[1]], axis=0)
    )


def gram_pair(rows):
    high, low = split(rows)
    return mm(high.T, jnp.concatenate([high, low], axis=1))


def gram_of(pair):
    width = pair.shape[0]
    cross = pair[:, width:]
    return pair[:, :width] + (cross + cross.T)


def fold(matrix):
    width = matrix.shape[0]
    half = width // 2
    row = lax.broadcasted_iota(jnp.int32, (half, width), 0)
    lane = lax.broadcasted_iota(jnp.int32, (half, width), 1)
    lower = matrix[half:]
    body = jnp.where(lane >= row, matrix[:half], pltpu.roll(lower, half, 1))
    ends = jnp.sum(jnp.where(lane == row + half, lower, 0.0), axis=0, keepdims=True)
    return jnp.concatenate([body, ends], axis=0)


def unfold(message):
    width = message.shape[1]
    half = width // 2
    row = lax.broadcasted_iota(jnp.int32, (half, width), 0)
    lane = lax.broadcasted_iota(jnp.int32, (half, width), 1)
    body = message[:half]
    ends = jnp.broadcast_to(message[half : half + 1], (half, width))
    top = jnp.where(lane >= row, body, 0.0)
    strict = jnp.where((lane >= half) & (lane - half < row), pltpu.roll(body, half, 1), 0.0)
    one_side = jnp.concatenate([top, jnp.where(lane == row + half, ends, strict)], axis=0)
    full_row = lax.broadcasted_iota(jnp.int32, (width, width), 0)
    full_lane = lax.broadcasted_iota(jnp.int32, (width, width), 1)
    return one_side + jnp.where(full_row == full_lane, 0.0, one_side.T)


def column(row):
    count = row.shape[1]
    spread = jnp.broadcast_to(row, (count, count))
    same = lax.broadcasted_iota(jnp.int32, (count, count), 0) == lax.broadcasted_iota(
        jnp.int32, (count, count), 1
    )
    picked = jnp.where(same, spread, 0).astype(F32)
    return jnp.sum(picked, axis=1, keepdims=True).astype(jnp.int32)


def partner(index, count, step):
    if count & (count - 1):
        return lax.rem(index + step, count)
    result = 0
    bit = 1
    while bit < count:
        held = lax.rem(lax.div(index, bit), 2)
        result = result + bit * ((1 - held) if step & bit else held)
        bit *= 2
    return result


def kernel(
    n_dp, n_mp, heads,
    ql_in, kl_in, qg_in, kg_in, qh_in, kh_in, qp_in, kp_in, qw_in, kw_in, qm_in, km_in,
    qw_out, kw_out, qm_out, km_out, qy_out, ky_out, final, shrink_out,
    latents, grads, act, picks, state, in_sems,
    near_send, near_recv, own, far_recv, raw_recv, peak_send, peak_recv, peak2_send, peak2_recv,
    grams, gram_recv, row_send, row_recv, mix,
    ns_s, ns_r, fs_s, fs_r, rw_r, pk_s, pk_r, pm_s, pm_r, g_s, g_r, y_s, y_r, m_s, m_r,
):
    dp = lax.axis_index("dp")
    mp = lax.axis_index("mp")
    n_outer = n_dp // 2
    outer = lax.div(dp, 2)
    inner = lax.rem(dp, 2)
    core = lax.rem(mp, 2)
    group = lax.div(mp, 2)
    n_group = n_mp // 2
    q_rows = qm_in.shape[1]
    k_rows = km_in.shape[1]
    width = qm_in.shape[2]
    tokens = qg_in.shape[0]
    tall = q_rows + k_rows
    top_rows = pl.ds(0, k_rows)
    low_rows = pl.ds(k_rows, q_rows)
    other_core = mp + 1 - 2 * core

    loads = (
        ((kl_in, latents.at[:, top_rows]), (ql_in, latents.at[:, low_rows])),
        ((kg_in, grads.at[1]), (qg_in, grads.at[0])),
        ((qp_in, picks.at[0]), (kp_in, picks.at[1])),
        ((qh_in, act.at[0]), (kh_in, act.at[1])),
        (
            (km_in.at[0], state.at[1, top_rows]), (qm_in.at[0], state.at[1, low_rows]),
            (kw_in.at[0], state.at[0, top_rows]), (qw_in.at[0], state.at[0, low_rows]),
        ),
    )
    for i, group_of in enumerate(loads):
        for src, dst in group_of:
            pltpu.make_async_copy(src, dst, in_sems.at[i]).start()

    def loaded(*which):
        for i in which:
            ref = (latents, grads, picks, act, state)[i]
            pltpu.make_async_copy(ref, ref, in_sems.at[i]).wait()

    barrier = pltpu.get_barrier_semaphore()
    for step in range(1, n_dp):
        pl.semaphore_signal(
            barrier, inc=1, device_id=(lax.rem(dp + step, n_dp), mp), device_id_type=MESH
        )
    def owner(step):
        across = lax.rem(dp + (step // n_group) * heads, n_dp)
        return across, 2 * lax.rem(group + step, n_group) + core

    for step in range(n_group + 1, 2 * n_group):
        pl.semaphore_signal(barrier, inc=1, device_id=owner(step), device_id_type=MESH)
    for step in range(1, n_mp):
        pl.semaphore_signal(
            barrier, inc=1, device_id=(dp, lax.rem(mp + step, n_mp)), device_id_type=MESH
        )

    def copy(src, dst, send, recv, where):
        return pltpu.make_async_remote_copy(
            src_ref=src, dst_ref=dst, send_sem=send, recv_sem=recv,
            device_id=where, device_id_type=MESH,
        )

    all_peaks = copy(peak_recv, peak_recv, pk_s, pk_r, (dp, other_core))
    all_peaks2 = copy(peak2_recv, peak2_recv, pm_s, pm_r, (dp, other_core))
    all_rows = copy(row_recv, row_recv, y_s, y_r, (dp, other_core))

    def term(dst, spot, to_outer, to_inner):
        slot = 2 * to_outer + to_inner
        half = lax.div(slot, heads)
        cols = pl.ds(pl.multiple_of(lax.rem(slot, heads) * width, width), width)
        first = spot * chunks
        dst[first] = mm(latents[half, :k_rows], grads[1, :, cols])
        rest = mm(latents[half, k_rows:], grads[0, :, cols])
        dst[first + 1 : first + chunks] = rest.reshape(chunks - 1, step_rows, width)

    step_rows = k_rows
    chunks = tall // step_rows
    loaded(0, 1)
    entered = n_dp + n_mp + n_group - 3
    neighbour = (dp + 1 - 2 * inner, mp)
    last = n_outer - 1
    line = n_outer == 4
    inside = lax.rem(lax.div(outer, 2) + lax.rem(outer, 2), 2)
    by = [partner(outer, n_outer, step) for step in range(n_outer)]

    def at(spot, chunk):
        return spot * chunks + chunk

    if line:
        split_to = by[2] + inside * (by[1] - by[2])
        whole_to = by[1] + inside * (by[2] - by[1])
        order = [by[3], split_to, whole_to, by[0]]
        kept = chunks // 2
        spans = [range(chunks), range(kept), range(chunks), range(chunks)]
    else:
        order = by[::-1]
        spans = [range(chunks)] * n_outer

    def near_copy(spot, chunk):
        where = at(spot, chunk)
        return copy(near_send.at[where], near_recv.at[where], ns_s, ns_r.at[where], neighbour)

    def far_copy(spot, slot, chunk, target):
        where = at(slot, chunk)
        return copy(
            own.at[at(spot, chunk)], far_recv.at[where], fs_s, fs_r.at[where],
            (2 * target + inner, mp),
        )

    def raw_copy(which):
        source = (near_send, own)[which]
        return copy(
            source.at[pl.ds(at(1, kept), chunks - kept)], raw_recv.at[which],
            fs_s, rw_r.at[which], (2 * split_to + inner, mp),
        )

    def send_near(spot, which):
        for chunk in which:
            near_copy(spot, chunk).start()

    raw = [raw_copy(0), raw_copy(1)] if line else []
    term(near_send, 0, order[0], 1 - inner)
    pl.semaphore_wait(barrier, entered)
    send_near(0, spans[0])
    if line:
        term(near_send, 1, order[1], 1 - inner)
        raw[0].start()
        term(own, 1, order[1], inner)
        raw[1].start()
        term(near_send, 2, order[2], 1 - inner)

        @pl.when(inside == 1)
        def _():
            send_near(2, spans[2])
            send_near(1, spans[1])

        @pl.when(inside == 0)
        def _():
            send_near(1, spans[1])
            send_near(2, spans[2])

    loaded(2, 3)
    local_heads = picks.shape[1]
    lane = lax.broadcasted_iota(jnp.int32, (1, width), 1)
    peaks = jnp.full((1, width), LOWEST, F32)
    ids = lax.broadcasted_iota(jnp.int32, (picks.shape[3], tokens), 1)
    for head in range(local_heads):
        span = slice(head * width, (head + 1) * width)
        pick_q = (ids == column(picks[0, head])).astype(F32).astype(BF16)
        pick_k = (ids == column(picks[1, head])).astype(F32).astype(BF16)
        score = jnp.sum(
            mm(pick_q, act[0, :, span]) * mm(pick_k, act[1, :, span]), axis=1, keepdims=True
        )
        top = jnp.max(score * SCORE_SCALE, axis=0, keepdims=True)
        peaks = jnp.where(lane == mp * local_heads + head, top, peaks)
    peak_send[...] = peaks
    for step in range(1, n_dp):
        each = copy(
            peak_send, peak_recv.at[step - 1], pk_s, pk_r,
            (lax.rem(dp + step, n_dp), mp),
        )
        each.start()

    if line:
        term(near_send, last, order[last], 1 - inner)
        send_near(last, range(kept))
    else:
        for spot in range(1, n_outer):
            term(near_send, spot, order[spot], 1 - inner)
            send_near(spot, spans[spot])
    for spot in range(n_outer):
        if not (line and spot == 1):
            term(own, spot, order[spot], inner)

    def meet(spot, chunk):
        near_copy(spot, chunk).wait_recv()
        where = at(spot, chunk)
        own[where] = own[where] + near_recv[where]

    def gather(slot, chunk):
        far_copy(0, slot, chunk, outer).wait_recv()
        return far_recv[at(slot, chunk)]

    relay = 3

    def pass_on(spot):
        for chunk in spans[spot]:
            meet(spot, chunk)
            far_copy(spot, spot, chunk, order[spot]).start()

    if line:
        first_to = by[1] + inside * (by[3] - by[1])
        for chunk in spans[0]:
            meet(0, chunk)
            far_copy(0, relay * (1 - inside), chunk, first_to).start()
        raw[0].wait_recv()
        low = pl.ds(at(last, kept), chunks - kept)
        near_send[low] = near_send[low] + raw_recv[0]
        send_near(last, range(kept, chunks))

        @pl.when(inside == 1)
        def _():
            for chunk in spans[2]:
                own[at(2, chunk)] = own[at(2, chunk)] + gather(relay, chunk)
                meet(2, chunk)
                far_copy(2, 2, chunk, whole_to).start()
            pass_on(1)
            for chunk in spans[0]:
                own[at(last, chunk)] = own[at(last, chunk)] + gather(0, chunk)

        @pl.when(inside == 0)
        def _():
            pass_on(1)
            pass_on(2)

        raw[1].wait_recv()
        own[low] = own[low] + raw_recv[1]
    else:
        for spot in range(last):
            pass_on(spot)

    loaded(4)

    def complete(chunk):
        where = at(last, chunk)
        meet(last, chunk)
        if line:
            if chunk in spans[1]:
                own[where] = own[where] + gather(1, chunk)
            total = own[where] + gather(2, chunk)
        else:
            total = own[where]
            for spot in range(last):
                total = total + gather(spot, chunk)
        rows = MOMENTUM * state[1, chunk * step_rows : (chunk + 1) * step_rows] + total
        if not chunk:
            km_out[0] = rows
        else:
            qm_out[0, (chunk - 1) * step_rows : chunk * step_rows] = rows
        return gram_pair(rows)

    swap = copy(grams.at[1 - core], gram_recv, g_s, g_r, (dp, other_core))
    grams[1] = fold(gram_of(complete(0)))

    @pl.when(core == 0)
    def _():
        swap.start()

    pair = complete(1)
    for chunk in range(2, chunks):
        pair = pair + complete(chunk)
    grams[0] = fold(gram_of(pair))

    @pl.when(core == 1)
    def _():
        swap.start()

    swap.wait_recv()
    whole = grams[core] + gram_recv[...]
    row_send[...] = whole
    for step in range(1, 2 * n_group):
        each = copy(
            row_send, row_recv.at[step - 1], y_s, y_r, owner(step)
        )
        each.start()
    all_peaks.wait_recv()
    peaks = jnp.maximum(peaks, jnp.max(peak_recv[...], axis=0))
    peak2_send[...] = peaks
    for step in range(1, n_mp):
        each = copy(
            peak2_send, peak2_recv.at[step - 1], pm_s, pm_r,
            (dp, lax.rem(mp + step, n_mp)),
        )
        each.start()

    all_rows.wait_recv()
    whole = unfold(whole + jnp.sum(row_recv[...], axis=0))

    eye = (
        lax.broadcasted_iota(jnp.int32, (width, width), 0)
        == lax.broadcasted_iota(jnp.int32, (width, width), 1)
    ).astype(F32)
    trace = jnp.sum(jnp.sum(whole * eye, axis=0, keepdims=True), axis=1, keepdims=True)
    scale = 1.0 / jnp.sqrt(trace + 1.0)
    current = whole * (scale * scale)
    mixed = None
    swap2 = [
        copy(ref.at[core], ref.at[core], m_s, m_r.at[i], (dp, other_core))
        for i, ref in enumerate((mix, final))
    ]
    for step in range(ITERS):
        parts = split(current)
        square = mm_deep(parts, parts)
        poly = COEFF_A * eye + COEFF_B * current + COEFF_C * square
        if step + 1 == ITERS:
            break
        pair = split(poly)
        mixed = poly * scale if mixed is None else mm_deep(split(mixed), pair)
        if step + 2 == ITERS:
            mix[core] = mixed
            swap2[0].start()
        current = mm_deep(split(mm_deep(pair, parts)), pair)
    final[core] = poly
    swap2[1].start()
    all_peaks2.wait_recv()
    peaks = jnp.maximum(peaks, jnp.max(peak2_recv[...], axis=0))
    mine = jnp.where(lane == lax.rem(dp, heads), peaks, LOWEST)
    peak = jnp.max(jnp.max(mine, axis=0, keepdims=True), axis=1, keepdims=True)
    shrink = jnp.sqrt(CLIP_LEVEL / jnp.maximum(peak, CLIP_LEVEL))
    keep = 1.0 - STEP_SIZE * DECAY
    shrink_out[...] = jnp.broadcast_to(shrink, shrink_out.shape)
    qw_out[0] = (state[0, k_rows:] * keep) * shrink
    kw_out[0] = (state[0, :k_rows] * keep) * shrink
    swap2[0].wait_recv()
    for which, (moment, part_out) in enumerate(((qm_out, qy_out), (km_out, ky_out))):
        part_out[0] = mm3(split(moment[0]), split(mix[which]))
    swap2[1].wait_recv()
    sent = sum(len(span) for span in spans)
    passed = sent - len(spans[last]) + (2 * (chunks - kept) if line else 0)
    for count, ref, sem in ((sent, near_send, ns_s), (passed, own, fs_s)):
        part = ref.at[pl.ds(0, count)]
        copy(part, part, sem, sem, (dp, other_core)).wait_send()
    copy(mix, mix, m_s, m_s, (dp, other_core)).wait_send()
    for each in (all_peaks, all_peaks2, swap, all_rows):
        each.wait_send()


def finish(
    n_mp, qw_ref, kw_ref, qm_ref, km_ref, qy_ref, ky_ref, final_ref, shrink_ref,
    qw_out, kw_out, qm_out, km_out, qw_new, kw_new, sems,
):
    stores = [
        pltpu.make_async_copy(src, dst, sems.at[i])
        for i, (src, dst) in enumerate((
            (qm_ref, qm_out), (km_ref, km_out), (kw_new, kw_out), (qw_new, qw_out),
        ))
    ]
    stores[0].start()
    stores[1].start()
    groups = ((1, kw_ref, ky_ref, kw_new, stores[2]), (0, qw_ref, qy_ref, qw_new, stores[3]))
    for which, weight, part, weight_new, store in groups:
        size = STEP_SIZE * 0.2 * math.sqrt(2 * n_mp * part.shape[1])
        ortho = mm3(split(part[0]), split(final_ref[which]))
        weight_new[0] = weight[0] - (size * ortho) * shrink_ref[...]
        store.start()
    for each in stores:
        each.wait()


def local(
    q_latent, kv_latent, q_head_grad, k_head_grad, q_heads, k_heads,
    query_pick, key_pick, q_weight, k_weight, q_moment, k_moment,
):
    n_dp = lax.axis_size("dp")
    n_mp = lax.axis_size("mp")
    heads = n_dp // 2
    n_outer = n_dp // 2
    n_group = n_mp // 2
    rows = q_latent.shape[2] + kv_latent.shape[2]
    width = q_moment.shape[2]
    operands = (
        q_latent.transpose(1, 2, 0), kv_latent.transpose(1, 2, 0), q_head_grad, k_head_grad,
        q_heads, k_heads, query_pick.transpose(2, 0, 1), key_pick.transpose(2, 0, 1),
        q_weight, k_weight, q_moment, k_moment,
    )
    vmem = pltpu.VMEM
    dma = pltpu.SemaphoreType.DMA
    square = (width, width)
    folded = (width // 2 + 1, width)
    tile = (1, width)
    tokens = q_latent.shape[0]
    k_rows = k_moment.shape[1]
    chunks = rows // k_rows

    def blocks(count):
        return vmem((count, k_rows, width), F32)

    shapes = [a.shape for a in (q_weight, k_weight, q_moment, k_moment)]
    parts = pl.pallas_call(
        functools.partial(kernel, n_dp, n_mp, heads),
        out_shape=[vmem(shape, F32) for shape in shapes + shapes[2:] + [(2,) + square, tile]],
        in_specs=[pl.BlockSpec(memory_space=pl.ANY)] * 12,
        out_specs=[pl.BlockSpec(memory_space=vmem)] * 8,
        scratch_shapes=[
            vmem((2, rows, tokens), BF16),
            vmem((2,) + q_head_grad.shape, BF16),
            vmem((2,) + q_heads.shape, BF16),
            vmem((2,) + operands[6].shape, jnp.int32),
            vmem((2, rows, width), F32),
            dma((5,)),
            blocks(n_outer * chunks), blocks(n_outer * chunks),
            blocks(n_outer * chunks), blocks(n_outer * chunks),
            vmem((2, chunks - chunks // 2, k_rows, width), F32),
            vmem(tile, F32),
            vmem((n_dp - 1,) + tile, F32),
            vmem(tile, F32),
            vmem((n_mp - 1,) + tile, F32),
            vmem((2,) + folded, F32),
            vmem(folded, F32),
            vmem(folded, F32),
            vmem((2 * n_group - 1,) + folded, F32),
            vmem((2,) + square, F32),
            dma, dma((n_outer * chunks,)),
            dma, dma((n_outer * chunks,)),
            dma((2,)),
            dma, dma, dma, dma, dma, dma, dma, dma,
            dma, dma((2,)),
        ],
        compiler_params=pltpu.CompilerParams(
            collective_id=0, has_side_effects=True, vmem_limit_bytes=56 * 1024 * 1024
        ),
    )(*operands)
    return pl.pallas_call(
        functools.partial(finish, n_mp),
        out_shape=[jax.ShapeDtypeStruct(shape, F32) for shape in shapes],
        in_specs=[pl.BlockSpec(memory_space=vmem)] * 8,
        out_specs=[pl.BlockSpec(memory_space=pl.ANY)] * 4,
        scratch_shapes=[vmem(shape, F32) for shape in shapes[:2]] + [dma((4,))],
    )(*[pltpu.with_memory_space_constraint(part, vmem) for part in parts])


def solution(mesh):
    rows3 = P("dp", "mp", None)
    in_specs = (
        P("dp", None, "mp"), P("dp", None, "mp"), P("dp", None), P("dp", None),
        P("dp", "mp"), P("dp", "mp"), P("dp", None, "mp"), P("dp", None, "mp"),
        rows3, rows3, rows3, rows3,
    )
    return jax.shard_map(
        lambda *args: tuple(local(*args)),
        mesh=mesh, in_specs=in_specs, out_specs=(rows3,) * 4, check_vma=False,
    )
```

```python
import functools
import math

import jax
import jax.numpy as jnp
from jax import lax
from jax.experimental import pallas as pl
from jax.experimental.pallas import tpu as pltpu
from jax.sharding import PartitionSpec as P

ITERS = 5
MOMENTUM = 0.95
STEP_SIZE = 1.0
DECAY = 0.1
CLIP_LEVEL = 0.1
SCORE_SCALE = 1.0 / math.sqrt(192.0)
COEFF_A = 3.4445
COEFF_B = -4.775
COEFF_C = 2.0315
LOWEST = -1e30
MESH = pl.DeviceIdType.MESH
F32 = jnp.float32
BF16 = jnp.bfloat16


def split(value):
    high = value.astype(BF16)
    return high, (value - high.astype(F32)).astype(BF16)


def mm(a, b):
    return jnp.dot(a, b, preferred_element_type=F32)


def mm3(a, b):
    both = mm(a[0], jnp.concatenate([b[0], b[1]], axis=1))
    width = b[0].shape[1]
    return both[:, :width] + (both[:, width:] + mm(a[1], b[0]))


def mm_deep(a, b):
    return mm(
        jnp.concatenate([a[0], a[1], a[0]], axis=1), jnp.concatenate([b[0], b[0], b[1]], axis=0)
    )


def gram_pair(rows):
    high, low = split(rows)
    return mm(high.T, jnp.concatenate([high, low], axis=1))


def gram_of(pair):
    width = pair.shape[0]
    cross = pair[:, width:]
    return pair[:, :width] + (cross + cross.T)


def fold(matrix):
    width = matrix.shape[0]
    half = width // 2
    row = lax.broadcasted_iota(jnp.int32, (half, width), 0)
    lane = lax.broadcasted_iota(jnp.int32, (half, width), 1)
    lower = matrix[half:]
    body = jnp.where(lane >= row, matrix[:half], pltpu.roll(lower, half, 1))
    ends = jnp.sum(jnp.where(lane == row + half, lower, 0.0), axis=0, keepdims=True)
    return jnp.concatenate([body, ends], axis=0)


def unfold(message):
    width = message.shape[1]
    half = width // 2
    row = lax.broadcasted_iota(jnp.int32, (half, width), 0)
    lane = lax.broadcasted_iota(jnp.int32, (half, width), 1)
    body = message[:half]
    ends = jnp.broadcast_to(message[half : half + 1], (half, width))
    top = jnp.where(lane >= row, body, 0.0)
    strict = jnp.where((lane >= half) & (lane - half < row), pltpu.roll(body, half, 1), 0.0)
    one_side = jnp.concatenate([top, jnp.where(lane == row + half, ends, strict)], axis=0)
    full_row = lax.broadcasted_iota(jnp.int32, (width, width), 0)
    full_lane = lax.broadcasted_iota(jnp.int32, (width, width), 1)
    return one_side + jnp.where(full_row == full_lane, 0.0, one_side.T)


def spread_down(row):
    count = row.shape[1]
    spread = jnp.broadcast_to(row, (count, count))
    same = lax.broadcasted_iota(jnp.int32, (count, count), 0) == lax.broadcasted_iota(
        jnp.int32, (count, count), 1
    )
    picked = jnp.where(same, spread, 0).astype(F32)
    return jnp.sum(picked, axis=1, keepdims=True).astype(jnp.int32)


def partner(index, count, step):
    if count & (count - 1):
        return lax.rem(index + step, count)
    result = 0
    bit = 1
    while bit < count:
        held = lax.rem(lax.div(index, bit), 2)
        result = result + bit * ((1 - held) if step & bit else held)
        bit *= 2
    return result


def kernel(
    n_dp, n_mp, heads,
    ql_in, kl_in, qg_in, kg_in, qh_in, kh_in, qp_in, kp_in, qw_in, kw_in, qm_in, km_in,
    qw_out, kw_out, qm_out, km_out, qy_out, ky_out, final, shrink_out,
    latents, grads, act, picks, state, in_sems,
    near_send, near_recv, own, relay_recv, raw_recv, fin, base, back_send, back_recv, peak_send, peak_recv, peak2_send, peak2_recv,
    row_send, row_recv, mix,
    ns_s, ns_r, fs_s, fin_r, rl_r, rw_r, b_s, b_r, bk_s, bk_r, pk_s, pk_r, pm_s, pm_r, y_s, y_r, m_s, m_r,
):
    dp = lax.axis_index("dp")
    mp = lax.axis_index("mp")
    n_outer = n_dp // 2
    outer = lax.div(dp, 2)
    inner = lax.rem(dp, 2)
    core = lax.rem(mp, 2)
    group = lax.div(mp, 2)
    n_group = n_mp // 2
    q_rows = qm_in.shape[1]
    k_rows = km_in.shape[1]
    width = qm_in.shape[2]
    tokens = qg_in.shape[0]
    tall = q_rows + k_rows
    top_rows = pl.ds(0, k_rows)
    low_rows = pl.ds(k_rows, q_rows)
    other_core = mp + 1 - 2 * core

    loads = (
        ((kl_in, latents.at[:, top_rows]), (ql_in, latents.at[:, low_rows])),
        ((kg_in, grads.at[1]), (qg_in, grads.at[0])),
        ((qp_in, picks.at[0]), (kp_in, picks.at[1])),
        ((qh_in, act.at[0]), (kh_in, act.at[1])),
        (
            (km_in.at[0], state.at[1, top_rows]), (qm_in.at[0], state.at[1, low_rows]),
            (kw_in.at[0], state.at[0, top_rows]), (qw_in.at[0], state.at[0, low_rows]),
        ),
    )
    for i, group_of in enumerate(loads):
        for src, dst in group_of:
            pltpu.make_async_copy(src, dst, in_sems.at[i]).start()

    def loaded(*which):
        for i in which:
            ref = (latents, grads, picks, act, state)[i]
            pltpu.make_async_copy(ref, ref, in_sems.at[i]).wait()

    barrier = pltpu.get_barrier_semaphore()
    for step in range(1, n_dp):
        for column in (mp, other_core):
            pl.semaphore_signal(
                barrier, inc=1, device_id=(lax.rem(dp + step, n_dp), column), device_id_type=MESH
            )
    def owner(step):
        across = lax.rem(dp + (step // n_group) * heads, n_dp)
        return across, 2 * lax.rem(group + step, n_group) + core

    for step in range(n_group + 1, 2 * n_group):
        pl.semaphore_signal(barrier, inc=1, device_id=owner(step), device_id_type=MESH)
    for step in range(1, n_mp):
        pl.semaphore_signal(
            barrier, inc=1, device_id=(dp, lax.rem(mp + step, n_mp)), device_id_type=MESH
        )

    def copy(src, dst, send, recv, where):
        return pltpu.make_async_remote_copy(
            src_ref=src, dst_ref=dst, send_sem=send, recv_sem=recv,
            device_id=where, device_id_type=MESH,
        )

    all_peaks = copy(peak_recv, peak_recv, pk_s, pk_r, (dp, other_core))
    all_peaks2 = copy(peak2_recv, peak2_recv, pm_s, pm_r, (dp, other_core))
    all_rows = copy(row_recv, row_recv, y_s, y_r, (dp, other_core))

    def term(dst, spot, to_outer, to_inner):
        slot = 2 * to_outer + to_inner
        half = lax.div(slot, heads)
        cols = pl.ds(pl.multiple_of(lax.rem(slot, heads) * width, width), width)
        first = spot * chunks
        dst[first] = mm(latents[half, :k_rows], grads[1, :, cols])
        rest = mm(latents[half, k_rows:], grads[0, :, cols])
        dst[first + 1 : first + chunks] = rest.reshape(chunks - 1, step_rows, width)

    step_rows = k_rows
    chunks = tall // step_rows
    loaded(0, 1)
    entered = 2 * (n_dp - 1) + (n_mp - 1) + (n_group - 1)
    across_x = dp + 1 - 2 * inner
    neighbour = (across_x, mp)
    partner_core = (dp, other_core)
    last = n_outer - 1
    line = n_outer == 4
    inside = lax.rem(lax.div(outer, 2) + lax.rem(outer, 2), 2)
    by = [partner(outer, n_outer, step) for step in range(n_outer)]

    def at(spot, chunk):
        return spot * chunks + chunk

    if line:
        split_to = by[2] + inside * (by[1] - by[2])
        whole_to = by[1] + inside * (by[2] - by[1])
        order = [by[3], split_to, whole_to, by[0]]
        kept = chunks // 2
        spans = [range(chunks), range(kept), range(chunks), range(chunks)]
    else:
        order = by[::-1]
        spans = [range(chunks)] * n_outer

    def near_copy(spot, chunk):
        where = at(spot, chunk)
        return copy(near_send.at[where], near_recv.at[where], ns_s, ns_r.at[where], neighbour)

    def home(chunk):
        return 2 * group + (1 if chunk else 0)

    def final_copy(source, spot, slot, chunk, sent, to):
        return copy(
            source.at[at(spot, chunk)], fin.at[slot, chunk, core], sent, fin_r.at[slot, chunk],
            (to, home(chunk)),
        )

    def far_copy(spot, chunk, target):
        return final_copy(own, spot, spot, chunk, fs_s, 2 * target + inner)

    def send_last(which):
        for chunk in which:
            final_copy(near_send, last, last, chunk, ns_s, across_x).start()

    def relay_copy(chunk):
        return copy(
            own.at[at(0, chunk)], relay_recv.at[chunk], fs_s, rl_r.at[chunk],
            (2 * by[1] + inner, mp),
        )

    def raw_copy():
        return copy(
            near_send.at[pl.ds(at(1, kept), chunks - kept)], raw_recv, fs_s, rw_r,
            (2 * split_to + inner, mp),
        )

    def send_near(spot, which):
        for chunk in which:
            near_copy(spot, chunk).start()

    term(near_send, 0, order[0], 1 - inner)
    pl.semaphore_wait(barrier, entered)
    send_near(0, spans[0])
    if line:
        term(near_send, 1, order[1], 1 - inner)
        raw_copy().start()
        term(own, 1, order[1], inner)
        for chunk in range(kept, chunks):
            far_copy(1, chunk, split_to).start()
        term(near_send, 2, order[2], 1 - inner)

        @pl.when(inside == 1)
        def _():
            send_near(2, spans[2])
            send_near(1, spans[1])

        @pl.when(inside == 0)
        def _():
            send_near(1, spans[1])
            send_near(2, spans[2])

    loaded(2, 3)
    local_heads = picks.shape[1]
    lane = lax.broadcasted_iota(jnp.int32, (1, width), 1)
    peaks = jnp.full((1, width), LOWEST, F32)
    ids = lax.broadcasted_iota(jnp.int32, (picks.shape[3], tokens), 1)
    for head in range(local_heads):
        span = slice(head * width, (head + 1) * width)
        pick_q = (ids == spread_down(picks[0, head])).astype(F32).astype(BF16)
        pick_k = (ids == spread_down(picks[1, head])).astype(F32).astype(BF16)
        score = jnp.sum(
            mm(pick_q, act[0, :, span]) * mm(pick_k, act[1, :, span]), axis=1, keepdims=True
        )
        top = jnp.max(score * SCORE_SCALE, axis=0, keepdims=True)
        peaks = jnp.where(lane == mp * local_heads + head, top, peaks)
    peak_send[...] = peaks
    for step in range(1, n_dp):
        each = copy(
            peak_send, peak_recv.at[step - 1], pk_s, pk_r,
            (lax.rem(dp + step, n_dp), mp),
        )
        each.start()

    if line:
        term(near_send, last, order[last], 1 - inner)
        send_last(range(kept))
    else:
        for spot in range(1, n_outer):
            term(near_send, spot, order[spot], 1 - inner)
            if spot < last:
                send_near(spot, spans[spot])
        send_last(range(chunks))
    for spot in range(n_outer):
        if not (line and spot == 1):
            term(own, spot, order[spot], inner)

    loaded(4)
    for chunk in range(chunks):
        moment = state[1, chunk * step_rows : (chunk + 1) * step_rows]
        own[at(last, chunk)] = MOMENTUM * moment + own[at(last, chunk)]

    def on_core(which):
        return pl.when(core == which)

    def shares(which):
        return pl.ds(0, 1) if which else pl.ds(1, chunks - 1)

    def base_copy(which):
        rows = shares(which)
        source = own.at[pl.ds(at(last, rows.start), rows.size)]
        return copy(source, base.at[rows], b_s, b_r, partner_core)

    def back_copy(which):
        rows = pl.ds(0, shares(1 - which).size)
        return copy(back_send.at[rows], back_recv.at[rows], bk_s, bk_r, partner_core)

    for which in range(2):

        @on_core(which)
        def _():
            base_copy(which).start()

    def meet(spot, chunk):
        near_copy(spot, chunk).wait_recv()
        where = at(spot, chunk)
        own[where] = own[where] + near_recv[where]

    def arrived(slot, chunk):
        ref = fin.at[slot, chunk]
        copy(ref, ref, fs_s, fin_r.at[slot, chunk], partner_core).wait_recv()
        return fin[slot, chunk]

    def pass_on(spot):
        for chunk in spans[spot]:
            meet(spot, chunk)
            far_copy(spot, chunk, order[spot]).start()

    if line:
        for chunk in spans[0]:
            meet(0, chunk)

            @pl.when(inside == 1)
            def _():
                far_copy(0, chunk, by[3]).start()

            @pl.when(inside == 0)
            def _():
                relay_copy(chunk).start()

        raw_copy().wait_recv()
        low = pl.ds(at(last, kept), chunks - kept)
        near_send[low] = near_send[low] + raw_recv[...]
        send_last(range(kept, chunks))

        @pl.when(inside == 1)
        def _():
            for chunk in spans[2]:
                relay_copy(chunk).wait_recv()
                own[at(2, chunk)] = own[at(2, chunk)] + relay_recv[chunk]
                meet(2, chunk)
                far_copy(2, chunk, whole_to).start()
            pass_on(1)

        @pl.when(inside == 0)
        def _():
            pass_on(1)
            pass_on(2)

    else:
        for spot in range(last):
            pass_on(spot)

    def complete(which, chunk):
        added = [arrived(slot, chunk) for slot in ((1, 2, last) if line else range(n_outer))]
        mine = own[at(last, chunk)]
        other = base[chunk]
        for each in added:
            mine = mine + each[which]
            other = other + each[1 - which]
        if which:
            qm_out[0, (chunk - 1) * step_rows : chunk * step_rows] = mine
            back_send[chunk - 1] = other
        else:
            km_out[0] = mine
            back_send[chunk] = other
        return gram_pair(jnp.concatenate([mine, other], axis=0))

    for which, members in enumerate((range(1), range(1, chunks))):

        @on_core(which)
        def _():
            base_copy(1 - which).wait_recv()
            if line:

                @pl.when(inside == 1)
                def _():
                    for chunk in members:
                        early = arrived(0, chunk)
                        own[at(last, chunk)] = own[at(last, chunk)] + early[which]
                        base[chunk] = base[chunk] + early[1 - which]

            pair = complete(which, members[0])
            for chunk in members[1:]:
                pair = pair + complete(which, chunk)
            row_send[...] = fold(gram_of(pair))

    for step in range(1, 2 * n_group):
        each = copy(
            row_send, row_recv.at[step - 1], y_s, y_r, owner(step)
        )
        each.start()
    for which in range(2):

        @on_core(which)
        def _():
            back_copy(which).start()

    all_peaks.wait_recv()
    peaks = jnp.maximum(peaks, jnp.max(peak_recv[...], axis=0))
    peak2_send[...] = peaks
    for step in range(1, n_mp):
        each = copy(
            peak2_send, peak2_recv.at[step - 1], pm_s, pm_r,
            (dp, lax.rem(mp + step, n_mp)),
        )
        each.start()

    @on_core(0)
    def _():
        back_copy(1).wait_recv()
        qm_out[0] = back_recv[...].reshape(q_rows, width)

    @on_core(1)
    def _():
        back_copy(0).wait_recv()
        km_out[0] = back_recv[0]

    all_rows.wait_recv()
    whole = unfold(row_send[...] + jnp.sum(row_recv[...], axis=0))

    eye = (
        lax.broadcasted_iota(jnp.int32, (width, width), 0)
        == lax.broadcasted_iota(jnp.int32, (width, width), 1)
    ).astype(F32)
    trace = jnp.sum(jnp.sum(whole * eye, axis=0, keepdims=True), axis=1, keepdims=True)
    scale = 1.0 / jnp.sqrt(trace + 1.0)
    current = whole * (scale * scale)
    mixed = None
    swap2 = [
        copy(ref.at[1 - core], ref.at[1 - core], m_s, m_r.at[i], (dp, other_core))
        for i, ref in enumerate((mix, final))
    ]
    for step in range(ITERS):
        parts = split(current)
        square = mm_deep(parts, parts)
        poly = COEFF_A * eye + COEFF_B * current + COEFF_C * square
        if step + 1 == ITERS:
            break
        pair = split(poly)
        mixed = poly * scale if mixed is None else mm_deep(split(mixed), pair)
        if step + 2 == ITERS:
            mix[1 - core] = mixed
            swap2[0].start()
        current = mm_deep(split(mm_deep(pair, parts)), pair)
    final[1 - core] = poly
    swap2[1].start()
    all_peaks2.wait_recv()
    peaks = jnp.maximum(peaks, jnp.max(peak2_recv[...], axis=0))
    mine = jnp.where(lane == lax.rem(dp, heads), peaks, LOWEST)
    peak = jnp.max(jnp.max(mine, axis=0, keepdims=True), axis=1, keepdims=True)
    shrink = jnp.sqrt(CLIP_LEVEL / jnp.maximum(peak, CLIP_LEVEL))
    keep = 1.0 - STEP_SIZE * DECAY
    shrink_out[...] = jnp.broadcast_to(shrink, shrink_out.shape)
    qw_out[0] = (state[0, k_rows:] * keep) * shrink
    kw_out[0] = (state[0, :k_rows] * keep) * shrink
    swap2[0].wait_recv()
    for which, (moment, part_out) in enumerate(((qm_out, qy_out), (km_out, ky_out))):
        part_out[0] = mm3(split(moment[0]), split(mix[which]))
    swap2[1].wait_recv()
    sent = sum(len(span) for span in spans)
    passed = sent - len(spans[last]) + (2 * (chunks - kept) if line else 0)
    for count, ref, sem in ((sent, near_send, ns_s), (passed, own, fs_s)):
        part = ref.at[pl.ds(0, count)]
        copy(part, part, sem, sem, (dp, other_core)).wait_send()
    copy(mix, mix, m_s, m_s, (dp, other_core)).wait_send()
    for each in (all_peaks, all_peaks2, all_rows):
        each.wait_send()
    for which in range(2):

        @on_core(which)
        def _():
            base_copy(which).wait_send()
            back_copy(which).wait_send()


def finish(
    n_mp, qw_ref, kw_ref, qm_ref, km_ref, qy_ref, ky_ref, final_ref, shrink_ref,
    qw_out, kw_out, qm_out, km_out, qw_new, kw_new, sems,
):
    stores = [
        pltpu.make_async_copy(src, dst, sems.at[i])
        for i, (src, dst) in enumerate((
            (qm_ref, qm_out), (km_ref, km_out), (kw_new, kw_out), (qw_new, qw_out),
        ))
    ]
    stores[0].start()
    stores[1].start()
    groups = ((1, kw_ref, ky_ref, kw_new, stores[2]), (0, qw_ref, qy_ref, qw_new, stores[3]))
    for which, weight, part, weight_new, store in groups:
        size = STEP_SIZE * 0.2 * math.sqrt(2 * n_mp * part.shape[1])
        ortho = mm3(split(part[0]), split(final_ref[which]))
        weight_new[0] = weight[0] - (size * ortho) * shrink_ref[...]
        store.start()
    for each in stores:
        each.wait()


def local(
    q_latent, kv_latent, q_head_grad, k_head_grad, q_heads, k_heads,
    query_pick, key_pick, q_weight, k_weight, q_moment, k_moment,
):
    n_dp = lax.axis_size("dp")
    n_mp = lax.axis_size("mp")
    heads = n_dp // 2
    n_outer = n_dp // 2
    n_group = n_mp // 2
    rows = q_latent.shape[2] + kv_latent.shape[2]
    width = q_moment.shape[2]
    operands = (
        q_latent.transpose(1, 2, 0), kv_latent.transpose(1, 2, 0), q_head_grad, k_head_grad,
        q_heads, k_heads, query_pick.transpose(2, 0, 1), key_pick.transpose(2, 0, 1),
        q_weight, k_weight, q_moment, k_moment,
    )
    vmem = pltpu.VMEM
    dma = pltpu.SemaphoreType.DMA
    square = (width, width)
    folded = (width // 2 + 1, width)
    tile = (1, width)
    tokens = q_latent.shape[0]
    k_rows = k_moment.shape[1]
    chunks = rows // k_rows

    def blocks(count):
        return vmem((count, k_rows, width), F32)

    shapes = [a.shape for a in (q_weight, k_weight, q_moment, k_moment)]
    parts = pl.pallas_call(
        functools.partial(kernel, n_dp, n_mp, heads),
        out_shape=[vmem(shape, F32) for shape in shapes + shapes[2:] + [(2,) + square, tile]],
        in_specs=[pl.BlockSpec(memory_space=pl.ANY)] * 12,
        out_specs=[pl.BlockSpec(memory_space=vmem)] * 8,
        scratch_shapes=[
            vmem((2, rows, tokens), BF16),
            vmem((2,) + q_head_grad.shape, BF16),
            vmem((2,) + q_heads.shape, BF16),
            vmem((2,) + operands[6].shape, jnp.int32),
            vmem((2, rows, width), F32),
            dma((5,)),
            blocks(n_outer * chunks), blocks((n_outer - 1) * chunks), blocks(n_outer * chunks),
            blocks(chunks), blocks(chunks - chunks // 2),
            vmem((n_outer, chunks, 2, k_rows, width), F32),
            blocks(chunks), blocks(chunks - 1), blocks(chunks - 1),
            vmem(tile, F32),
            vmem((n_dp - 1,) + tile, F32),
            vmem(tile, F32),
            vmem((n_mp - 1,) + tile, F32),
            vmem(folded, F32),
            vmem((2 * n_group - 1,) + folded, F32),
            vmem((2,) + square, F32),
            dma, dma(((n_outer - 1) * chunks,)),
            dma, dma((n_outer, chunks)), dma((chunks,)), dma,
            dma, dma, dma, dma, dma, dma, dma, dma, dma, dma,
            dma, dma((2,)),
        ],
        compiler_params=pltpu.CompilerParams(
            collective_id=0, has_side_effects=True, vmem_limit_bytes=56 * 1024 * 1024
        ),
    )(*operands)
    return pl.pallas_call(
        functools.partial(finish, n_mp),
        out_shape=[jax.ShapeDtypeStruct(shape, F32) for shape in shapes],
        in_specs=[pl.BlockSpec(memory_space=vmem)] * 8,
        out_specs=[pl.BlockSpec(memory_space=pl.ANY)] * 4,
        scratch_shapes=[vmem(shape, F32) for shape in shapes[:2]] + [dma((4,))],
    )(*[pltpu.with_memory_space_constraint(part, vmem) for part in parts])


def solution(mesh):
    rows3 = P("dp", "mp", None)
    in_specs = (
        P("dp", None, "mp"), P("dp", None, "mp"), P("dp", None), P("dp", None),
        P("dp", "mp"), P("dp", "mp"), P("dp", None, "mp"), P("dp", None, "mp"),
        rows3, rows3, rows3, rows3,
    )
    return jax.shard_map(
        lambda *args: tuple(local(*args)),
        mesh=mesh, in_specs=in_specs, out_specs=(rows3,) * 4, check_vma=False,
    )
```

```python
import functools
import math

import jax
import jax.numpy as jnp
from jax import lax
from jax.experimental import pallas as pl
from jax.experimental.pallas import tpu as pltpu
from jax.sharding import PartitionSpec as P

ITERS = 5
MOMENTUM = 0.95
STEP_SIZE = 1.0
DECAY = 0.1
CLIP_LEVEL = 0.1
SCORE_SCALE = 1.0 / math.sqrt(192.0)
COEFF_A = 3.4445
COEFF_B = -4.775
COEFF_C = 2.0315
LOWEST = -1e30
MESH = pl.DeviceIdType.MESH
F32 = jnp.float32
BF16 = jnp.bfloat16


def split(value):
    high = value.astype(BF16)
    return high, (value - high.astype(F32)).astype(BF16)


def mm(a, b):
    return jnp.dot(a, b, preferred_element_type=F32)


def mm3(a, b):
    both = mm(a[0], jnp.concatenate([b[0], b[1]], axis=1))
    width = b[0].shape[1]
    return both[:, :width] + (both[:, width:] + mm(a[1], b[0]))


def mm_deep(a, b):
    return mm(
        jnp.concatenate([a[0], a[1], a[0]], axis=1), jnp.concatenate([b[0], b[0], b[1]], axis=0)
    )


def gram_pair(rows):
    high, low = split(rows)
    return mm(high.T, jnp.concatenate([high, low], axis=1))


def gram_of(pair):
    width = pair.shape[0]
    cross = pair[:, width:]
    return pair[:, :width] + (cross + cross.T)


def fold(matrix):
    width = matrix.shape[0]
    half = width // 2
    row = lax.broadcasted_iota(jnp.int32, (half, width), 0)
    lane = lax.broadcasted_iota(jnp.int32, (half, width), 1)
    lower = matrix[half:]
    body = jnp.where(lane >= row, matrix[:half], pltpu.roll(lower, half, 1))
    ends = jnp.sum(jnp.where(lane == row + half, lower, 0.0), axis=0, keepdims=True)
    return jnp.concatenate([body, ends], axis=0)


def unfold(message):
    width = message.shape[1]
    half = width // 2
    row = lax.broadcasted_iota(jnp.int32, (half, width), 0)
    lane = lax.broadcasted_iota(jnp.int32, (half, width), 1)
    body = message[:half]
    ends = jnp.broadcast_to(message[half : half + 1], (half, width))
    top = jnp.where(lane >= row, body, 0.0)
    strict = jnp.where((lane >= half) & (lane - half < row), pltpu.roll(body, half, 1), 0.0)
    one_side = jnp.concatenate([top, jnp.where(lane == row + half, ends, strict)], axis=0)
    full_row = lax.broadcasted_iota(jnp.int32, (width, width), 0)
    full_lane = lax.broadcasted_iota(jnp.int32, (width, width), 1)
    return one_side + jnp.where(full_row == full_lane, 0.0, one_side.T)


def spread_down(row):
    count = row.shape[1]
    spread = jnp.broadcast_to(row, (count, count))
    same = lax.broadcasted_iota(jnp.int32, (count, count), 0) == lax.broadcasted_iota(
        jnp.int32, (count, count), 1
    )
    picked = jnp.where(same, spread, 0).astype(F32)
    return jnp.sum(picked, axis=1, keepdims=True).astype(jnp.int32)


def partner(index, count, step):
    if count & (count - 1):
        return lax.rem(index + step, count)
    result = 0
    bit = 1
    while bit < count:
        held = lax.rem(lax.div(index, bit), 2)
        result = result + bit * ((1 - held) if step & bit else held)
        bit *= 2
    return result


def kernel(
    n_dp, n_mp, heads,
    ql_in, kl_in, qg_in, kg_in, qh_in, kh_in, qp_in, kp_in, qw_in, kw_in, qm_in, km_in,
    qw_out, kw_out, qm_out, km_out, qy_out, ky_out, final, shrink_out,
    latents, grads, act, picks, state, in_sems,
    near_send, near_recv, own, relay_recv, raw_recv, fin, base, back_send, back_recv, peak_send, peak_recv, peak2_send, peak2_recv,
    row_send, row_recv, mix,
    ns_s, ns_r, fs_s, fin_r, rl_r, rw_r, b_s, b_r, bk_s, bk_r, pk_s, pk_r, pm_s, pm_r, y_s, y_r, m_s, m_r,
):
    dp = lax.axis_index("dp")
    mp = lax.axis_index("mp")
    n_outer = n_dp // 2
    outer = lax.div(dp, 2)
    inner = lax.rem(dp, 2)
    core = lax.rem(mp, 2)
    group = lax.div(mp, 2)
    n_group = n_mp // 2
    q_rows = qm_in.shape[1]
    k_rows = km_in.shape[1]
    width = qm_in.shape[2]
    tokens = qg_in.shape[0]
    tall = q_rows + k_rows
    top_rows = pl.ds(0, k_rows)
    low_rows = pl.ds(k_rows, q_rows)
    other_core = mp + 1 - 2 * core

    loads = (
        ((kl_in, latents.at[:, top_rows]), (ql_in, latents.at[:, low_rows])),
        ((kg_in, grads.at[1]), (qg_in, grads.at[0])),
        ((qp_in, picks.at[0]), (kp_in, picks.at[1])),
        ((qh_in, act.at[0]), (kh_in, act.at[1])),
        (
            (km_in.at[0], state.at[1, top_rows]), (qm_in.at[0], state.at[1, low_rows]),
            (kw_in.at[0], state.at[0, top_rows]), (qw_in.at[0], state.at[0, low_rows]),
        ),
    )
    for i, group_of in enumerate(loads):
        for src, dst in group_of:
            pltpu.make_async_copy(src, dst, in_sems.at[i]).start()

    def loaded(*which):
        for i in which:
            ref = (latents, grads, picks, act, state)[i]
            pltpu.make_async_copy(ref, ref, in_sems.at[i]).wait()

    barrier = pltpu.get_barrier_semaphore()
    for step in range(1, n_dp):
        for column in (mp, other_core):
            pl.semaphore_signal(
                barrier, inc=1, device_id=(lax.rem(dp + step, n_dp), column), device_id_type=MESH
            )
    def owner(step):
        across = lax.rem(dp + (step // n_group) * heads, n_dp)
        return across, 2 * lax.rem(group + step, n_group) + core

    for step in range(n_group + 1, 2 * n_group):
        pl.semaphore_signal(barrier, inc=1, device_id=owner(step), device_id_type=MESH)
    for step in range(1, n_mp):
        pl.semaphore_signal(
            barrier, inc=1, device_id=(dp, lax.rem(mp + step, n_mp)), device_id_type=MESH
        )

    def copy(src, dst, send, recv, where):
        return pltpu.make_async_remote_copy(
            src_ref=src, dst_ref=dst, send_sem=send, recv_sem=recv,
            device_id=where, device_id_type=MESH,
        )

    all_peaks = copy(peak_recv, peak_recv, pk_s, pk_r, (dp, other_core))
    all_peaks2 = copy(peak2_recv, peak2_recv, pm_s, pm_r, (dp, other_core))
    all_rows = copy(row_recv, row_recv, y_s, y_r, (dp, other_core))

    def term(dst, spot, to_outer, to_inner):
        slot = 2 * to_outer + to_inner
        half = lax.div(slot, heads)
        cols = pl.ds(pl.multiple_of(lax.rem(slot, heads) * width, width), width)
        first = spot * chunks
        dst[first] = mm(latents[half, :k_rows], grads[1, :, cols])
        rest = mm(latents[half, k_rows:], grads[0, :, cols])
        dst[first + 1 : first + chunks] = rest.reshape(chunks - 1, step_rows, width)

    step_rows = k_rows
    chunks = tall // step_rows
    loaded(0, 1)
    entered = 2 * (n_dp - 1) + (n_mp - 1) + (n_group - 1)
    across_x = dp + 1 - 2 * inner
    neighbour = (across_x, mp)
    partner_core = (dp, other_core)
    last = n_outer - 1
    line = n_outer == 4
    inside = lax.rem(lax.div(outer, 2) + lax.rem(outer, 2), 2)
    by = [partner(outer, n_outer, step) for step in range(n_outer)]

    def at(spot, chunk):
        return spot * chunks + chunk

    if line:
        split_to = by[2] + inside * (by[1] - by[2])
        whole_to = by[1] + inside * (by[2] - by[1])
        order = [by[3], split_to, whole_to, by[0]]
        kept = chunks // 2
        spans = [range(chunks), range(kept), range(chunks), range(chunks)]
    else:
        order = by[::-1]
        spans = [range(chunks)] * n_outer

    def near_copy(spot, chunk):
        where = at(spot, chunk)
        return copy(near_send.at[where], near_recv.at[where], ns_s, ns_r.at[where], neighbour)

    def home(chunk):
        return 2 * group + (1 if chunk else 0)

    def final_copy(source, spot, slot, chunk, sent, to):
        return copy(
            source.at[at(spot, chunk)], fin.at[slot, chunk, core], sent, fin_r.at[slot, chunk],
            (to, home(chunk)),
        )

    def far_copy(spot, chunk, target):
        return final_copy(own, spot, spot, chunk, fs_s, 2 * target + inner)

    def send_last(which):
        for chunk in which:
            final_copy(near_send, last, last, chunk, ns_s, across_x).start()

    def relay_copy(chunk):
        return copy(
            own.at[at(0, chunk)], relay_recv.at[chunk], fs_s, rl_r.at[chunk],
            (2 * by[1] + inner, mp),
        )

    def raw_copy():
        return copy(
            near_send.at[pl.ds(at(1, kept), chunks - kept)], raw_recv, fs_s, rw_r,
            (2 * split_to + inner, mp),
        )

    def send_near(spot, which):
        for chunk in which:
            near_copy(spot, chunk).start()

    term(near_send, 0, order[0], 1 - inner)
    pl.semaphore_wait(barrier, entered)
    send_near(0, spans[0])
    if line:
        term(near_send, 1, order[1], 1 - inner)
        raw_copy().start()
        term(own, 1, order[1], inner)
        for chunk in range(kept, chunks):
            far_copy(1, chunk, split_to).start()
        term(near_send, 2, order[2], 1 - inner)

        send_near(1, spans[1])
        send_near(2, spans[2])

    loaded(2, 3)
    local_heads = picks.shape[1]
    lane = lax.broadcasted_iota(jnp.int32, (1, width), 1)
    peaks = jnp.full((1, width), LOWEST, F32)
    ids = lax.broadcasted_iota(jnp.int32, (picks.shape[3], tokens), 1)
    for head in range(local_heads):
        span = slice(head * width, (head + 1) * width)
        pick_q = (ids == spread_down(picks[0, head])).astype(F32).astype(BF16)
        pick_k = (ids == spread_down(picks[1, head])).astype(F32).astype(BF16)
        score = jnp.sum(
            mm(pick_q, act[0, :, span]) * mm(pick_k, act[1, :, span]), axis=1, keepdims=True
        )
        top = jnp.max(score * SCORE_SCALE, axis=0, keepdims=True)
        peaks = jnp.where(lane == mp * local_heads + head, top, peaks)
    peak_send[...] = peaks
    for step in range(1, n_dp):
        each = copy(
            peak_send, peak_recv.at[step - 1], pk_s, pk_r,
            (lax.rem(dp + step, n_dp), mp),
        )
        each.start()

    if line:
        term(near_send, last, order[last], 1 - inner)
        send_last(range(kept))
    else:
        for spot in range(1, n_outer):
            term(near_send, spot, order[spot], 1 - inner)
            if spot < last:
                send_near(spot, spans[spot])
        send_last(range(chunks))
    for spot in range(n_outer):
        if not (line and spot == 1):
            term(own, spot, order[spot], inner)

    loaded(4)
    for chunk in range(chunks):
        moment = state[1, chunk * step_rows : (chunk + 1) * step_rows]
        own[at(last, chunk)] = MOMENTUM * moment + own[at(last, chunk)]

    def on_core(which):
        return pl.when(core == which)

    def shares(which):
        return pl.ds(0, 1) if which else pl.ds(1, chunks - 1)

    def base_copy(which):
        rows = shares(which)
        source = own.at[pl.ds(at(last, rows.start), rows.size)]
        return copy(source, base.at[rows], b_s, b_r, partner_core)

    def back_copy(which):
        rows = pl.ds(0, shares(1 - which).size)
        return copy(back_send.at[rows], back_recv.at[rows], bk_s, bk_r, partner_core)

    for which in range(2):

        @on_core(which)
        def _():
            base_copy(which).start()

    def meet(spot, chunk):
        near_copy(spot, chunk).wait_recv()
        where = at(spot, chunk)
        own[where] = own[where] + near_recv[where]

    def arrived(slot, chunk):
        ref = fin.at[slot, chunk]
        copy(ref, ref, fs_s, fin_r.at[slot, chunk], partner_core).wait_recv()
        return fin[slot, chunk]

    def pass_on(spot):
        for chunk in spans[spot]:
            meet(spot, chunk)
            far_copy(spot, chunk, order[spot]).start()

    if line:
        def forward(held):
            for chunk in spans[0]:
                meet(0, chunk)
                if held:
                    far_copy(0, chunk, by[3]).start()
                else:
                    relay_copy(chunk).start()
            pass_on(1)
            raw_copy().wait_recv()
            low = pl.ds(at(last, kept), chunks - kept)
            near_send[low] = near_send[low] + raw_recv[...]
            send_last(range(kept, chunks))
            for chunk in spans[2]:
                if held:
                    relay_copy(chunk).wait_recv()
                    own[at(2, chunk)] = own[at(2, chunk)] + relay_recv[chunk]
                meet(2, chunk)
                far_copy(2, chunk, whole_to).start()

        for held in range(2):

            @pl.when(inside == held)
            def _():
                forward(held)

    else:
        for spot in range(last):
            pass_on(spot)

    def complete(which, chunk):
        added = [arrived(slot, chunk) for slot in ((1, 2, last) if line else range(n_outer))]
        mine = own[at(last, chunk)]
        other = base[chunk]
        for each in added:
            mine = mine + each[which]
            other = other + each[1 - which]
        if which:
            qm_out[0, (chunk - 1) * step_rows : chunk * step_rows] = mine
            back_send[chunk - 1] = other
        else:
            km_out[0] = mine
            back_send[chunk] = other
        return gram_pair(jnp.concatenate([mine, other], axis=0))

    for which, members in enumerate((range(1), range(1, chunks))):

        @on_core(which)
        def _():
            base_copy(1 - which).wait_recv()
            if line:

                @pl.when(inside == 1)
                def _():
                    for chunk in members:
                        early = arrived(0, chunk)
                        own[at(last, chunk)] = own[at(last, chunk)] + early[which]
                        base[chunk] = base[chunk] + early[1 - which]

            pair = complete(which, members[0])
            for chunk in members[1:]:
                pair = pair + complete(which, chunk)
            row_send[...] = fold(gram_of(pair))

    for step in range(1, 2 * n_group):
        each = copy(
            row_send, row_recv.at[step - 1], y_s, y_r, owner(step)
        )
        each.start()
    for which in range(2):

        @on_core(which)
        def _():
            back_copy(which).start()

    all_peaks.wait_recv()
    peaks = jnp.maximum(peaks, jnp.max(peak_recv[...], axis=0))
    peak2_send[...] = peaks
    for step in range(1, n_mp):
        each = copy(
            peak2_send, peak2_recv.at[step - 1], pm_s, pm_r,
            (dp, lax.rem(mp + step, n_mp)),
        )
        each.start()

    @on_core(0)
    def _():
        back_copy(1).wait_recv()
        qm_out[0] = back_recv[...].reshape(q_rows, width)

    @on_core(1)
    def _():
        back_copy(0).wait_recv()
        km_out[0] = back_recv[0]

    all_rows.wait_recv()
    whole = unfold(row_send[...] + jnp.sum(row_recv[...], axis=0))

    eye = (
        lax.broadcasted_iota(jnp.int32, (width, width), 0)
        == lax.broadcasted_iota(jnp.int32, (width, width), 1)
    ).astype(F32)
    trace = jnp.sum(jnp.sum(whole * eye, axis=0, keepdims=True), axis=1, keepdims=True)
    scale = 1.0 / jnp.sqrt(trace + 1.0)
    current = whole * (scale * scale)
    mixed = None
    swap2 = [
        copy(ref.at[1 - core], ref.at[1 - core], m_s, m_r.at[i], (dp, other_core))
        for i, ref in enumerate((mix, final))
    ]
    for step in range(ITERS):
        parts = split(current)
        square = mm_deep(parts, parts)
        poly = COEFF_A * eye + COEFF_B * current + COEFF_C * square
        if step + 1 == ITERS:
            break
        pair = split(poly)
        mixed = poly * scale if mixed is None else mm_deep(split(mixed), pair)
        if step + 2 == ITERS:
            mix[1 - core] = mixed
            swap2[0].start()
        current = mm_deep(split(mm_deep(pair, parts)), pair)
    final[1 - core] = poly
    swap2[1].start()
    all_peaks2.wait_recv()
    peaks = jnp.maximum(peaks, jnp.max(peak2_recv[...], axis=0))
    mine = jnp.where(lane == lax.rem(dp, heads), peaks, LOWEST)
    peak = jnp.max(jnp.max(mine, axis=0, keepdims=True), axis=1, keepdims=True)
    shrink = jnp.sqrt(CLIP_LEVEL / jnp.maximum(peak, CLIP_LEVEL))
    keep = 1.0 - STEP_SIZE * DECAY
    shrink_out[...] = jnp.broadcast_to(shrink, shrink_out.shape)
    qw_out[0] = (state[0, k_rows:] * keep) * shrink
    kw_out[0] = (state[0, :k_rows] * keep) * shrink
    swap2[0].wait_recv()
    for which, (moment, part_out) in enumerate(((qm_out, qy_out), (km_out, ky_out))):
        part_out[0] = mm3(split(moment[0]), split(mix[which]))
    swap2[1].wait_recv()
    sent = sum(len(span) for span in spans)
    passed = sent - len(spans[last]) + (2 * (chunks - kept) if line else 0)
    for count, ref, sem in ((sent, near_send, ns_s), (passed, own, fs_s)):
        part = ref.at[pl.ds(0, count)]
        copy(part, part, sem, sem, (dp, other_core)).wait_send()
    copy(mix, mix, m_s, m_s, (dp, other_core)).wait_send()
    for each in (all_peaks, all_peaks2, all_rows):
        each.wait_send()
    for which in range(2):

        @on_core(which)
        def _():
            base_copy(which).wait_send()
            back_copy(which).wait_send()


def finish(
    n_mp, qw_ref, kw_ref, qm_ref, km_ref, qy_ref, ky_ref, final_ref, shrink_ref,
    qw_out, kw_out, qm_out, km_out, qw_new, kw_new, sems,
):
    stores = [
        pltpu.make_async_copy(src, dst, sems.at[i])
        for i, (src, dst) in enumerate((
            (qm_ref, qm_out), (km_ref, km_out), (kw_new, kw_out), (qw_new, qw_out),
        ))
    ]
    stores[0].start()
    stores[1].start()
    groups = ((1, kw_ref, ky_ref, kw_new, stores[2]), (0, qw_ref, qy_ref, qw_new, stores[3]))
    for which, weight, part, weight_new, store in groups:
        size = STEP_SIZE * 0.2 * math.sqrt(2 * n_mp * part.shape[1])
        ortho = mm3(split(part[0]), split(final_ref[which]))
        weight_new[0] = weight[0] - (size * ortho) * shrink_ref[...]
        store.start()
    for each in stores:
        each.wait()


def local(
    q_latent, kv_latent, q_head_grad, k_head_grad, q_heads, k_heads,
    query_pick, key_pick, q_weight, k_weight, q_moment, k_moment,
):
    n_dp = lax.axis_size("dp")
    n_mp = lax.axis_size("mp")
    heads = n_dp // 2
    n_outer = n_dp // 2
    n_group = n_mp // 2
    rows = q_latent.shape[2] + kv_latent.shape[2]
    width = q_moment.shape[2]
    operands = (
        q_latent.transpose(1, 2, 0), kv_latent.transpose(1, 2, 0), q_head_grad, k_head_grad,
        q_heads, k_heads, query_pick.transpose(2, 0, 1), key_pick.transpose(2, 0, 1),
        q_weight, k_weight, q_moment, k_moment,
    )
    vmem = pltpu.VMEM
    dma = pltpu.SemaphoreType.DMA
    square = (width, width)
    folded = (width // 2 + 1, width)
    tile = (1, width)
    tokens = q_latent.shape[0]
    k_rows = k_moment.shape[1]
    chunks = rows // k_rows

    def blocks(count):
        return vmem((count, k_rows, width), F32)

    shapes = [a.shape for a in (q_weight, k_weight, q_moment, k_moment)]
    parts = pl.pallas_call(
        functools.partial(kernel, n_dp, n_mp, heads),
        out_shape=[vmem(shape, F32) for shape in shapes + shapes[2:] + [(2,) + square, tile]],
        in_specs=[pl.BlockSpec(memory_space=pl.ANY)] * 12,
        out_specs=[pl.BlockSpec(memory_space=vmem)] * 8,
        scratch_shapes=[
            vmem((2, rows, tokens), BF16),
            vmem((2,) + q_head_grad.shape, BF16),
            vmem((2,) + q_heads.shape, BF16),
            vmem((2,) + operands[6].shape, jnp.int32),
            vmem((2, rows, width), F32),
            dma((5,)),
            blocks(n_outer * chunks), blocks((n_outer - 1) * chunks), blocks(n_outer * chunks),
            blocks(chunks), blocks(chunks - chunks // 2),
            vmem((n_outer, chunks, 2, k_rows, width), F32),
            blocks(chunks), blocks(chunks - 1), blocks(chunks - 1),
            vmem(tile, F32),
            vmem((n_dp - 1,) + tile, F32),
            vmem(tile, F32),
            vmem((n_mp - 1,) + tile, F32),
            vmem(folded, F32),
            vmem((2 * n_group - 1,) + folded, F32),
            vmem((2,) + square, F32),
            dma, dma(((n_outer - 1) * chunks,)),
            dma, dma((n_outer, chunks)), dma((chunks,)), dma,
            dma, dma, dma, dma, dma, dma, dma, dma, dma, dma,
            dma, dma((2,)),
        ],
        compiler_params=pltpu.CompilerParams(
            collective_id=0, has_side_effects=True, vmem_limit_bytes=56 * 1024 * 1024
        ),
    )(*operands)
    return pl.pallas_call(
        functools.partial(finish, n_mp),
        out_shape=[jax.ShapeDtypeStruct(shape, F32) for shape in shapes],
        in_specs=[pl.BlockSpec(memory_space=vmem)] * 8,
        out_specs=[pl.BlockSpec(memory_space=pl.ANY)] * 4,
        scratch_shapes=[vmem(shape, F32) for shape in shapes[:2]] + [dma((4,))],
    )(*[pltpu.with_memory_space_constraint(part, vmem) for part in parts])


def solution(mesh):
    rows3 = P("dp", "mp", None)
    in_specs = (
        P("dp", None, "mp"), P("dp", None, "mp"), P("dp", None), P("dp", None),
        P("dp", "mp"), P("dp", "mp"), P("dp", None, "mp"), P("dp", None, "mp"),
        rows3, rows3, rows3, rows3,
    )
    return jax.shard_map(
        lambda *args: tuple(local(*args)),
        mesh=mesh, in_specs=in_specs, out_specs=(rows3,) * 4, check_vma=False,
    )
```

```python
import functools
import math

import jax
import jax.numpy as jnp
from jax import lax
from jax.experimental import pallas as pl
from jax.experimental.pallas import tpu as pltpu
from jax.sharding import PartitionSpec as P

ITERS = 5
MOMENTUM = 0.95
STEP_SIZE = 1.0
DECAY = 0.1
CLIP_LEVEL = 0.1
SCORE_SCALE = 1.0 / math.sqrt(192.0)
COEFF_A = 3.4445
COEFF_B = -4.775
COEFF_C = 2.0315
LOWEST = -1e30
MESH = pl.DeviceIdType.MESH
F32 = jnp.float32
BF16 = jnp.bfloat16


def split(value):
    high = value.astype(BF16)
    return high, (value - high.astype(F32)).astype(BF16)


def mm(a, b):
    return jnp.dot(a, b, preferred_element_type=F32)


def mm3(a, b):
    both = mm(a[0], jnp.concatenate([b[0], b[1]], axis=1))
    width = b[0].shape[1]
    return both[:, :width] + (both[:, width:] + mm(a[1], b[0]))


def mm_deep(a, b):
    return mm(
        jnp.concatenate([a[0], a[1], a[0]], axis=1), jnp.concatenate([b[0], b[0], b[1]], axis=0)
    )


def gram(rows):
    high, low = split(rows)
    left = jnp.concatenate([high, low, high], axis=0)
    return mm(left.T, jnp.concatenate([high, high, low], axis=0))


def fold(matrix):
    width = matrix.shape[0]
    half = width // 2
    row = lax.broadcasted_iota(jnp.int32, (half, width), 0)
    lane = lax.broadcasted_iota(jnp.int32, (half, width), 1)
    lower = matrix[half:]
    body = jnp.where(lane >= row, matrix[:half], pltpu.roll(lower, half, 1))
    ends = jnp.sum(jnp.where(lane == row + half, lower, 0.0), axis=0, keepdims=True)
    return jnp.concatenate([body, ends], axis=0)


def unfold(message):
    width = message.shape[1]
    half = width // 2
    row = lax.broadcasted_iota(jnp.int32, (half, width), 0)
    lane = lax.broadcasted_iota(jnp.int32, (half, width), 1)
    body = message[:half]
    ends = jnp.broadcast_to(message[half : half + 1], (half, width))
    top = jnp.where(lane >= row, body, 0.0)
    strict = jnp.where((lane >= half) & (lane - half < row), pltpu.roll(body, half, 1), 0.0)
    one_side = jnp.concatenate([top, jnp.where(lane == row + half, ends, strict)], axis=0)
    full_row = lax.broadcasted_iota(jnp.int32, (width, width), 0)
    full_lane = lax.broadcasted_iota(jnp.int32, (width, width), 1)
    return one_side + jnp.where(full_row == full_lane, 0.0, one_side.T)


def spread_down(row):
    count = row.shape[1]
    spread = jnp.broadcast_to(row, (count, count))
    same = lax.broadcasted_iota(jnp.int32, (count, count), 0) == lax.broadcasted_iota(
        jnp.int32, (count, count), 1
    )
    picked = jnp.where(same, spread, 0).astype(F32)
    return jnp.sum(picked, axis=1, keepdims=True).astype(jnp.int32)


def partner(index, count, step):
    if count & (count - 1):
        return lax.rem(index + step, count)
    result = 0
    bit = 1
    while bit < count:
        held = lax.rem(lax.div(index, bit), 2)
        result = result + bit * ((1 - held) if step & bit else held)
        bit *= 2
    return result


def kernel(
    n_dp, n_mp, heads,
    ql_in, kl_in, qg_in, kg_in, qh_in, kh_in, qp_in, kp_in, qw_in, kw_in, qm_in, km_in,
    qw_out, kw_out, qm_out, km_out, qy_out, ky_out, final, shrink_out,
    latents, grads, act, picks, state, in_sems,
    near_send, near_recv, own, relay_recv, raw_recv, fin, base, back_send, back_recv, peak_send, peak_recv, peak2_send, peak2_recv,
    row_send, row_recv, mix,
    ns_s, ns_r, fs_s, fin_r, rl_r, rw_r, b_s, b_r, bk_s, bk_r, pk_s, pk_r, pm_s, pm_r, y_s, y_r, m_s, m_r,
):
    dp = lax.axis_index("dp")
    mp = lax.axis_index("mp")
    n_outer = n_dp // 2
    outer = lax.div(dp, 2)
    inner = lax.rem(dp, 2)
    core = lax.rem(mp, 2)
    group = lax.div(mp, 2)
    n_group = n_mp // 2
    q_rows = qm_in.shape[1]
    k_rows = km_in.shape[1]
    width = qm_in.shape[2]
    tokens = qg_in.shape[0]
    tall = q_rows + k_rows
    top_rows = pl.ds(0, k_rows)
    low_rows = pl.ds(k_rows, q_rows)
    other_core = mp + 1 - 2 * core

    loads = (
        ((kl_in, latents.at[:, top_rows]), (ql_in, latents.at[:, low_rows])),
        ((kg_in, grads.at[1]), (qg_in, grads.at[0])),
        ((qp_in, picks.at[0]), (kp_in, picks.at[1])),
        ((qh_in, act.at[0]), (kh_in, act.at[1])),
        (
            (km_in.at[0], state.at[1, top_rows]), (qm_in.at[0], state.at[1, low_rows]),
            (kw_in.at[0], state.at[0, top_rows]), (qw_in.at[0], state.at[0, low_rows]),
        ),
    )
    for i, group_of in enumerate(loads):
        for src, dst in group_of:
            pltpu.make_async_copy(src, dst, in_sems.at[i]).start()

    def loaded(*which):
        for i in which:
            ref = (latents, grads, picks, act, state)[i]
            pltpu.make_async_copy(ref, ref, in_sems.at[i]).wait()

    barrier = pltpu.get_barrier_semaphore()
    for step in range(1, n_dp):
        for column in (mp, other_core):
            pl.semaphore_signal(
                barrier, inc=1, device_id=(lax.rem(dp + step, n_dp), column), device_id_type=MESH
            )
    def owner(step):
        across = lax.rem(dp + (step // n_group) * heads, n_dp)
        return across, 2 * lax.rem(group + step, n_group) + core

    for step in range(n_group + 1, 2 * n_group):
        pl.semaphore_signal(barrier, inc=1, device_id=owner(step), device_id_type=MESH)
    for step in range(1, n_mp):
        pl.semaphore_signal(
            barrier, inc=1, device_id=(dp, lax.rem(mp + step, n_mp)), device_id_type=MESH
        )

    def copy(src, dst, send, recv, where):
        return pltpu.make_async_remote_copy(
            src_ref=src, dst_ref=dst, send_sem=send, recv_sem=recv,
            device_id=where, device_id_type=MESH,
        )

    all_peaks = copy(peak_recv, peak_recv, pk_s, pk_r, (dp, other_core))
    all_peaks2 = copy(peak2_recv, peak2_recv, pm_s, pm_r, (dp, other_core))
    all_rows = copy(row_recv, row_recv, y_s, y_r, (dp, other_core))

    def term(dst, spot, to_outer, to_inner, parts=(0, 1)):
        slot = 2 * to_outer + to_inner
        half = lax.div(slot, heads)
        cols = pl.ds(pl.multiple_of(lax.rem(slot, heads) * width, width), width)
        first = spot * chunks
        if 0 in parts:
            dst[first] = mm(latents[half, :k_rows], grads[1, :, cols])
        if 1 in parts:
            rest = mm(latents[half, k_rows:], grads[0, :, cols])
            dst[first + 1 : first + chunks] = rest.reshape(chunks - 1, step_rows, width)

    step_rows = k_rows
    chunks = tall // step_rows
    loaded(0, 1)
    entered = 2 * (n_dp - 1) + (n_mp - 1) + (n_group - 1)
    across_x = dp + 1 - 2 * inner
    neighbour = (across_x, mp)
    partner_core = (dp, other_core)
    last = n_outer - 1
    line = n_outer == 4
    inside = lax.rem(lax.div(outer, 2) + lax.rem(outer, 2), 2)
    by = [partner(outer, n_outer, step) for step in range(n_outer)]

    def at(spot, chunk):
        return spot * chunks + chunk

    if line:
        split_to = by[2] + inside * (by[1] - by[2])
        whole_to = by[1] + inside * (by[2] - by[1])
        order = [by[3], split_to, whole_to, by[0]]
        kept = chunks // 2
        spans = [range(chunks), range(kept), range(chunks), range(chunks)]
    else:
        order = by[::-1]
        spans = [range(chunks)] * n_outer

    def near_copy(spot, chunk):
        where = at(spot, chunk)
        return copy(near_send.at[where], near_recv.at[where], ns_s, ns_r.at[where], neighbour)

    def home(chunk):
        return 2 * group + (1 if chunk else 0)

    def landed(slot, chunk):
        return fin_r.at[slot, max(chunk - 1, 0)]

    def final_copy(source, spot, slot, chunk, sent, to):
        return copy(
            source.at[at(spot, chunk)], fin.at[slot, chunk, core], sent, landed(slot, chunk),
            (to, home(chunk)),
        )

    def far_copy(spot, chunk, target):
        return final_copy(own, spot, spot, chunk, fs_s, 2 * target + inner)

    def send_last(which):
        for chunk in which:
            final_copy(near_send, last, last, chunk, ns_s, across_x).start()

    def relay_copy(chunk):
        return copy(
            own.at[at(0, chunk)], relay_recv.at[chunk], fs_s, rl_r.at[chunk],
            (2 * by[1] + inner, mp),
        )

    def raw_copy():
        return copy(
            near_send.at[pl.ds(at(1, kept), chunks - kept)], raw_recv, fs_s, rw_r,
            (2 * split_to + inner, mp),
        )

    def send_near(spot, which):
        for chunk in which:
            near_copy(spot, chunk).start()

    term(near_send, 0, order[0], 1 - inner, (0,))
    pl.semaphore_wait(barrier, entered)
    send_near(0, spans[0][:1])
    term(near_send, 0, order[0], 1 - inner, (1,))
    send_near(0, spans[0][1:])
    if line:
        term(near_send, 1, order[1], 1 - inner)
        raw_copy().start()
        term(own, 1, order[1], inner)
        for chunk in range(kept, chunks):
            far_copy(1, chunk, split_to).start()
        term(near_send, 2, order[2], 1 - inner)

        send_near(1, spans[1])
        send_near(2, spans[2])

    loaded(2, 3)
    local_heads = picks.shape[1]
    lane = lax.broadcasted_iota(jnp.int32, (1, width), 1)
    peaks = jnp.full((1, width), LOWEST, F32)
    ids = lax.broadcasted_iota(jnp.int32, (picks.shape[3], tokens), 1)
    for head in range(local_heads):
        span = slice(head * width, (head + 1) * width)
        pick_q = (ids == spread_down(picks[0, head])).astype(F32).astype(BF16)
        pick_k = (ids == spread_down(picks[1, head])).astype(F32).astype(BF16)
        score = jnp.sum(
            mm(pick_q, act[0, :, span]) * mm(pick_k, act[1, :, span]), axis=1, keepdims=True
        )
        top = jnp.max(score * SCORE_SCALE, axis=0, keepdims=True)
        peaks = jnp.where(lane == mp * local_heads + head, top, peaks)
    peak_send[...] = peaks
    for step in range(1, n_dp):
        each = copy(
            peak_send, peak_recv.at[step - 1], pk_s, pk_r,
            (lax.rem(dp + step, n_dp), mp),
        )
        each.start()

    if line:
        term(near_send, last, order[last], 1 - inner)
        send_last(range(kept))
    else:
        for spot in range(1, n_outer):
            term(near_send, spot, order[spot], 1 - inner)
            if spot < last:
                send_near(spot, spans[spot])
        send_last(range(chunks))
    for spot in range(n_outer):
        if not (line and spot == 1):
            term(own, spot, order[spot], inner)

    loaded(4)
    for chunk in range(chunks):
        moment = state[1, chunk * step_rows : (chunk + 1) * step_rows]
        own[at(last, chunk)] = MOMENTUM * moment + own[at(last, chunk)]

    def on_core(which):
        return pl.when(core == which)

    def shares(which):
        return pl.ds(0, 1) if which else pl.ds(1, chunks - 1)

    def base_copy(which):
        rows = shares(which)
        source = own.at[pl.ds(at(last, rows.start), rows.size)]
        return copy(source, base.at[rows], b_s, b_r, partner_core)

    def back_copy(which):
        rows = pl.ds(0, shares(1 - which).size)
        return copy(back_send.at[rows], back_recv.at[rows], bk_s, bk_r, partner_core)

    for which in range(2):

        @on_core(which)
        def _():
            base_copy(which).start()

    def meet(spot, chunk):
        near_copy(spot, chunk).wait_recv()
        where = at(spot, chunk)
        own[where] = own[where] + near_recv[where]

    def arrived(slot, chunk):
        ref = fin.at[slot, chunk]
        copy(ref, ref, fs_s, landed(slot, chunk), partner_core).wait_recv()
        return fin[slot, chunk]

    def pass_on(spot):
        for chunk in spans[spot]:
            meet(spot, chunk)
            far_copy(spot, chunk, order[spot]).start()

    if line:
        def forward(held):
            for chunk in spans[0]:
                meet(0, chunk)
                if held:
                    far_copy(0, chunk, by[3]).start()
                else:
                    relay_copy(chunk).start()
            pass_on(1)
            raw_copy().wait_recv()
            low = pl.ds(at(last, kept), chunks - kept)
            near_send[low] = near_send[low] + raw_recv[...]
            send_last(range(kept, chunks))
            for chunk in spans[2]:
                if held:
                    relay_copy(chunk).wait_recv()
                    own[at(2, chunk)] = own[at(2, chunk)] + relay_recv[chunk]
                meet(2, chunk)
                far_copy(2, chunk, whole_to).start()

        for held in range(2):

            @pl.when(inside == held)
            def _():
                forward(held)

    else:
        for spot in range(last):
            pass_on(spot)

    def complete(which, chunk):
        added = [arrived(slot, chunk) for slot in ((1, 2, last) if line else range(n_outer))]
        mine = own[at(last, chunk)]
        other = base[chunk]
        for each in added:
            mine = mine + each[which]
            other = other + each[1 - which]
        if which:
            qm_out[0, (chunk - 1) * step_rows : chunk * step_rows] = mine
            back_send[chunk - 1] = other
        else:
            km_out[0] = mine
            back_send[chunk] = other
        return gram(jnp.concatenate([mine, other], axis=0))

    for which, members in enumerate((range(1), range(1, chunks))):

        @on_core(which)
        def _():
            base_copy(1 - which).wait_recv()
            if line:

                @pl.when(inside == 1)
                def _():
                    for chunk in members:
                        early = arrived(0, chunk)
                        own[at(last, chunk)] = own[at(last, chunk)] + early[which]
                        base[chunk] = base[chunk] + early[1 - which]

            pair = complete(which, members[0])
            for chunk in members[1:]:
                pair = pair + complete(which, chunk)
            row_send[...] = fold(pair)

    for step in reversed(range(1, 2 * n_group)):
        each = copy(
            row_send, row_recv.at[step - 1], y_s, y_r, owner(step)
        )
        each.start()
    for which in range(2):

        @on_core(which)
        def _():
            back_copy(which).start()

    all_peaks.wait_recv()
    peaks = jnp.maximum(peaks, jnp.max(peak_recv[...], axis=0))
    peak2_send[...] = peaks
    for step in range(1, n_mp):
        each = copy(
            peak2_send, peak2_recv.at[step - 1], pm_s, pm_r,
            (dp, lax.rem(mp + step, n_mp)),
        )
        each.start()

    @on_core(0)
    def _():
        back_copy(1).wait_recv()
        qm_out[0] = back_recv[...].reshape(q_rows, width)

    @on_core(1)
    def _():
        back_copy(0).wait_recv()
        km_out[0] = back_recv[0]

    all_rows.wait_recv()
    whole = unfold(row_send[...] + jnp.sum(row_recv[...], axis=0))

    eye = (
        lax.broadcasted_iota(jnp.int32, (width, width), 0)
        == lax.broadcasted_iota(jnp.int32, (width, width), 1)
    ).astype(F32)
    trace = jnp.sum(jnp.sum(whole * eye, axis=0, keepdims=True), axis=1, keepdims=True)
    scale = 1.0 / jnp.sqrt(trace + 1.0)
    current = whole * (scale * scale)
    mixed = None
    swap2 = [
        copy(ref.at[1 - core], ref.at[1 - core], m_s, m_r.at[i], (dp, other_core))
        for i, ref in enumerate((mix, final))
    ]
    for step in range(ITERS):
        parts = split(current)
        square = mm_deep(parts, parts)
        poly = COEFF_A * eye + COEFF_B * current + COEFF_C * square
        if step + 1 == ITERS:
            break
        pair = split(poly)
        mixed = poly * scale if mixed is None else mm_deep(split(mixed), pair)
        if step + 2 == ITERS:
            mix[1 - core] = mixed
            swap2[0].start()
        current = mm_deep(split(mm_deep(pair, parts)), pair)
    final[1 - core] = poly
    swap2[1].start()
    all_peaks2.wait_recv()
    peaks = jnp.maximum(peaks, jnp.max(peak2_recv[...], axis=0))
    mine = jnp.where(lane == lax.rem(dp, heads), peaks, LOWEST)
    peak = jnp.max(jnp.max(mine, axis=0, keepdims=True), axis=1, keepdims=True)
    shrink = jnp.sqrt(CLIP_LEVEL / jnp.maximum(peak, CLIP_LEVEL))
    keep = 1.0 - STEP_SIZE * DECAY
    shrink_out[...] = jnp.broadcast_to(shrink, shrink_out.shape)
    qw_out[0] = (state[0, k_rows:] * keep) * shrink
    kw_out[0] = (state[0, :k_rows] * keep) * shrink
    swap2[0].wait_recv()
    for which, (moment, part_out) in enumerate(((qm_out, qy_out), (km_out, ky_out))):
        part_out[0] = mm3(split(moment[0]), split(mix[which]))
    swap2[1].wait_recv()
    sent = sum(len(span) for span in spans)
    passed = sent - len(spans[last]) + (2 * (chunks - kept) if line else 0)
    for count, ref, sem in ((sent, near_send, ns_s), (passed, own, fs_s)):
        part = ref.at[pl.ds(0, count)]
        copy(part, part, sem, sem, (dp, other_core)).wait_send()
    copy(mix, mix, m_s, m_s, (dp, other_core)).wait_send()
    for each in (all_peaks, all_peaks2, all_rows):
        each.wait_send()
    for which in range(2):

        @on_core(which)
        def _():
            base_copy(which).wait_send()
            back_copy(which).wait_send()


def finish(
    n_mp, qw_ref, kw_ref, qm_ref, km_ref, qy_ref, ky_ref, final_ref, shrink_ref,
    qw_out, kw_out, qm_out, km_out, qw_new, kw_new, sems,
):
    stores = [
        pltpu.make_async_copy(src, dst, sems.at[i])
        for i, (src, dst) in enumerate((
            (qm_ref, qm_out), (km_ref, km_out), (kw_new, kw_out), (qw_new, qw_out),
        ))
    ]
    stores[0].start()
    stores[1].start()
    groups = ((1, kw_ref, ky_ref, kw_new, stores[2]), (0, qw_ref, qy_ref, qw_new, stores[3]))
    for which, weight, part, weight_new, store in groups:
        size = STEP_SIZE * 0.2 * math.sqrt(2 * n_mp * part.shape[1])
        ortho = mm3(split(part[0]), split(final_ref[which]))
        weight_new[0] = weight[0] - (size * ortho) * shrink_ref[...]
        store.start()
    for each in stores:
        each.wait()


def local(
    q_latent, kv_latent, q_head_grad, k_head_grad, q_heads, k_heads,
    query_pick, key_pick, q_weight, k_weight, q_moment, k_moment,
):
    n_dp = lax.axis_size("dp")
    n_mp = lax.axis_size("mp")
    heads = n_dp // 2
    n_outer = n_dp // 2
    n_group = n_mp // 2
    rows = q_latent.shape[2] + kv_latent.shape[2]
    width = q_moment.shape[2]
    operands = (
        q_latent.transpose(1, 2, 0), kv_latent.transpose(1, 2, 0), q_head_grad, k_head_grad,
        q_heads, k_heads, query_pick.transpose(2, 0, 1), key_pick.transpose(2, 0, 1),
        q_weight, k_weight, q_moment, k_moment,
    )
    vmem = pltpu.VMEM
    dma = pltpu.SemaphoreType.DMA
    square = (width, width)
    folded = (width // 2 + 1, width)
    tile = (1, width)
    tokens = q_latent.shape[0]
    k_rows = k_moment.shape[1]
    chunks = rows // k_rows

    def blocks(count):
        return vmem((count, k_rows, width), F32)

    shapes = [a.shape for a in (q_weight, k_weight, q_moment, k_moment)]
    parts = pl.pallas_call(
        functools.partial(kernel, n_dp, n_mp, heads),
        out_shape=[vmem(shape, F32) for shape in shapes + shapes[2:] + [(2,) + square, tile]],
        in_specs=[pl.BlockSpec(memory_space=pl.ANY)] * 12,
        out_specs=[pl.BlockSpec(memory_space=vmem)] * 8,
        scratch_shapes=[
            vmem((2, rows, tokens), BF16),
            vmem((2,) + q_head_grad.shape, BF16),
            vmem((2,) + q_heads.shape, BF16),
            vmem((2,) + operands[6].shape, jnp.int32),
            vmem((2, rows, width), F32),
            dma((5,)),
            blocks(n_outer * chunks), blocks((n_outer - 1) * chunks), blocks(n_outer * chunks),
            blocks(chunks), blocks(chunks - chunks // 2),
            vmem((n_outer, chunks, 2, k_rows, width), F32),
            blocks(chunks), blocks(chunks - 1), blocks(chunks - 1),
            vmem(tile, F32),
            vmem((n_dp - 1,) + tile, F32),
            vmem(tile, F32),
            vmem((n_mp - 1,) + tile, F32),
            vmem(folded, F32),
            vmem((2 * n_group - 1,) + folded, F32),
            vmem((2,) + square, F32),
            dma, dma(((n_outer - 1) * chunks,)),
            dma, dma((n_outer, chunks - 1)), dma((chunks,)), dma,
            dma, dma, dma, dma, dma, dma, dma, dma, dma, dma,
            dma, dma((2,)),
        ],
        compiler_params=pltpu.CompilerParams(
            collective_id=0, has_side_effects=True, vmem_limit_bytes=56 * 1024 * 1024
        ),
    )(*operands)
    return pl.pallas_call(
        functools.partial(finish, n_mp),
        out_shape=[jax.ShapeDtypeStruct(shape, F32) for shape in shapes],
        in_specs=[pl.BlockSpec(memory_space=vmem)] * 8,
        out_specs=[pl.BlockSpec(memory_space=pl.ANY)] * 4,
        scratch_shapes=[vmem(shape, F32) for shape in shapes[:2]] + [dma((4,))],
    )(*[pltpu.with_memory_space_constraint(part, vmem) for part in parts])


def solution(mesh):
    rows3 = P("dp", "mp", None)
    in_specs = (
        P("dp", None, "mp"), P("dp", None, "mp"), P("dp", None), P("dp", None),
        P("dp", "mp"), P("dp", "mp"), P("dp", None, "mp"), P("dp", None, "mp"),
        rows3, rows3, rows3, rows3,
    )
    return jax.shard_map(
        lambda *args: tuple(local(*args)),
        mesh=mesh, in_specs=in_specs, out_specs=(rows3,) * 4, check_vma=False,
    )
```

```python
import functools
import math

import jax
import jax.numpy as jnp
from jax import lax
from jax.experimental import pallas as pl
from jax.experimental.pallas import tpu as pltpu
from jax.sharding import PartitionSpec as P

ITERS = 5
MOMENTUM = 0.95
STEP_SIZE = 1.0
DECAY = 0.1
CLIP_LEVEL = 0.1
SCORE_SCALE = 1.0 / math.sqrt(192.0)
COEFF_A = 3.4445
COEFF_B = -4.775
COEFF_C = 2.0315
LOWEST = -1e30
MESH = pl.DeviceIdType.MESH
F32 = jnp.float32
BF16 = jnp.bfloat16


def split(value):
    high = value.astype(BF16)
    return high, (value - high.astype(F32)).astype(BF16)


def mm(a, b):
    return jnp.dot(a, b, preferred_element_type=F32)


def mm3(a, b):
    both = mm(a[0], jnp.concatenate([b[0], b[1]], axis=1))
    width = b[0].shape[1]
    return both[:, :width] + (both[:, width:] + mm(a[1], b[0]))


def mm_deep(a, b):
    return mm(
        jnp.concatenate([a[0], a[1], a[0]], axis=1), jnp.concatenate([b[0], b[0], b[1]], axis=0)
    )


def gram(rows):
    high, low = split(rows)
    left = jnp.concatenate([high, low, high], axis=0)
    return mm(left.T, jnp.concatenate([high, high, low], axis=0))


def fold(matrix):
    width = matrix.shape[0]
    half = width // 2
    row = lax.broadcasted_iota(jnp.int32, (half, width), 0)
    lane = lax.broadcasted_iota(jnp.int32, (half, width), 1)
    lower = matrix[half:]
    body = jnp.where(lane >= row, matrix[:half], pltpu.roll(lower, half, 1))
    ends = jnp.sum(jnp.where(lane == row + half, lower, 0.0), axis=0, keepdims=True)
    return jnp.concatenate([body, ends], axis=0)


def unfold(message):
    width = message.shape[1]
    half = width // 2
    row = lax.broadcasted_iota(jnp.int32, (half, width), 0)
    lane = lax.broadcasted_iota(jnp.int32, (half, width), 1)
    body = message[:half]
    ends = jnp.broadcast_to(message[half : half + 1], (half, width))
    top = jnp.where(lane >= row, body, 0.0)
    strict = jnp.where((lane >= half) & (lane - half < row), pltpu.roll(body, half, 1), 0.0)
    one_side = jnp.concatenate([top, jnp.where(lane == row + half, ends, strict)], axis=0)
    full_row = lax.broadcasted_iota(jnp.int32, (width, width), 0)
    full_lane = lax.broadcasted_iota(jnp.int32, (width, width), 1)
    return one_side + jnp.where(full_row == full_lane, 0.0, one_side.T)


def spread_down(row):
    count = row.shape[1]
    spread = jnp.broadcast_to(row, (count, count))
    same = lax.broadcasted_iota(jnp.int32, (count, count), 0) == lax.broadcasted_iota(
        jnp.int32, (count, count), 1
    )
    picked = jnp.where(same, spread, 0).astype(F32)
    return jnp.sum(picked, axis=1, keepdims=True).astype(jnp.int32)


def partner(index, count, step):
    if count & (count - 1):
        return lax.rem(index + step, count)
    result = 0
    bit = 1
    while bit < count:
        held = lax.rem(lax.div(index, bit), 2)
        result = result + bit * ((1 - held) if step & bit else held)
        bit *= 2
    return result


def kernel(
    n_dp, n_mp, heads,
    ql_in, kl_in, qg_in, kg_in, qh_in, kh_in, qp_in, kp_in, qw_in, kw_in, qm_in, km_in,
    qw_out, kw_out, qm_out, km_out, qy_out, ky_out, final, shrink_out,
    latents, grads, act, picks, state, in_sems,
    near_send, near_recv, own, relay_recv, raw_recv, fin, base, back_send, back_recv, peak_send, peak_recv, peak2_send, peak2_recv,
    row_send, row_recv, mix,
    ns_s, ns_r, fs_s, fin_r, rl_r, rw_r, b_s, b_r, bk_s, bk_r, pk_s, pk_r, pm_s, pm_r, y_s, y_r, m_s, m_r,
):
    dp = lax.axis_index("dp")
    mp = lax.axis_index("mp")
    n_outer = n_dp // 2
    outer = lax.div(dp, 2)
    inner = lax.rem(dp, 2)
    core = lax.rem(mp, 2)
    group = lax.div(mp, 2)
    n_group = n_mp // 2
    q_rows = qm_in.shape[1]
    k_rows = km_in.shape[1]
    width = qm_in.shape[2]
    tokens = qg_in.shape[0]
    tall = q_rows + k_rows
    top_rows = pl.ds(0, k_rows)
    low_rows = pl.ds(k_rows, q_rows)
    other_core = mp + 1 - 2 * core

    loads = (
        ((kl_in, latents.at[:, top_rows]), (ql_in, latents.at[:, low_rows])),
        ((kg_in, grads.at[1]), (qg_in, grads.at[0])),
        ((qp_in, picks.at[0]), (kp_in, picks.at[1])),
        ((qh_in, act.at[0]), (kh_in, act.at[1])),
        (
            (km_in.at[0], state.at[1, top_rows]), (qm_in.at[0], state.at[1, low_rows]),
            (kw_in.at[0], state.at[0, top_rows]), (qw_in.at[0], state.at[0, low_rows]),
        ),
    )
    for i, group_of in enumerate(loads):
        for src, dst in group_of:
            pltpu.make_async_copy(src, dst, in_sems.at[i]).start()

    def loaded(*which):
        for i in which:
            ref = (latents, grads, picks, act, state)[i]
            pltpu.make_async_copy(ref, ref, in_sems.at[i]).wait()

    barrier = pltpu.get_barrier_semaphore()

    def greet(*where):
        pl.semaphore_signal(barrier, inc=1, device_id=where, device_id_type=MESH)

    def owner(step):
        across = lax.rem(dp + (step // n_group) * heads, n_dp)
        return across, 2 * lax.rem(group + step, n_group) + core

    across_x = dp + 1 - 2 * inner
    by = [partner(outer, n_outer, step) for step in range(n_outer)]
    for step in range(n_outer - 1, 0, -1):
        greet(2 * by[step] + inner, mp)
        greet(2 * by[step] + inner, other_core)
        greet(2 * by[step] + 1 - inner, mp)
    greet(across_x, mp)
    greet(across_x, other_core)
    for step in range(2 * n_group - 1, n_group, -1):
        greet(*owner(step))
    for step in range(1, n_mp):
        greet(dp, lax.rem(mp + step, n_mp))

    def copy(src, dst, send, recv, where):
        return pltpu.make_async_remote_copy(
            src_ref=src, dst_ref=dst, send_sem=send, recv_sem=recv,
            device_id=where, device_id_type=MESH,
        )

    all_peaks = copy(peak_recv, peak_recv, pk_s, pk_r, (dp, other_core))
    all_peaks2 = copy(peak2_recv, peak2_recv, pm_s, pm_r, (dp, other_core))
    all_rows = copy(row_recv, row_recv, y_s, y_r, (dp, other_core))

    def term(dst, spot, to_outer, to_inner, parts=(0, 1)):
        slot = 2 * to_outer + to_inner
        half = lax.div(slot, heads)
        cols = pl.ds(pl.multiple_of(lax.rem(slot, heads) * width, width), width)
        first = spot * chunks
        if 0 in parts:
            dst[first] = mm(latents[half, :k_rows], grads[1, :, cols])
        if 1 in parts:
            rest = mm(latents[half, k_rows:], grads[0, :, cols])
            dst[first + 1 : first + chunks] = rest.reshape(chunks - 1, step_rows, width)

    step_rows = k_rows
    chunks = tall // step_rows
    loaded(0, 1)
    entered = 3 * (n_outer - 1) + 2 + (n_mp - 1) + (n_group - 1)
    neighbour = (across_x, mp)
    partner_core = (dp, other_core)
    last = n_outer - 1
    line = n_outer == 4
    inside = lax.rem(lax.div(outer, 2) + lax.rem(outer, 2), 2)

    def at(spot, chunk):
        return spot * chunks + chunk

    if line:
        split_to = by[2] + inside * (by[1] - by[2])
        whole_to = by[1] + inside * (by[2] - by[1])
        order = [by[3], split_to, whole_to, by[0]]
        kept = chunks // 2
        spans = [range(chunks), range(kept), range(chunks), range(chunks)]
    else:
        order = by[::-1]
        spans = [range(chunks)] * n_outer

    def near_copy(spot, chunk):
        where = at(spot, chunk)
        return copy(near_send.at[where], near_recv.at[where], ns_s, ns_r.at[where], neighbour)

    def home(chunk):
        return 2 * group + (1 if chunk else 0)

    fine_slot = 2 if line else n_outer

    def landed(slot, chunk):
        return fin_r.at[n_outer + max(chunk - 1, 0) if slot == fine_slot else slot]

    def final_copy(source, spot, slot, chunk, sent, to):
        return copy(
            source.at[at(spot, chunk)], fin.at[slot, chunk, core], sent, landed(slot, chunk),
            (to, home(chunk)),
        )

    def far_copy(spot, chunk, target):
        return final_copy(own, spot, spot, chunk, fs_s, 2 * target + inner)

    def send_last(which):
        for chunk in which:
            final_copy(near_send, last, last, chunk, ns_s, across_x).start()

    def relay_copy(chunk):
        return copy(
            own.at[at(0, chunk)], relay_recv.at[chunk], fs_s, rl_r.at[chunk],
            (2 * by[1] + inner, mp),
        )

    def raw_copy(first):
        count = chunks - first
        return copy(
            near_send.at[pl.ds(at(1, first), count)], raw_recv.at[pl.ds(first, count)],
            fs_s, rw_r, (2 * split_to + inner, mp),
        )

    def by_role(act):
        for held in range(2):
            pl.when(inside == held)(functools.partial(act, held))

    def send_near(spot, which):
        for chunk in which:
            near_copy(spot, chunk).start()

    term(near_send, 0, order[0], 1 - inner, (0,))
    pl.semaphore_wait(barrier, entered)
    send_near(0, spans[0][:1])
    term(near_send, 0, order[0], 1 - inner, (1,))
    send_near(0, spans[0][1:])
    if line:
        term(near_send, 1, order[1], 1 - inner)
        by_role(lambda held: raw_copy(0 if held else kept).start())
        term(own, 1, order[1], inner)

        def send_split(held):
            for chunk in range(0 if held else kept, chunks):
                far_copy(1, chunk, split_to).start()
            if not held:
                send_near(1, range(kept))

        by_role(send_split)
        term(near_send, 2, order[2], 1 - inner)
        send_near(2, spans[2])

    loaded(2, 3)
    local_heads = picks.shape[1]
    lane = lax.broadcasted_iota(jnp.int32, (1, width), 1)
    peaks = jnp.full((1, width), LOWEST, F32)
    ids = lax.broadcasted_iota(jnp.int32, (picks.shape[3], tokens), 1)
    for head in range(local_heads):
        span = slice(head * width, (head + 1) * width)
        pick_q = (ids == spread_down(picks[0, head])).astype(F32).astype(BF16)
        pick_k = (ids == spread_down(picks[1, head])).astype(F32).astype(BF16)
        score = jnp.sum(
            mm(pick_q, act[0, :, span]) * mm(pick_k, act[1, :, span]), axis=1, keepdims=True
        )
        top = jnp.max(score * SCORE_SCALE, axis=0, keepdims=True)
        peaks = jnp.where(lane == mp * local_heads + head, top, peaks)
    peak_send[...] = peaks
    for step in range(1, n_dp):
        each = copy(
            peak_send, peak_recv.at[step - 1], pk_s, pk_r,
            (lax.rem(dp + step, n_dp), mp),
        )
        each.start()

    if line:
        term(near_send, last, order[last], 1 - inner)
        by_role(lambda held: send_last(range(kept)) if held else None)
    else:
        for spot in range(1, n_outer):
            term(near_send, spot, order[spot], 1 - inner)
            if spot < last:
                send_near(spot, spans[spot])
        send_last(range(chunks))
    for spot in range(n_outer):
        if not (line and spot == 1):
            term(own, spot, order[spot], inner)

    loaded(4)
    for chunk in range(chunks):
        moment = state[1, chunk * step_rows : (chunk + 1) * step_rows]
        own[at(last, chunk)] = MOMENTUM * moment + own[at(last, chunk)]

    def on_core(which):
        return pl.when(core == which)

    def shares(which):
        return pl.ds(0, 1) if which else pl.ds(1, chunks - 1)

    def base_copy(which):
        rows = shares(which)
        source = own.at[pl.ds(at(last, rows.start), rows.size)]
        return copy(source, base.at[rows], b_s, b_r, partner_core)

    def back_copy(which):
        rows = pl.ds(0, shares(1 - which).size)
        return copy(back_send.at[rows], back_recv.at[rows], bk_s, bk_r, partner_core)

    for which in range(2):

        @on_core(which)
        def _():
            base_copy(which).start()

    def meet(spot, chunk):
        near_copy(spot, chunk).wait_recv()
        where = at(spot, chunk)
        own[where] = own[where] + near_recv[where]

    def arrived(slot, members):
        ref = fin.at[slot, pl.ds(members[0], len(members))]
        sem = landed(slot, members[0])
        copy(ref, ref, fs_s, sem, partner_core).wait_recv()

    def pass_on(spot):
        for chunk in spans[spot]:
            meet(spot, chunk)
            far_copy(spot, chunk, order[spot]).start()

    if line:
        def forward(held):
            for chunk in spans[0]:
                meet(0, chunk)
                if held:
                    far_copy(0, chunk, by[3]).start()
                else:
                    relay_copy(chunk).start()
            if not held:
                pass_on(1)
            first = kept if held else 0
            raw_copy(first).wait_recv()
            part = pl.ds(at(last, first), chunks - first)
            near_send[part] = near_send[part] + raw_recv[pl.ds(first, chunks - first)]
            send_last(range(first, chunks))
            for chunk in spans[2]:
                if held:
                    relay_copy(chunk).wait_recv()
                    own[at(2, chunk)] = own[at(2, chunk)] + relay_recv[chunk]
                meet(2, chunk)
                far_copy(2, chunk, whole_to).start()

        by_role(forward)

    else:
        for spot in range(last):
            pass_on(spot)

    def complete(which, chunk):
        if line:
            arrived(2, range(chunk, chunk + 1))
        added = [fin[slot, chunk] for slot in range(1 if line else 0, n_outer)]
        mine = own[at(last, chunk)]
        other = base[chunk]
        for each in added:
            mine = mine + each[which]
            other = other + each[1 - which]
        if which:
            qm_out[0, (chunk - 1) * step_rows : chunk * step_rows] = mine
            back_send[chunk - 1] = other
        else:
            km_out[0] = mine
            back_send[chunk] = other
        return gram(jnp.concatenate([mine, other], axis=0))

    for which, members in enumerate((range(1), range(1, chunks))):

        @on_core(which)
        def _():
            base_copy(1 - which).wait_recv()
            if line:

                @pl.when(inside == 1)
                def _():
                    arrived(0, members)
                    for chunk in members:
                        early = fin[0, chunk]
                        own[at(last, chunk)] = own[at(last, chunk)] + early[which]
                        base[chunk] = base[chunk] + early[1 - which]

            for slot in (1, last) if line else range(n_outer):
                arrived(slot, members)
            pair = complete(which, members[0])
            for chunk in members[1:]:
                pair = pair + complete(which, chunk)
            row_send[...] = fold(pair)

    for step in reversed(range(1, 2 * n_group)):
        each = copy(
            row_send, row_recv.at[step - 1], y_s, y_r, owner(step)
        )
        each.start()
    for which in range(2):

        @on_core(which)
        def _():
            back_copy(which).start()

    all_peaks.wait_recv()
    peaks = jnp.maximum(peaks, jnp.max(peak_recv[...], axis=0))
    peak2_send[...] = peaks
    for step in range(1, n_mp):
        each = copy(
            peak2_send, peak2_recv.at[step - 1], pm_s, pm_r,
            (dp, lax.rem(mp + step, n_mp)),
        )
        each.start()

    @on_core(0)
    def _():
        back_copy(1).wait_recv()
        qm_out[0] = back_recv[...].reshape(q_rows, width)

    @on_core(1)
    def _():
        back_copy(0).wait_recv()
        km_out[0] = back_recv[0]

    all_rows.wait_recv()
    whole = unfold(row_send[...] + jnp.sum(row_recv[...], axis=0))

    eye = (
        lax.broadcasted_iota(jnp.int32, (width, width), 0)
        == lax.broadcasted_iota(jnp.int32, (width, width), 1)
    ).astype(F32)
    trace = jnp.sum(jnp.sum(whole * eye, axis=0, keepdims=True), axis=1, keepdims=True)
    scale = 1.0 / jnp.sqrt(trace + 1.0)
    current = whole * (scale * scale)
    mixed = None
    swap2 = [
        copy(ref.at[1 - core], ref.at[1 - core], m_s, m_r.at[i], (dp, other_core))
        for i, ref in enumerate((mix, final))
    ]
    for step in range(ITERS):
        parts = split(current)
        square = mm_deep(parts, parts)
        poly = COEFF_A * eye + COEFF_B * current + COEFF_C * square
        if step + 1 == ITERS:
            break
        pair = split(poly)
        mixed = poly * scale if mixed is None else mm_deep(split(mixed), pair)
        if step + 2 == ITERS:
            mix[1 - core] = mixed
            swap2[0].start()
        current = mm_deep(split(mm_deep(pair, parts)), pair)
    final[1 - core] = poly
    swap2[1].start()
    all_peaks2.wait_recv()
    peaks = jnp.maximum(peaks, jnp.max(peak2_recv[...], axis=0))
    mine = jnp.where(lane == lax.rem(dp, heads), peaks, LOWEST)
    peak = jnp.max(jnp.max(mine, axis=0, keepdims=True), axis=1, keepdims=True)
    shrink = jnp.sqrt(CLIP_LEVEL / jnp.maximum(peak, CLIP_LEVEL))
    keep = 1.0 - STEP_SIZE * DECAY
    shrink_out[...] = jnp.broadcast_to(shrink, shrink_out.shape)
    qw_out[0] = (state[0, k_rows:] * keep) * shrink
    kw_out[0] = (state[0, :k_rows] * keep) * shrink
    def drain(sent, passed):
        for count, ref, sem in ((sent, near_send, ns_s), (passed, own, fs_s)):
            part = ref.at[pl.ds(0, count)]
            copy(part, part, sem, sem, partner_core).wait_send()

    if line:
        by_role(
            lambda held: drain(
                last * chunks + (0 if held else kept), last * chunks + (chunks if held else kept)
            )
        )
    else:
        drain(n_outer * chunks, last * chunks)
    for each in (all_peaks, all_peaks2, all_rows):
        each.wait_send()
    for which in range(2):

        @on_core(which)
        def _():
            base_copy(which).wait_send()
            back_copy(which).wait_send()

    swap2[0].wait_recv()
    for which, (moment, part_out) in enumerate(((qm_out, qy_out), (km_out, ky_out))):
        part_out[0] = mm3(split(moment[0]), split(mix[which]))
    swap2[1].wait_recv()
    copy(mix, mix, m_s, m_s, (dp, other_core)).wait_send()


def finish(
    n_mp, qw_ref, kw_ref, qm_ref, km_ref, qy_ref, ky_ref, final_ref, shrink_ref,
    qw_out, kw_out, qm_out, km_out, qw_new, kw_new, sems,
):
    stores = [
        pltpu.make_async_copy(src, dst, sems.at[i])
        for i, (src, dst) in enumerate((
            (qm_ref, qm_out), (km_ref, km_out), (kw_new, kw_out), (qw_new, qw_out),
        ))
    ]
    stores[0].start()
    stores[1].start()
    groups = ((1, kw_ref, ky_ref, kw_new, stores[2]), (0, qw_ref, qy_ref, qw_new, stores[3]))
    for which, weight, part, weight_new, store in groups:
        size = STEP_SIZE * 0.2 * math.sqrt(2 * n_mp * part.shape[1])
        ortho = mm3(split(part[0]), split(final_ref[which]))
        weight_new[0] = weight[0] - (size * ortho) * shrink_ref[...]
        store.start()
    for each in stores:
        each.wait()


def local(
    q_latent, kv_latent, q_head_grad, k_head_grad, q_heads, k_heads,
    query_pick, key_pick, q_weight, k_weight, q_moment, k_moment,
):
    n_dp = lax.axis_size("dp")
    n_mp = lax.axis_size("mp")
    heads = n_dp // 2
    n_outer = n_dp // 2
    n_group = n_mp // 2
    rows = q_latent.shape[2] + kv_latent.shape[2]
    width = q_moment.shape[2]
    operands = (
        q_latent.transpose(1, 2, 0), kv_latent.transpose(1, 2, 0), q_head_grad, k_head_grad,
        q_heads, k_heads, query_pick.transpose(2, 0, 1), key_pick.transpose(2, 0, 1),
        q_weight, k_weight, q_moment, k_moment,
    )
    vmem = pltpu.VMEM
    dma = pltpu.SemaphoreType.DMA
    square = (width, width)
    folded = (width // 2 + 1, width)
    tile = (1, width)
    tokens = q_latent.shape[0]
    k_rows = k_moment.shape[1]
    chunks = rows // k_rows

    def blocks(count):
        return vmem((count, k_rows, width), F32)

    shapes = [a.shape for a in (q_weight, k_weight, q_moment, k_moment)]
    parts = pl.pallas_call(
        functools.partial(kernel, n_dp, n_mp, heads),
        out_shape=[vmem(shape, F32) for shape in shapes + shapes[2:] + [(2,) + square, tile]],
        in_specs=[pl.BlockSpec(memory_space=pl.ANY)] * 12,
        out_specs=[pl.BlockSpec(memory_space=vmem)] * 8,
        scratch_shapes=[
            vmem((2, rows, tokens), BF16),
            vmem((2,) + q_head_grad.shape, BF16),
            vmem((2,) + q_heads.shape, BF16),
            vmem((2,) + operands[6].shape, jnp.int32),
            vmem((2, rows, width), F32),
            dma((5,)),
            blocks(n_outer * chunks), blocks((n_outer - 1) * chunks), blocks(n_outer * chunks),
            blocks(chunks), blocks(chunks),
            vmem((n_outer, chunks, 2, k_rows, width), F32),
            blocks(chunks), blocks(chunks - 1), blocks(chunks - 1),
            vmem(tile, F32),
            vmem((n_dp - 1,) + tile, F32),
            vmem(tile, F32),
            vmem((n_mp - 1,) + tile, F32),
            vmem(folded, F32),
            vmem((2 * n_group - 1,) + folded, F32),
            vmem((2,) + square, F32),
            dma, dma(((n_outer - 1) * chunks,)),
            dma, dma((n_outer + (chunks - 1 if n_outer == 4 else 0),)), dma((chunks,)), dma,
            dma, dma, dma, dma, dma, dma, dma, dma, dma, dma,
            dma, dma((2,)),
        ],
        compiler_params=pltpu.CompilerParams(
            collective_id=0, has_side_effects=True, vmem_limit_bytes=56 * 1024 * 1024
        ),
    )(*operands)
    return pl.pallas_call(
        functools.partial(finish, n_mp),
        out_shape=[jax.ShapeDtypeStruct(shape, F32) for shape in shapes],
        in_specs=[pl.BlockSpec(memory_space=vmem)] * 8,
        out_specs=[pl.BlockSpec(memory_space=pl.ANY)] * 4,
        scratch_shapes=[vmem(shape, F32) for shape in shapes[:2]] + [dma((4,))],
    )(*[pltpu.with_memory_space_constraint(part, vmem) for part in parts])


def solution(mesh):
    rows3 = P("dp", "mp", None)
    in_specs = (
        P("dp", None, "mp"), P("dp", None, "mp"), P("dp", None), P("dp", None),
        P("dp", "mp"), P("dp", "mp"), P("dp", None, "mp"), P("dp", None, "mp"),
        rows3, rows3, rows3, rows3,
    )
    return jax.shard_map(
        lambda *args: tuple(local(*args)),
        mesh=mesh, in_specs=in_specs, out_specs=(rows3,) * 4, check_vma=False,
    )
```

```python
import functools
import math

import jax
import jax.numpy as jnp
from jax import lax
from jax.experimental import pallas as pl
from jax.experimental.pallas import tpu as pltpu
from jax.sharding import PartitionSpec as P

ITERS = 5
MOMENTUM = 0.95
STEP_SIZE = 1.0
DECAY = 0.1
CLIP_LEVEL = 0.1
SCORE_SCALE = 1.0 / math.sqrt(192.0)
COEFF_A = 3.4445
COEFF_B = -4.775
COEFF_C = 2.0315
LOWEST = -1e30
MESH = pl.DeviceIdType.MESH
F32 = jnp.float32
BF16 = jnp.bfloat16


def split(value):
    high = value.astype(BF16)
    return high, (value - high.astype(F32)).astype(BF16)


def mm(a, b):
    return jnp.dot(a, b, preferred_element_type=F32)


def mm3(a, b):
    both = mm(a[0], jnp.concatenate([b[0], b[1]], axis=1))
    width = b[0].shape[1]
    return both[:, :width] + (both[:, width:] + mm(a[1], b[0]))


def mm_deep(a, b):
    return mm(
        jnp.concatenate([a[0], a[1], a[0]], axis=1), jnp.concatenate([b[0], b[0], b[1]], axis=0)
    )


def gram(rows):
    high, low = split(rows)
    left = jnp.concatenate([high, low, high], axis=0)
    return mm(left.T, jnp.concatenate([high, high, low], axis=0))


def fold(matrix):
    width = matrix.shape[0]
    half = width // 2
    row = lax.broadcasted_iota(jnp.int32, (half, width), 0)
    lane = lax.broadcasted_iota(jnp.int32, (half, width), 1)
    lower = matrix[half:]
    body = jnp.where(lane >= row, matrix[:half], pltpu.roll(lower, half, 1))
    ends = jnp.sum(jnp.where(lane == row + half, lower, 0.0), axis=0, keepdims=True)
    return jnp.concatenate([body, ends], axis=0)


def unfold(message):
    width = message.shape[1]
    half = width // 2
    row = lax.broadcasted_iota(jnp.int32, (half, width), 0)
    lane = lax.broadcasted_iota(jnp.int32, (half, width), 1)
    body = message[:half]
    ends = jnp.broadcast_to(message[half : half + 1], (half, width))
    top = jnp.where(lane >= row, body, 0.0)
    strict = jnp.where((lane >= half) & (lane - half < row), pltpu.roll(body, half, 1), 0.0)
    one_side = jnp.concatenate([top, jnp.where(lane == row + half, ends, strict)], axis=0)
    full_row = lax.broadcasted_iota(jnp.int32, (width, width), 0)
    full_lane = lax.broadcasted_iota(jnp.int32, (width, width), 1)
    return one_side + jnp.where(full_row == full_lane, 0.0, one_side.T)


def spread_down(row):
    count = row.shape[1]
    spread = jnp.broadcast_to(row, (count, count))
    same = lax.broadcasted_iota(jnp.int32, (count, count), 0) == lax.broadcasted_iota(
        jnp.int32, (count, count), 1
    )
    picked = jnp.where(same, spread, 0).astype(F32)
    return jnp.sum(picked, axis=1, keepdims=True).astype(jnp.int32)


def partner(index, count, step):
    if count & (count - 1):
        return lax.rem(index + step, count)
    result = 0
    bit = 1
    while bit < count:
        held = lax.rem(lax.div(index, bit), 2)
        result = result + bit * ((1 - held) if step & bit else held)
        bit *= 2
    return result


def kernel(
    n_dp, n_mp, heads,
    ql_in, kl_in, qg_in, kg_in, qh_in, kh_in, qp_in, kp_in, qw_in, kw_in, qm_in, km_in,
    qw_out, kw_out, qm_out, km_out, qy_out, ky_out, final, shrink_out,
    latents, grads, act, picks, state, in_sems,
    near_send, near_recv, own, relay_recv, raw_recv, fin, base, back_send, back_recv, peak_send, peak_recv, peak2_send, peak2_recv,
    row_send, row_recv, mix,
    ns_s, ns_r, fs_s, fin_r, rl_r, rw_r, b_s, b_r, bk_s, bk_r, pk_s, pk_r, pm_s, pm_r, y_s, y_r, m_s, m_r,
):
    dp = lax.axis_index("dp")
    mp = lax.axis_index("mp")
    n_outer = n_dp // 2
    outer = lax.div(dp, 2)
    inner = lax.rem(dp, 2)
    core = lax.rem(mp, 2)
    group = lax.div(mp, 2)
    n_group = n_mp // 2
    q_rows = qm_in.shape[1]
    k_rows = km_in.shape[1]
    width = qm_in.shape[2]
    tokens = qg_in.shape[0]
    tall = q_rows + k_rows
    top_rows = pl.ds(0, k_rows)
    low_rows = pl.ds(k_rows, q_rows)
    other_core = mp + 1 - 2 * core

    loads = (
        ((kl_in, latents.at[:, top_rows]), (ql_in, latents.at[:, low_rows])),
        ((kg_in, grads.at[1]), (qg_in, grads.at[0])),
        ((qp_in, picks.at[0]), (kp_in, picks.at[1])),
        ((qh_in, act.at[0]), (kh_in, act.at[1])),
        (
            (km_in.at[0], state.at[1, top_rows]), (qm_in.at[0], state.at[1, low_rows]),
            (kw_in.at[0], state.at[0, top_rows]), (qw_in.at[0], state.at[0, low_rows]),
        ),
    )
    for i, group_of in enumerate(loads):
        for src, dst in group_of:
            pltpu.make_async_copy(src, dst, in_sems.at[i]).start()

    def loaded(*which):
        for i in which:
            ref = (latents, grads, picks, act, state)[i]
            pltpu.make_async_copy(ref, ref, in_sems.at[i]).wait()

    barrier = pltpu.get_barrier_semaphore()

    def greet(*where):
        pl.semaphore_signal(barrier, inc=1, device_id=where, device_id_type=MESH)

    def owner(step):
        across = lax.rem(dp + (step // n_group) * heads, n_dp)
        return across, 2 * lax.rem(group + step, n_group) + core

    across_x = dp + 1 - 2 * inner
    by = [partner(outer, n_outer, step) for step in range(n_outer)]
    for step in range(n_outer - 1, 0, -1):
        greet(2 * by[step] + inner, mp)
        greet(2 * by[step] + inner, other_core)
        greet(2 * by[step] + 1 - inner, mp)
    greet(across_x, mp)
    greet(across_x, other_core)
    for step in range(2 * n_group - 1, n_group, -1):
        greet(*owner(step))
    for step in range(1, n_mp):
        greet(dp, lax.rem(mp + step, n_mp))

    def copy(src, dst, send, recv, where):
        return pltpu.make_async_remote_copy(
            src_ref=src, dst_ref=dst, send_sem=send, recv_sem=recv,
            device_id=where, device_id_type=MESH,
        )

    all_peaks = copy(peak_recv, peak_recv, pk_s, pk_r, (dp, other_core))
    all_peaks2 = copy(peak2_recv, peak2_recv, pm_s, pm_r, (dp, other_core))
    all_rows = copy(row_recv, row_recv, y_s, y_r, (dp, other_core))

    def term(dst, spot, to_outer, to_inner, parts=(0, 1)):
        slot = 2 * to_outer + to_inner
        half = lax.div(slot, heads)
        cols = pl.ds(pl.multiple_of(lax.rem(slot, heads) * width, width), width)
        first = spot * chunks
        if 0 in parts:
            dst[first] = mm(latents[half, :k_rows], grads[1, :, cols])
        if 1 in parts:
            rest = mm(latents[half, k_rows:], grads[0, :, cols])
            dst[first + 1 : first + chunks] = rest.reshape(chunks - 1, step_rows, width)

    step_rows = k_rows
    chunks = tall // step_rows
    loaded(0, 1)
    entered = 3 * (n_outer - 1) + 2 + (n_mp - 1) + (n_group - 1)
    neighbour = (across_x, mp)
    partner_core = (dp, other_core)
    last = n_outer - 1
    line = n_outer == 4
    inside = lax.rem(lax.div(outer, 2) + lax.rem(outer, 2), 2)

    def at(spot, chunk):
        return spot * chunks + chunk

    if line:
        split_to = by[2] + inside * (by[1] - by[2])
        whole_to = by[1] + inside * (by[2] - by[1])
        order = [by[3], split_to, whole_to, by[0]]
        kept = chunks // 2
        spans = [range(chunks), range(kept), range(chunks), range(chunks)]
    else:
        order = by[::-1]
        spans = [range(chunks)] * n_outer

    def near_copy(spot, chunk):
        where = at(spot, chunk)
        return copy(near_send.at[where], near_recv.at[where], ns_s, ns_r.at[where], neighbour)

    def home(chunk):
        return 2 * group + (1 if chunk else 0)

    fine_slot = 2 if line else n_outer

    def landed(slot, chunk):
        return fin_r.at[n_outer + max(chunk - 1, 0) if slot == fine_slot else slot]

    def final_copy(source, spot, slot, chunk, sent, to):
        return copy(
            source.at[at(spot, chunk)], fin.at[slot, chunk, core], sent, landed(slot, chunk),
            (to, home(chunk)),
        )

    def far_copy(spot, chunk, target):
        return final_copy(own, spot, spot, chunk, fs_s, 2 * target + inner)

    def send_last(which):
        for chunk in which:
            final_copy(near_send, last, last, chunk, ns_s, across_x).start()

    def relay_copy(chunk):
        return copy(
            own.at[at(0, chunk)], relay_recv.at[chunk], fs_s, rl_r.at[chunk],
            (2 * by[1] + inner, mp),
        )

    def raw_copy(first):
        count = chunks - first
        return copy(
            near_send.at[pl.ds(at(1, first), count)], raw_recv.at[pl.ds(first, count)],
            fs_s, rw_r, (2 * split_to + inner, mp),
        )

    def by_role(act):
        for held in range(2):
            pl.when(inside == held)(functools.partial(act, held))

    def send_near(spot, which):
        for chunk in which:
            near_copy(spot, chunk).start()

    term(near_send, 0, order[0], 1 - inner, (0,))
    pl.semaphore_wait(barrier, entered)
    send_near(0, spans[0][:1])
    term(near_send, 0, order[0], 1 - inner, (1,))
    send_near(0, spans[0][1:])
    if line:
        term(near_send, 1, order[1], 1 - inner)
        by_role(lambda held: raw_copy(0 if held else kept).start())
        term(own, 1, order[1], inner)

        def send_split(held):
            for chunk in range(0 if held else kept, chunks):
                far_copy(1, chunk, split_to).start()
            if not held:
                send_near(1, range(kept))

        by_role(send_split)
        term(near_send, 2, order[2], 1 - inner)
        send_near(2, spans[2])

    loaded(2, 3)
    local_heads = picks.shape[1]
    lane = lax.broadcasted_iota(jnp.int32, (1, width), 1)
    peaks = jnp.full((1, width), LOWEST, F32)
    ids = lax.broadcasted_iota(jnp.int32, (picks.shape[3], tokens), 1)
    for head in range(local_heads):
        span = slice(head * width, (head + 1) * width)
        pick_q = (ids == spread_down(picks[0, head])).astype(F32).astype(BF16)
        pick_k = (ids == spread_down(picks[1, head])).astype(F32).astype(BF16)
        score = jnp.sum(
            mm(pick_q, act[0, :, span]) * mm(pick_k, act[1, :, span]), axis=1, keepdims=True
        )
        top = jnp.max(score * SCORE_SCALE, axis=0, keepdims=True)
        peaks = jnp.where(lane == mp * local_heads + head, top, peaks)
    peak_send[...] = peaks
    for step in range(1, n_dp):
        each = copy(
            peak_send, peak_recv.at[step - 1], pk_s, pk_r,
            (lax.rem(dp + step, n_dp), mp),
        )
        each.start()

    if line:
        term(near_send, last, order[last], 1 - inner)
        by_role(lambda held: send_last(range(kept)) if held else None)
    else:
        for spot in range(1, n_outer):
            term(near_send, spot, order[spot], 1 - inner)
            if spot < last:
                send_near(spot, spans[spot])
        send_last(range(chunks))
    for spot in range(n_outer):
        if not (line and spot == 1):
            term(own, spot, order[spot], inner)

    loaded(4)
    for chunk in range(chunks):
        moment = state[1, chunk * step_rows : (chunk + 1) * step_rows]
        own[at(last, chunk)] = MOMENTUM * moment + own[at(last, chunk)]

    def on_core(which):
        return pl.when(core == which)

    def shares(which):
        return pl.ds(0, 1) if which else pl.ds(1, chunks - 1)

    def base_copy(which):
        rows = shares(which)
        source = own.at[pl.ds(at(last, rows.start), rows.size)]
        return copy(source, base.at[rows], b_s, b_r, partner_core)

    def back_copy(which):
        rows = pl.ds(0, shares(1 - which).size)
        return copy(back_send.at[rows], back_recv.at[rows], bk_s, bk_r, partner_core)

    for which in range(2):

        @on_core(which)
        def _():
            base_copy(which).start()

    def meet(spot, chunk):
        near_copy(spot, chunk).wait_recv()
        where = at(spot, chunk)
        own[where] = own[where] + near_recv[where]

    def arrived(slot, members):
        ref = fin.at[slot, pl.ds(members[0], len(members))]
        sem = landed(slot, members[0])
        copy(ref, ref, fs_s, sem, partner_core).wait_recv()

    def pass_on(spot):
        for chunk in spans[spot]:
            meet(spot, chunk)
            far_copy(spot, chunk, order[spot]).start()

    if line:
        def forward(held):
            for chunk in spans[0]:
                meet(0, chunk)
                if held:
                    far_copy(0, chunk, by[3]).start()
                else:
                    relay_copy(chunk).start()
            if not held:
                pass_on(1)
            first = kept if held else 0
            raw_copy(first).wait_recv()
            part = pl.ds(at(last, first), chunks - first)
            near_send[part] = near_send[part] + raw_recv[pl.ds(first, chunks - first)]
            send_last(range(first, chunks))
            for chunk in spans[2]:
                if held:
                    relay_copy(chunk).wait_recv()
                    own[at(2, chunk)] = own[at(2, chunk)] + relay_recv[chunk]
                meet(2, chunk)
                far_copy(2, chunk, whole_to).start()

        by_role(forward)

    else:
        for spot in range(last):
            pass_on(spot)

    def complete(which, chunk):
        if line:
            arrived(2, range(chunk, chunk + 1))
        added = [fin[slot, chunk] for slot in range(1 if line else 0, n_outer)]
        mine = own[at(last, chunk)]
        other = base[chunk]
        for each in added:
            mine = mine + each[which]
            other = other + each[1 - which]
        if which:
            qm_out[0, (chunk - 1) * step_rows : chunk * step_rows] = mine
            back_send[chunk - 1] = other
        else:
            km_out[0] = mine
            back_send[chunk] = other
        return gram(jnp.concatenate([mine, other], axis=0))

    for which, members in enumerate((range(1), range(1, chunks))):

        @on_core(which)
        def _():
            base_copy(1 - which).wait_recv()
            if line:

                @pl.when(inside == 1)
                def _():
                    arrived(0, members)
                    for chunk in members:
                        early = fin[0, chunk]
                        own[at(last, chunk)] = own[at(last, chunk)] + early[which]
                        base[chunk] = base[chunk] + early[1 - which]

            for slot in (1, last) if line else range(n_outer):
                arrived(slot, members)
            pair = complete(which, members[0])
            for chunk in members[1:]:
                pair = pair + complete(which, chunk)
            row_send[...] = fold(pair)

    for step in reversed(range(1, 2 * n_group)):
        each = copy(
            row_send, row_recv.at[step - 1], y_s, y_r, owner(step)
        )
        each.start()
    for which in range(2):

        @on_core(which)
        def _():
            back_copy(which).start()

    all_peaks.wait_recv()
    peaks = jnp.maximum(peaks, jnp.max(peak_recv[...], axis=0))
    peak2_send[...] = peaks
    for step in range(1, n_mp):
        each = copy(
            peak2_send, peak2_recv.at[step - 1], pm_s, pm_r,
            (dp, lax.rem(mp + step, n_mp)),
        )
        each.start()

    @on_core(0)
    def _():
        back_copy(1).wait_recv()
        qm_out[0] = back_recv[...].reshape(q_rows, width)

    @on_core(1)
    def _():
        back_copy(0).wait_recv()
        km_out[0] = back_recv[0]

    all_rows.wait_recv()
    folded = row_send[...] + jnp.sum(row_recv[...], axis=0)
    whole = unfold(folded)
    raw = split(whole)
    raw_square = mm_deep(raw, raw)

    eye = (
        lax.broadcasted_iota(jnp.int32, (width, width), 0)
        == lax.broadcasted_iota(jnp.int32, (width, width), 1)
    ).astype(F32)
    top = width // 2
    diagonal = jnp.sum(folded[:top] * eye[:top], axis=0, keepdims=True) + folded[top:]
    trace = jnp.sum(diagonal, axis=1, keepdims=True)
    scale = 1.0 / jnp.sqrt(trace + 1.0)
    shift = scale * scale
    current = whole * shift
    mixed = None
    swap2 = [
        copy(ref.at[1 - core], ref.at[1 - core], m_s, m_r.at[i], (dp, other_core))
        for i, ref in enumerate((mix, final))
    ]
    for step in range(ITERS):
        parts = split(current)
        square = mm_deep(parts, parts) if step else raw_square * (shift * shift)
        poly = COEFF_A * eye + COEFF_B * current + COEFF_C * square
        if step + 1 == ITERS:
            break
        pair = split(poly)
        mixed = poly * scale if mixed is None else mm_deep(split(mixed), pair)
        if step + 2 == ITERS:
            mix[1 - core] = mixed
            swap2[0].start()
        current = mm_deep(split(mm_deep(pair, parts)), pair)
    final[1 - core] = poly
    swap2[1].start()
    all_peaks2.wait_recv()
    peaks = jnp.maximum(peaks, jnp.max(peak2_recv[...], axis=0))
    mine = jnp.where(lane == lax.rem(dp, heads), peaks, LOWEST)
    peak = jnp.max(jnp.max(mine, axis=0, keepdims=True), axis=1, keepdims=True)
    shrink = jnp.sqrt(CLIP_LEVEL / jnp.maximum(peak, CLIP_LEVEL))
    keep = 1.0 - STEP_SIZE * DECAY
    shrink_out[...] = jnp.broadcast_to(shrink, shrink_out.shape)
    qw_out[0] = (state[0, k_rows:] * keep) * shrink
    kw_out[0] = (state[0, :k_rows] * keep) * shrink
    def drain(sent, passed):
        for count, ref, sem in ((sent, near_send, ns_s), (passed, own, fs_s)):
            part = ref.at[pl.ds(0, count)]
            copy(part, part, sem, sem, partner_core).wait_send()

    if line:
        by_role(
            lambda held: drain(
                last * chunks + (0 if held else kept), last * chunks + (chunks if held else kept)
            )
        )
    else:
        drain(n_outer * chunks, last * chunks)
    for each in (all_peaks, all_peaks2, all_rows):
        each.wait_send()
    for which in range(2):

        @on_core(which)
        def _():
            base_copy(which).wait_send()
            back_copy(which).wait_send()

    swap2[0].wait_recv()
    for which, (moment, part_out) in enumerate(((qm_out, qy_out), (km_out, ky_out))):
        part_out[0] = mm3(split(moment[0]), split(mix[which]))
    swap2[1].wait_recv()
    copy(mix, mix, m_s, m_s, (dp, other_core)).wait_send()


def finish(
    n_mp, qw_ref, kw_ref, qm_ref, km_ref, qy_ref, ky_ref, final_ref, shrink_ref,
    qw_out, kw_out, qm_out, km_out, qw_new, kw_new, sems,
):
    stores = [
        pltpu.make_async_copy(src, dst, sems.at[i])
        for i, (src, dst) in enumerate((
            (qm_ref, qm_out), (km_ref, km_out), (kw_new, kw_out), (qw_new, qw_out),
        ))
    ]
    stores[0].start()
    stores[1].start()
    groups = ((1, kw_ref, ky_ref, kw_new, stores[2]), (0, qw_ref, qy_ref, qw_new, stores[3]))
    for which, weight, part, weight_new, store in groups:
        size = STEP_SIZE * 0.2 * math.sqrt(2 * n_mp * part.shape[1])
        ortho = mm3(split(part[0]), split(final_ref[which]))
        weight_new[0] = weight[0] - (size * ortho) * shrink_ref[...]
        store.start()
    for each in stores:
        each.wait()


def local(
    q_latent, kv_latent, q_head_grad, k_head_grad, q_heads, k_heads,
    query_pick, key_pick, q_weight, k_weight, q_moment, k_moment,
):
    n_dp = lax.axis_size("dp")
    n_mp = lax.axis_size("mp")
    heads = n_dp // 2
    n_outer = n_dp // 2
    n_group = n_mp // 2
    rows = q_latent.shape[2] + kv_latent.shape[2]
    width = q_moment.shape[2]
    operands = (
        q_latent.transpose(1, 2, 0), kv_latent.transpose(1, 2, 0), q_head_grad, k_head_grad,
        q_heads, k_heads, query_pick.transpose(2, 0, 1), key_pick.transpose(2, 0, 1),
        q_weight, k_weight, q_moment, k_moment,
    )
    vmem = pltpu.VMEM
    dma = pltpu.SemaphoreType.DMA
    square = (width, width)
    folded = (width // 2 + 1, width)
    tile = (1, width)
    tokens = q_latent.shape[0]
    k_rows = k_moment.shape[1]
    chunks = rows // k_rows

    def blocks(count):
        return vmem((count, k_rows, width), F32)

    shapes = [a.shape for a in (q_weight, k_weight, q_moment, k_moment)]
    parts = pl.pallas_call(
        functools.partial(kernel, n_dp, n_mp, heads),
        out_shape=[vmem(shape, F32) for shape in shapes + shapes[2:] + [(2,) + square, tile]],
        in_specs=[pl.BlockSpec(memory_space=pl.ANY)] * 12,
        out_specs=[pl.BlockSpec(memory_space=vmem)] * 8,
        scratch_shapes=[
            vmem((2, rows, tokens), BF16),
            vmem((2,) + q_head_grad.shape, BF16),
            vmem((2,) + q_heads.shape, BF16),
            vmem((2,) + operands[6].shape, jnp.int32),
            vmem((2, rows, width), F32),
            dma((5,)),
            blocks(n_outer * chunks), blocks((n_outer - 1) * chunks), blocks(n_outer * chunks),
            blocks(chunks), blocks(chunks),
            vmem((n_outer, chunks, 2, k_rows, width), F32),
            blocks(chunks), blocks(chunks - 1), blocks(chunks - 1),
            vmem(tile, F32),
            vmem((n_dp - 1,) + tile, F32),
            vmem(tile, F32),
            vmem((n_mp - 1,) + tile, F32),
            vmem(folded, F32),
            vmem((2 * n_group - 1,) + folded, F32),
            vmem((2,) + square, F32),
            dma, dma(((n_outer - 1) * chunks,)),
            dma, dma((n_outer + (chunks - 1 if n_outer == 4 else 0),)), dma((chunks,)), dma,
            dma, dma, dma, dma, dma, dma, dma, dma, dma, dma,
            dma, dma((2,)),
        ],
        compiler_params=pltpu.CompilerParams(
            collective_id=0, has_side_effects=True, vmem_limit_bytes=56 * 1024 * 1024
        ),
    )(*operands)
    return pl.pallas_call(
        functools.partial(finish, n_mp),
        out_shape=[jax.ShapeDtypeStruct(shape, F32) for shape in shapes],
        in_specs=[pl.BlockSpec(memory_space=vmem)] * 8,
        out_specs=[pl.BlockSpec(memory_space=pl.ANY)] * 4,
        scratch_shapes=[vmem(shape, F32) for shape in shapes[:2]] + [dma((4,))],
    )(*[pltpu.with_memory_space_constraint(part, vmem) for part in parts])


def solution(mesh):
    rows3 = P("dp", "mp", None)
    in_specs = (
        P("dp", None, "mp"), P("dp", None, "mp"), P("dp", None), P("dp", None),
        P("dp", "mp"), P("dp", "mp"), P("dp", None, "mp"), P("dp", None, "mp"),
        rows3, rows3, rows3, rows3,
    )
    return jax.shard_map(
        lambda *args: tuple(local(*args)),
        mesh=mesh, in_specs=in_specs, out_specs=(rows3,) * 4, check_vma=False,
    )
```

```python
import functools
import math

import jax
import jax.numpy as jnp
from jax import lax
from jax.experimental import pallas as pl
from jax.experimental.pallas import tpu as pltpu
from jax.sharding import PartitionSpec as P

ITERS = 5
MOMENTUM = 0.95
STEP_SIZE = 1.0
DECAY = 0.1
CLIP_LEVEL = 0.1
SCORE_SCALE = 1.0 / math.sqrt(192.0)
COEFF_A = 3.4445
COEFF_B = -4.775
COEFF_C = 2.0315
LOWEST = -1e30
MESH = pl.DeviceIdType.MESH
F32 = jnp.float32
BF16 = jnp.bfloat16


def split(value):
    high = value.astype(BF16)
    return high, (value - high.astype(F32)).astype(BF16)


def mm(a, b):
    return jnp.dot(a, b, preferred_element_type=F32)


def mm3(a, b):
    both = mm(a[0], jnp.concatenate([b[0], b[1]], axis=1))
    width = b[0].shape[1]
    return both[:, :width] + (both[:, width:] + mm(a[1], b[0]))


def mm_deep(a, b):
    return mm(
        jnp.concatenate([a[0], a[1], a[0]], axis=1), jnp.concatenate([b[0], b[0], b[1]], axis=0)
    )


def gram(rows):
    high, low = split(rows)
    left = jnp.concatenate([high, low, high], axis=0)
    return mm(left.T, jnp.concatenate([high, high, low], axis=0))


def fold(matrix):
    width = matrix.shape[0]
    half = width // 2
    row = lax.broadcasted_iota(jnp.int32, (half, width), 0)
    lane = lax.broadcasted_iota(jnp.int32, (half, width), 1)
    lower = matrix[half:]
    body = jnp.where(lane >= row, matrix[:half], pltpu.roll(lower, half, 1))
    ends = jnp.sum(jnp.where(lane == row + half, lower, 0.0), axis=0, keepdims=True)
    return jnp.concatenate([body, ends], axis=0)


def unfold(message):
    width = message.shape[1]
    half = width // 2
    row = lax.broadcasted_iota(jnp.int32, (half, width), 0)
    lane = lax.broadcasted_iota(jnp.int32, (half, width), 1)
    body = message[:half]
    ends = jnp.broadcast_to(message[half : half + 1], (half, width))
    top = jnp.where(lane >= row, body, 0.0)
    strict = jnp.where((lane >= half) & (lane - half < row), pltpu.roll(body, half, 1), 0.0)
    one_side = jnp.concatenate([top, jnp.where(lane == row + half, ends, strict)], axis=0)
    full_row = lax.broadcasted_iota(jnp.int32, (width, width), 0)
    full_lane = lax.broadcasted_iota(jnp.int32, (width, width), 1)
    return one_side + jnp.where(full_row == full_lane, 0.0, one_side.T)


def spread_down(row):
    count = row.shape[1]
    spread = jnp.broadcast_to(row, (count, count))
    same = lax.broadcasted_iota(jnp.int32, (count, count), 0) == lax.broadcasted_iota(
        jnp.int32, (count, count), 1
    )
    picked = jnp.where(same, spread, 0).astype(F32)
    return jnp.sum(picked, axis=1, keepdims=True).astype(jnp.int32)


def partner(index, count, step):
    if count & (count - 1):
        return lax.rem(index + step, count)
    result = 0
    bit = 1
    while bit < count:
        held = lax.rem(lax.div(index, bit), 2)
        result = result + bit * ((1 - held) if step & bit else held)
        bit *= 2
    return result


def kernel(
    n_dp, n_mp, heads,
    ql_in, kl_in, qg_in, kg_in, qh_in, kh_in, qp_in, kp_in, qw_in, kw_in, qm_in, km_in,
    qw_out, kw_out, qm_out, km_out, qy_out, ky_out, final, shrink_out,
    latents, grads, act, picks, state, in_sems,
    near_send, near_recv, own, relay_recv, raw_recv, fin, base, back_send, back_recv, peak_send, peak_recv, peak2_send, peak2_recv,
    row_send, row_recv, mix,
    ns_s, ns_r, fs_s, fin_r, rl_r, rw_r, b_s, b_r, bk_s, bk_r, pk_s, pk_r, pm_s, pm_r, y_s, y_r, m_s, m_r,
):
    dp = lax.axis_index("dp")
    mp = lax.axis_index("mp")
    n_outer = n_dp // 2
    outer = lax.div(dp, 2)
    inner = lax.rem(dp, 2)
    core = lax.rem(mp, 2)
    group = lax.div(mp, 2)
    n_group = n_mp // 2
    q_rows = qm_in.shape[1]
    k_rows = km_in.shape[1]
    width = qm_in.shape[2]
    tokens = qg_in.shape[0]
    tall = q_rows + k_rows
    top_rows = pl.ds(0, k_rows)
    low_rows = pl.ds(k_rows, q_rows)
    other_core = mp + 1 - 2 * core

    loads = (
        ((kl_in, latents.at[:, top_rows]), (ql_in, latents.at[:, low_rows])),
        ((kg_in, grads.at[1]), (qg_in, grads.at[0])),
        ((qp_in, picks.at[0]), (kp_in, picks.at[1])),
        ((qh_in, act.at[0]), (kh_in, act.at[1])),
        (
            (km_in.at[0], state.at[1, top_rows]), (qm_in.at[0], state.at[1, low_rows]),
            (kw_in.at[0], state.at[0, top_rows]), (qw_in.at[0], state.at[0, low_rows]),
        ),
    )
    for i, group_of in enumerate(loads):
        for src, dst in group_of:
            pltpu.make_async_copy(src, dst, in_sems.at[i]).start()

    def loaded(*which):
        for i in which:
            ref = (latents, grads, picks, act, state)[i]
            pltpu.make_async_copy(ref, ref, in_sems.at[i]).wait()

    barrier = pltpu.get_barrier_semaphore()

    def greet(*where):
        pl.semaphore_signal(barrier, inc=1, device_id=where, device_id_type=MESH)

    def owner(step):
        across = lax.rem(dp + (step // n_group) * heads, n_dp)
        return across, 2 * lax.rem(group + step, n_group) + core

    across_x = dp + 1 - 2 * inner
    by = [partner(outer, n_outer, step) for step in range(n_outer)]
    for step in range(n_outer - 1, 0, -1):
        greet(2 * by[step] + inner, mp)
        greet(2 * by[step] + inner, other_core)
        greet(2 * by[step] + 1 - inner, mp)
    greet(across_x, mp)
    greet(across_x, other_core)
    for step in range(2 * n_group - 1, n_group, -1):
        greet(*owner(step))
    for step in range(1, n_mp):
        greet(dp, lax.rem(mp + step, n_mp))

    def copy(src, dst, send, recv, where):
        return pltpu.make_async_remote_copy(
            src_ref=src, dst_ref=dst, send_sem=send, recv_sem=recv,
            device_id=where, device_id_type=MESH,
        )

    all_peaks = copy(peak_recv, peak_recv, pk_s, pk_r, (dp, other_core))
    all_peaks2 = copy(peak2_recv, peak2_recv, pm_s, pm_r, (dp, other_core))
    all_rows = copy(row_recv, row_recv, y_s, y_r, (dp, other_core))

    def term(dst, spot, to_outer, to_inner, parts=(0, 1)):
        slot = 2 * to_outer + to_inner
        half = lax.div(slot, heads)
        cols = pl.ds(pl.multiple_of(lax.rem(slot, heads) * width, width), width)
        first = spot * chunks
        if 0 in parts:
            dst[first] = mm(latents[half, :k_rows], grads[1, :, cols])
        if 1 in parts:
            rest = mm(latents[half, k_rows:], grads[0, :, cols])
            dst[first + 1 : first + chunks] = rest.reshape(chunks - 1, step_rows, width)

    step_rows = k_rows
    chunks = tall // step_rows
    loaded(0, 1)
    entered = 3 * (n_outer - 1) + 2 + (n_mp - 1) + (n_group - 1)
    neighbour = (across_x, mp)
    partner_core = (dp, other_core)
    last = n_outer - 1
    line = n_outer == 4
    inside = lax.rem(lax.div(outer, 2) + lax.rem(outer, 2), 2)

    def at(spot, chunk):
        return spot * chunks + chunk

    if line:
        split_to = by[2] + inside * (by[1] - by[2])
        whole_to = by[1] + inside * (by[2] - by[1])
        order = [by[3], split_to, whole_to, by[0]]
        kept = chunks // 2
        spans = [range(chunks), range(kept), range(chunks), range(chunks)]
    else:
        order = by[::-1]
        spans = [range(chunks)] * n_outer

    def near_copy(spot, chunk):
        where = at(spot, chunk)
        return copy(near_send.at[where], near_recv.at[where], ns_s, ns_r.at[where], neighbour)

    def home(chunk):
        return 2 * group + (1 if chunk else 0)

    fine_slot = 2 if line else n_outer

    def landed(slot, chunk):
        return fin_r.at[n_outer + max(chunk - 1, 0) if slot == fine_slot else slot]

    def final_copy(source, spot, slot, chunk, sent, to):
        return copy(
            source.at[at(spot, chunk)], fin.at[slot, chunk, core], sent, landed(slot, chunk),
            (to, home(chunk)),
        )

    def far_copy(spot, chunk, target):
        return final_copy(own, spot, spot, chunk, fs_s, 2 * target + inner)

    def send_last(which):
        for chunk in which:
            final_copy(near_send, last, last, chunk, ns_s, across_x).start()

    def relay_copy(chunk):
        return copy(
            own.at[at(0, chunk)], relay_recv.at[chunk], fs_s, rl_r.at[chunk],
            (2 * by[1] + inner, mp),
        )

    def raw_copy(first):
        count = chunks - first
        return copy(
            near_send.at[pl.ds(at(1, first), count)], raw_recv.at[pl.ds(first, count)],
            fs_s, rw_r, (2 * split_to + inner, mp),
        )

    def by_role(act):
        for held in range(2):
            pl.when(inside == held)(functools.partial(act, held))

    def send_near(spot, which):
        for chunk in which:
            near_copy(spot, chunk).start()

    term(near_send, 0, order[0], 1 - inner, (0,))
    pl.semaphore_wait(barrier, entered)
    send_near(0, spans[0][:1])
    term(near_send, 0, order[0], 1 - inner, (1,))
    send_near(0, spans[0][1:])
    if line:
        term(near_send, 1, order[1], 1 - inner)
        by_role(lambda held: raw_copy(0 if held else kept).start())
        term(own, 1, order[1], inner)

        def send_split(held):
            for chunk in range(0 if held else kept, chunks):
                far_copy(1, chunk, split_to).start()
            if not held:
                send_near(1, range(kept))

        by_role(send_split)
        term(near_send, 2, order[2], 1 - inner)
        send_near(2, spans[2])

    loaded(2, 3)
    local_heads = picks.shape[1]
    lane = lax.broadcasted_iota(jnp.int32, (1, width), 1)
    peaks = jnp.full((1, width), LOWEST, F32)
    ids = lax.broadcasted_iota(jnp.int32, (picks.shape[3], tokens), 1)
    for head in range(local_heads):
        span = slice(head * width, (head + 1) * width)
        pick_q = (ids == spread_down(picks[0, head])).astype(F32).astype(BF16)
        pick_k = (ids == spread_down(picks[1, head])).astype(F32).astype(BF16)
        score = jnp.sum(
            mm(pick_q, act[0, :, span]) * mm(pick_k, act[1, :, span]), axis=1, keepdims=True
        )
        top = jnp.max(score * SCORE_SCALE, axis=0, keepdims=True)
        peaks = jnp.where(lane == mp * local_heads + head, top, peaks)
    peak_send[...] = peaks
    for step in range(1, n_dp):
        each = copy(
            peak_send, peak_recv.at[step - 1], pk_s, pk_r,
            (lax.rem(dp + step, n_dp), mp),
        )
        each.start()

    if line:
        term(near_send, last, order[last], 1 - inner)
        by_role(lambda held: send_last(range(kept)) if held else None)
    else:
        for spot in range(1, n_outer):
            term(near_send, spot, order[spot], 1 - inner)
            if spot < last:
                send_near(spot, spans[spot])
        send_last(range(chunks))
    for spot in range(n_outer):
        if not (line and spot == 1):
            term(own, spot, order[spot], inner)

    loaded(4)
    for chunk in range(chunks):
        moment = state[1, chunk * step_rows : (chunk + 1) * step_rows]
        own[at(last, chunk)] = MOMENTUM * moment + own[at(last, chunk)]

    def on_core(which):
        return pl.when(core == which)

    def shares(which):
        return pl.ds(0, 1) if which else pl.ds(1, chunks - 1)

    def base_copy(which):
        rows = shares(which)
        source = own.at[pl.ds(at(last, rows.start), rows.size)]
        return copy(source, base.at[rows], b_s, b_r, partner_core)

    def back_copy(which):
        rows = pl.ds(0, shares(1 - which).size)
        return copy(back_send.at[rows], back_recv.at[rows], bk_s, bk_r, partner_core)

    for which in range(2):

        @on_core(which)
        def _():
            base_copy(which).start()

    def meet(spot, chunk):
        near_copy(spot, chunk).wait_recv()
        where = at(spot, chunk)
        own[where] = own[where] + near_recv[where]

    def arrived(slot, members):
        ref = fin.at[slot, pl.ds(members[0], len(members))]
        sem = landed(slot, members[0])
        copy(ref, ref, fs_s, sem, partner_core).wait_recv()

    def pass_on(spot):
        for chunk in spans[spot]:
            meet(spot, chunk)
            far_copy(spot, chunk, order[spot]).start()

    if line:
        def forward(held):
            for chunk in spans[0]:
                meet(0, chunk)
                if held:
                    far_copy(0, chunk, by[3]).start()
                else:
                    relay_copy(chunk).start()
            first = kept if held else 0
            raw_copy(first).wait_recv()
            part = pl.ds(at(last, first), chunks - first)
            near_send[part] = near_send[part] + raw_recv[pl.ds(first, chunks - first)]
            send_last(range(first, chunks))
            if not held:
                pass_on(1)
            for chunk in spans[2]:
                if held:
                    relay_copy(chunk).wait_recv()
                    own[at(2, chunk)] = own[at(2, chunk)] + relay_recv[chunk]
                meet(2, chunk)
                far_copy(2, chunk, whole_to).start()

        by_role(forward)

    else:
        for spot in range(last):
            pass_on(spot)

    def complete(which, chunk):
        if line:
            arrived(2, range(chunk, chunk + 1))
        added = [fin[slot, chunk] for slot in range(1 if line else 0, n_outer)]
        mine = own[at(last, chunk)]
        other = base[chunk]
        for each in added:
            mine = mine + each[which]
            other = other + each[1 - which]
        if which:
            qm_out[0, (chunk - 1) * step_rows : chunk * step_rows] = mine
            back_send[chunk - 1] = other
        else:
            km_out[0] = mine
            back_send[chunk] = other
        return gram(jnp.concatenate([mine, other], axis=0))

    for which, members in enumerate((range(1), range(1, chunks))):

        @on_core(which)
        def _():
            base_copy(1 - which).wait_recv()
            if line:

                @pl.when(inside == 1)
                def _():
                    arrived(0, members)
                    for chunk in members:
                        early = fin[0, chunk]
                        own[at(last, chunk)] = own[at(last, chunk)] + early[which]
                        base[chunk] = base[chunk] + early[1 - which]

            for slot in (1, last) if line else range(n_outer):
                arrived(slot, members)
            pair = complete(which, members[0])
            for chunk in members[1:]:
                pair = pair + complete(which, chunk)
            row_send[...] = fold(pair)

    for step in reversed(range(1, 2 * n_group)):
        each = copy(
            row_send, row_recv.at[step - 1], y_s, y_r, owner(step)
        )
        each.start()
    for which in range(2):

        @on_core(which)
        def _():
            back_copy(which).start()

    all_peaks.wait_recv()
    peaks = jnp.maximum(peaks, jnp.max(peak_recv[...], axis=0))
    peak2_send[...] = peaks
    for step in range(1, n_mp):
        each = copy(
            peak2_send, peak2_recv.at[step - 1], pm_s, pm_r,
            (dp, lax.rem(mp + step, n_mp)),
        )
        each.start()

    @on_core(0)
    def _():
        back_copy(1).wait_recv()
        qm_out[0] = back_recv[...].reshape(q_rows, width)

    @on_core(1)
    def _():
        back_copy(0).wait_recv()
        km_out[0] = back_recv[0]

    all_rows.wait_recv()
    folded = row_send[...] + jnp.sum(row_recv[...], axis=0)
    whole = unfold(folded)
    raw = split(whole)
    raw_square = mm_deep(raw, raw)

    eye = (
        lax.broadcasted_iota(jnp.int32, (width, width), 0)
        == lax.broadcasted_iota(jnp.int32, (width, width), 1)
    ).astype(F32)
    top = width // 2
    diagonal = jnp.sum(folded[:top] * eye[:top], axis=0, keepdims=True) + folded[top:]
    trace = jnp.sum(diagonal, axis=1, keepdims=True)
    scale = 1.0 / jnp.sqrt(trace + 1.0)
    shift = scale * scale
    current = whole * shift
    mixed = None
    swap2 = [
        copy(ref.at[1 - core], ref.at[1 - core], m_s, m_r.at[i], (dp, other_core))
        for i, ref in enumerate((mix, final))
    ]
    for step in range(ITERS):
        parts = split(current)
        square = mm_deep(parts, parts) if step else raw_square * (shift * shift)
        poly = COEFF_A * eye + COEFF_B * current + COEFF_C * square
        if step + 1 == ITERS:
            break
        pair = split(poly)
        mixed = poly * scale if mixed is None else mm_deep(split(mixed), pair)
        if step + 2 == ITERS:
            mix[1 - core] = mixed
            swap2[0].start()
        current = mm_deep(split(mm_deep(pair, parts)), pair)
    final[1 - core] = poly
    swap2[1].start()
    all_peaks2.wait_recv()
    peaks = jnp.maximum(peaks, jnp.max(peak2_recv[...], axis=0))
    mine = jnp.where(lane == lax.rem(dp, heads), peaks, LOWEST)
    peak = jnp.max(jnp.max(mine, axis=0, keepdims=True), axis=1, keepdims=True)
    shrink = jnp.sqrt(CLIP_LEVEL / jnp.maximum(peak, CLIP_LEVEL))
    keep = 1.0 - STEP_SIZE * DECAY
    shrink_out[...] = jnp.broadcast_to(shrink, shrink_out.shape)
    qw_out[0] = (state[0, k_rows:] * keep) * shrink
    kw_out[0] = (state[0, :k_rows] * keep) * shrink
    def drain(sent, passed):
        for count, ref, sem in ((sent, near_send, ns_s), (passed, own, fs_s)):
            part = ref.at[pl.ds(0, count)]
            copy(part, part, sem, sem, partner_core).wait_send()

    if line:
        by_role(
            lambda held: drain(
                last * chunks + (0 if held else kept), last * chunks + (chunks if held else kept)
            )
        )
    else:
        drain(n_outer * chunks, last * chunks)
    for each in (all_peaks, all_peaks2, all_rows):
        each.wait_send()
    for which in range(2):

        @on_core(which)
        def _():
            base_copy(which).wait_send()
            back_copy(which).wait_send()

    swap2[0].wait_recv()
    for which, (moment, part_out) in enumerate(((qm_out, qy_out), (km_out, ky_out))):
        part_out[0] = mm3(split(moment[0]), split(mix[which]))
    swap2[1].wait_recv()
    copy(mix, mix, m_s, m_s, (dp, other_core)).wait_send()


def finish(
    n_mp, qw_ref, kw_ref, qm_ref, km_ref, qy_ref, ky_ref, final_ref, shrink_ref,
    qw_out, kw_out, qm_out, km_out, qw_new, kw_new, sems,
):
    stores = [
        pltpu.make_async_copy(src, dst, sems.at[i])
        for i, (src, dst) in enumerate((
            (qm_ref, qm_out), (km_ref, km_out), (kw_new, kw_out), (qw_new, qw_out),
        ))
    ]
    stores[0].start()
    stores[1].start()
    groups = ((1, kw_ref, ky_ref, kw_new, stores[2]), (0, qw_ref, qy_ref, qw_new, stores[3]))
    for which, weight, part, weight_new, store in groups:
        size = STEP_SIZE * 0.2 * math.sqrt(2 * n_mp * part.shape[1])
        ortho = mm3(split(part[0]), split(final_ref[which]))
        weight_new[0] = weight[0] - (size * ortho) * shrink_ref[...]
        store.start()
    for each in stores:
        each.wait()


def local(
    q_latent, kv_latent, q_head_grad, k_head_grad, q_heads, k_heads,
    query_pick, key_pick, q_weight, k_weight, q_moment, k_moment,
):
    n_dp = lax.axis_size("dp")
    n_mp = lax.axis_size("mp")
    heads = n_dp // 2
    n_outer = n_dp // 2
    n_group = n_mp // 2
    rows = q_latent.shape[2] + kv_latent.shape[2]
    width = q_moment.shape[2]
    operands = (
        q_latent.transpose(1, 2, 0), kv_latent.transpose(1, 2, 0), q_head_grad, k_head_grad,
        q_heads, k_heads, query_pick.transpose(2, 0, 1), key_pick.transpose(2, 0, 1),
        q_weight, k_weight, q_moment, k_moment,
    )
    vmem = pltpu.VMEM
    dma = pltpu.SemaphoreType.DMA
    square = (width, width)
    folded = (width // 2 + 1, width)
    tile = (1, width)
    tokens = q_latent.shape[0]
    k_rows = k_moment.shape[1]
    chunks = rows // k_rows

    def blocks(count):
        return vmem((count, k_rows, width), F32)

    shapes = [a.shape for a in (q_weight, k_weight, q_moment, k_moment)]
    parts = pl.pallas_call(
        functools.partial(kernel, n_dp, n_mp, heads),
        out_shape=[vmem(shape, F32) for shape in shapes + shapes[2:] + [(2,) + square, tile]],
        in_specs=[pl.BlockSpec(memory_space=pl.ANY)] * 12,
        out_specs=[pl.BlockSpec(memory_space=vmem)] * 8,
        scratch_shapes=[
            vmem((2, rows, tokens), BF16),
            vmem((2,) + q_head_grad.shape, BF16),
            vmem((2,) + q_heads.shape, BF16),
            vmem((2,) + operands[6].shape, jnp.int32),
            vmem((2, rows, width), F32),
            dma((5,)),
            blocks(n_outer * chunks), blocks((n_outer - 1) * chunks), blocks(n_outer * chunks),
            blocks(chunks), blocks(chunks),
            vmem((n_outer, chunks, 2, k_rows, width), F32),
            blocks(chunks), blocks(chunks - 1), blocks(chunks - 1),
            vmem(tile, F32),
            vmem((n_dp - 1,) + tile, F32),
            vmem(tile, F32),
            vmem((n_mp - 1,) + tile, F32),
            vmem(folded, F32),
            vmem((2 * n_group - 1,) + folded, F32),
            vmem((2,) + square, F32),
            dma, dma(((n_outer - 1) * chunks,)),
            dma, dma((n_outer + (chunks - 1 if n_outer == 4 else 0),)), dma((chunks,)), dma,
            dma, dma, dma, dma, dma, dma, dma, dma, dma, dma,
            dma, dma((2,)),
        ],
        compiler_params=pltpu.CompilerParams(
            collective_id=0, has_side_effects=True, vmem_limit_bytes=56 * 1024 * 1024
        ),
    )(*operands)
    return pl.pallas_call(
        functools.partial(finish, n_mp),
        out_shape=[jax.ShapeDtypeStruct(shape, F32) for shape in shapes],
        in_specs=[pl.BlockSpec(memory_space=vmem)] * 8,
        out_specs=[pl.BlockSpec(memory_space=pl.ANY)] * 4,
        scratch_shapes=[vmem(shape, F32) for shape in shapes[:2]] + [dma((4,))],
    )(*[pltpu.with_memory_space_constraint(part, vmem) for part in parts])


def solution(mesh):
    rows3 = P("dp", "mp", None)
    in_specs = (
        P("dp", None, "mp"), P("dp", None, "mp"), P("dp", None), P("dp", None),
        P("dp", "mp"), P("dp", "mp"), P("dp", None, "mp"), P("dp", None, "mp"),
        rows3, rows3, rows3, rows3,
    )
    return jax.shard_map(
        lambda *args: tuple(local(*args)),
        mesh=mesh, in_specs=in_specs, out_specs=(rows3,) * 4, check_vma=False,
    )
```
